32 devices in a mesh: rep: 1 (over z), dp: 32 (over x, y, core).
Axes of the slice: x: 4, y: 4, z: 1, core: 2. Of those that a mesh axis runs over, the one named last changes fastest.
The devices are a block of a 4x4x8 slice.
Arguments:
- x: bfloat16 [32, 1024, 1280], P(('rep', 'dp'))
- dy: bfloat16 [32, 1024, 1280], P(('rep', 'dp'))
- wq: bfloat16 [2, 1280, 1280], P(None, 'dp')
- wk: bfloat16 [2, 1280, 1280], P(None, 'dp')
- wv: bfloat16 [2, 1280, 1280], P(None, 'dp')
- wo: bfloat16 [2, 1280, 1280], P(None, 'dp')
- w_gate: bfloat16 [2, 1280, 3456], P(None, 'dp')
- w_up: bfloat16 [2, 1280, 3456], P(None, 'dp')
- w_down: bfloat16 [2, 3456, 1280], P(None, 'dp')
Outputs:
- output 1: bfloat16 [32, 1024, 1280], P(('rep', 'dp'))
- output 2: bfloat16 [2, 1280, 1280], P('rep', 'dp')
- output 3: bfloat16 [2, 1280, 1280], P('rep', 'dp')
- output 4: bfloat16 [2, 1280, 1280], P('rep', 'dp')
- output 5: bfloat16 [2, 1280, 1280], P('rep', 'dp')
- output 6: bfloat16 [2, 1280, 3456], P('rep', 'dp')
- output 7: bfloat16 [2, 1280, 3456], P('rep', 'dp')
- output 8: bfloat16 [2, 3456, 1280], P('rep', 'dp')
All inputs are finite; a program needn't handle non-finite values.
Results may differ from the reference program's by a relative error of at most 0.0255.
Values are sent between devices in bfloat16 or wider.
A program may use at most 768 MiB of HBM per device.

```python
import jax
import jax.numpy as jnp
from jax import lax

SEQUENCES = 32
TOKENS = 1024
D = 1280
HEADS = 10
KV_HEADS = 10
HEAD = 128
FF = 3456
LAYERS = 2
THETA = 10000
NAMES = ("wq", "wk", "wv", "wo", "w_gate", "w_up", "w_down")
SHAPES = {
    "wq": (LAYERS, D, HEADS * HEAD),
    "wk": (LAYERS, D, KV_HEADS * HEAD),
    "wv": (LAYERS, D, KV_HEADS * HEAD),
    "wo": (LAYERS, HEADS * HEAD, D),
    "w_gate": (LAYERS, D, FF),
    "w_up": (LAYERS, D, FF),
    "w_down": (LAYERS, FF, D),
}


def bump(key, n, height):
    away = (jnp.arange(n, dtype=jnp.int32) - jax.random.randint(key, (), 0, n, jnp.int32)) % n
    return jnp.where(away < n // 8, height, 1.0)


def together(key, own, strength):
    shared = jax.random.normal(key, own.shape[1:], jnp.float32)
    return (own + strength * shared) * lax.rsqrt(1 + strength * strength)


def setup_inputs(seed: int = 0, part: int = 0) -> dict:
    kx, kdy, ka, kb, kz, kf, kh, kl, *keys = jax.random.split(jax.random.key(seed), 8 + 3 * len(NAMES))
    kx, kdy, ka, kb = (jax.random.fold_in(k, part) for k in (kx, kdy, ka, kb))
    kw, km, kv = (keys[i::3] for i in range(3))
    shape = (SEQUENCES, TOKENS, D)
    much_x, much_dy = jax.random.uniform(kz, (2,), jnp.float32, 0.0, 1.0)
    loud = 2.0 ** jax.random.uniform(jax.random.fold_in(kz, 1), (), jnp.float32, -1.0, 2.0)
    layers = 2.0 ** jax.random.uniform(kl, (LAYERS, 1, 1), jnp.float32, -1.0, 1.0)
    times = {"wq": 1.0, "wk": 1.0, "wv": 2.0, "wo": layers, "w_gate": 1.0, "w_up": bump(kh, FF, 4.0), "w_down": layers}
    x = together(ka, jax.random.normal(kx, shape, jnp.float32), much_x) * bump(kf, D, 4.0)
    dy = together(kb, jax.random.normal(kdy, shape, jnp.float32), much_dy)
    drawn = {"x": x.astype(jnp.bfloat16), "dy": (loud * dy * (SEQUENCES * TOKENS) ** -0.5).astype(jnp.bfloat16)}
    for key, name in zip(kw, NAMES, strict=True):
        drawn[name] = (jax.random.normal(key, SHAPES[name], jnp.float32) * SHAPES[name][1] ** -0.5 * times[name]).astype(jnp.bfloat16)
    return drawn


def matmul(a, w):
    return jnp.dot(a, w, preferred_element_type=jnp.float32).astype(jnp.bfloat16)


def normed(h):
    wide = h.astype(jnp.float32)
    scale = lax.rsqrt(jnp.mean(wide**2, -1, keepdims=True) + 1e-6)
    return (wide * scale).astype(jnp.bfloat16)


def turned(t, theta):
    half = t.shape[-1] // 2
    angle = jnp.arange(t.shape[0], dtype=jnp.float32)[:, None] * theta ** (-jnp.arange(half, dtype=jnp.float32) / half)
    cos, sin = jnp.cos(angle)[:, None], jnp.sin(angle)[:, None]
    a, b = t[..., :half].astype(jnp.float32), t[..., half:].astype(jnp.float32)
    return jnp.concatenate([a * cos - b * sin, b * cos + a * sin], -1).astype(jnp.bfloat16)


def seen_by(q, k, v):
    tokens, kv = q.shape[0], k.shape[1]
    q = q.reshape(tokens, kv, -1, q.shape[-1])
    scores = jnp.einsum("tgsd,ugd->gstu", q.astype(jnp.float32), k.astype(jnp.float32)) * q.shape[-1] ** -0.5
    place = jnp.arange(tokens)
    weights = jax.nn.softmax(jnp.where(place[:, None] >= place, scores, -jnp.inf), -1).astype(jnp.bfloat16)
    return jnp.einsum("gstu,ugd->tgsd", weights.astype(jnp.float32), v.astype(jnp.float32)).astype(jnp.bfloat16).reshape(tokens, -1)


def layer(h, w):
    a = normed(h)
    q, k = (turned(matmul(a, w[name]).reshape(h.shape[0], -1, HEAD), THETA) for name in ("wq", "wk"))
    h = h + matmul(seen_by(q, k, matmul(a, w["wv"]).reshape(h.shape[0], -1, HEAD)), w["wo"])
    b = normed(h)
    gate = jnp.dot(b, w["w_gate"], preferred_element_type=jnp.float32)
    up = jnp.dot(b, w["w_up"], preferred_element_type=jnp.float32)
    return h + matmul((jax.nn.silu(gate) * up).astype(jnp.bfloat16), w["w_down"])


def stack(weights, h):
    return lax.scan(lambda h, w: (layer(h, w), None), h, weights)[0]


def reference(x, dy, wq, wk, wv, wo, w_gate, w_up, w_down):
    weights = dict(zip(NAMES, (wq, wk, wv, wo, w_gate, w_up, w_down), strict=True))

    def take(so_far, sequence):
        h, by_y = sequence
        _, back = jax.vjp(stack, weights, h)
        by_weights, by_h = back(by_y)
        return jax.tree.map(lambda total, term: total + term.astype(jnp.float32), so_far, by_weights), by_h

    none_yet = {name: jnp.zeros(w.shape, jnp.float32) for name, w in weights.items()}
    by_weights, by_x = lax.scan(take, none_yet, (x, dy))
    return (by_x, *(by_weights[name].astype(jnp.bfloat16) for name in NAMES))
```

```python
import functools

import jax
import jax.numpy as jnp
from jax import lax
from jax.experimental import pallas as pl
from jax.experimental.pallas import tpu as pltpu
from jax.sharding import PartitionSpec as P

HEAD = 128
THETA = 10000
EPS = 1e-6
LOG2E = 1.4426950408889634
HIDDEN = -2e30
VMEM = 62 * 2**20
FF = 512
COLS = 256
BQ = 256
INTERPRET = False

bf16, f32 = jnp.bfloat16, jnp.float32


def dot(a, b, ca=1, cb=0):
    return lax.dot_general(a, b, (((ca,), (cb,)), ((), ())), preferred_element_type=f32)


def call(body, name, grid, ins, outs, shapes, scratch=(), flops=0, args=(), alias=None):
    size = sum(a.size * a.dtype.itemsize for a in args)
    return pl.pallas_call(
        body,
        name=name,
        grid=grid,
        in_specs=ins,
        out_specs=outs,
        out_shape=shapes,
        scratch_shapes=list(scratch),
        input_output_aliases=alias or {},
        compiler_params=pltpu.CompilerParams(dimension_semantics=("arbitrary",) * len(grid), vmem_limit_bytes=VMEM),
        cost_estimate=pl.CostEstimate(flops=flops, bytes_accessed=size, transcendentals=0),
        interpret=INTERPRET,
    )(*args)


def still(shape):
    return pl.BlockSpec(shape, lambda *_: (0,) * len(shape), pipeline_mode=pl.Buffered(1))


def columns(shape, first=0):
    return pl.BlockSpec(shape, lambda j: (0, first + j))


def struct(shape, dtype=bf16):
    return jax.ShapeDtypeStruct(shape, dtype)


def scale_of(wide):
    return lax.rsqrt(jnp.mean(wide * wide, -1, keepdims=True) + EPS)


def normed(h):
    wide = h.astype(f32)
    return (wide * scale_of(wide)).astype(bf16)


def norm_back(h, by_a, by_h):
    wide = h.astype(f32)
    scale = scale_of(wide)
    by_a = by_a.astype(bf16).astype(f32)
    mine = scale * by_a - wide * (scale * scale * scale * jnp.mean(by_a * wide, -1, keepdims=True))
    return (by_h.astype(f32) + mine.astype(bf16).astype(f32)).astype(bf16)


def qkv_body(h_ref, w_ref, cos_ref, sin_ref, out_ref, a_s):
    j = pl.program_id(0)

    @pl.when(j == 0)
    def _():
        a_s[...] = normed(h_ref[...])

    def piece(at, turn):
        got = dot(a_s[...], w_ref[:, at : at + COLS]).astype(bf16)
        for n in range(0, COLS, HEAD):
            t = got[:, n : n + HEAD]
            if turn:
                t = t.astype(f32)
                t = (t * cos_ref[...] + pltpu.roll(t, HEAD // 2, 1) * sin_ref[...]).astype(bf16)
            out_ref[:, at + n : at + n + HEAD] = t

    @pl.when(j < 2)
    def _():
        for at in range(0, w_ref.shape[1], COLS):
            piece(at, True)

    @pl.when(j == 2)
    def _():
        for at in range(0, w_ref.shape[1], COLS):
            piece(at, False)


def qkv_of(h, wa, cos, sin):
    t, d = h.shape
    q = wa.shape[1] // 4
    return call(qkv_body, "qkv", (3,), [still((t, d)), columns((d, q)), still((t, HEAD)), still((t, HEAD))], columns((t, q)),
                struct((t, 3 * q)), [pltpu.VMEM((t, d), bf16)], 2 * t * d * 3 * q, (h, wa, cos, sin))


def attend_body(q_ref, k_ref, v_ref, o_ref, lse_ref, *, scale):
    t, heads = q_ref.shape[0], q_ref.shape[1] // HEAD
    e = scale * LOG2E
    seen = lax.broadcasted_iota(jnp.int32, (BQ, BQ), 1) >= lax.broadcasted_iota(jnp.int32, (BQ, BQ), 0)
    for n in range(heads):
        lanes = slice(n * HEAD, (n + 1) * HEAD)
        for at in range(0, t, BQ):
            end = at + BQ
            s = dot(k_ref[:end, lanes], q_ref[at:end, lanes], 1, 1)
            low = jnp.where(seen, s[at:], HIDDEN)
            s = low if at == 0 else jnp.concatenate([s[:at], low], axis=0)
            top = s.max(axis=0, keepdims=True)
            p = jnp.exp2((s - top) * e)
            total = p.sum(axis=0, keepdims=True)
            out = dot(v_ref[:end, lanes].T, p.astype(bf16), 1, 0)
            o_ref[at:end, lanes] = (out * (1 / total)).T.astype(bf16)
            lse_ref[0, n : n + 1, at:end] = top * scale + jnp.log(total)


def attend(qkv):
    t, q = qkv.shape[0], qkv.shape[1] // 3
    w = 2 * HEAD
    blocks = q // w
    return call(functools.partial(attend_body, scale=HEAD**-0.5), "attend", (blocks,),
                [columns((t, w)), columns((t, w), blocks), columns((t, w), 2 * blocks)],
                [columns((t, w)), pl.BlockSpec((1, 2, t), lambda j: (j, 0, 0))], [struct((t, q)), struct((blocks, 2, t), f32)], (),
                3 * t * t * q, (qkv, qkv, qkv))


def add_body(a_ref, w_ref, h_ref, out_ref):
    out_ref[...] = (h_ref[...].astype(f32) + dot(a_ref[...], w_ref[...]).astype(bf16).astype(f32)).astype(bf16)


def added(name, a, w, h, first=0):
    (t, k), d = a.shape, h.shape[1]
    return call(add_body, name, (d // COLS,), [still((t, k)), columns((k, COLS), first), columns((t, COLS))], columns((t, COLS)), struct((t, d)),
                (), 2 * t * k * d, (a, w, h))


def up_body(h_ref, w_ref, gu_ref, p_ref, b_s):
    @pl.when(pl.program_id(0) == 0)
    def _():
        b_s[...] = normed(h_ref[...])

    for at in range(0, FF, COLS):
        gate = dot(b_s[...], w_ref[:, at : at + COLS])
        up = dot(b_s[...], w_ref[:, FF + at : FF + at + COLS])
        gu_ref[:, at : at + COLS] = gate
        gu_ref[:, FF + at : FF + at + COLS] = up
        p_ref[:, at : at + COLS] = (gate * jax.nn.sigmoid(gate) * up).astype(bf16)


def gate_up(h, wg):
    (t, d), f = h.shape, wg.shape[1] // 2
    return call(up_body, "gate_up", (f // FF,), [still((t, d)), columns((d, 2 * FF))], [columns((t, 2 * FF)), columns((t, FF))],
                [struct((t, 2 * f), f32), struct((t, f))], [pltpu.VMEM((t, d), bf16)], 4 * t * d * f, (h, wg))


def mlp_back_body(dh_ref, h_ref, wd_ref, wg_ref, gu_ref, out_ref, dwd_ref, dwg_ref, bt_s, acc_s):
    i = pl.program_id(0)

    @pl.when(i == 0)
    def _():
        bt_s[...] = normed(h_ref[...]).T
        acc_s[...] = jnp.zeros_like(acc_s)

    for at in range(0, FF, COLS):
        gates, ups = slice(at, at + COLS), slice(FF + at, FF + at + COLS)
        dp = dot(dh_ref[...], wd_ref[gates, :], 1, 1).astype(bf16).astype(f32)
        gate, up = gu_ref[:, gates], gu_ref[:, ups]
        s = jax.nn.sigmoid(gate)
        silu = gate * s
        p = (silu * up).astype(bf16)
        by_up = (dp * silu).astype(bf16)
        by_gate = (dp * up * (s * (1 + gate * (1 - s)))).astype(bf16)
        dwd_ref[gates, :] = dot(p.T, dh_ref[...]).astype(bf16)
        dwg_ref[:, gates] = dot(bt_s[...], by_gate).astype(bf16)
        dwg_ref[:, ups] = dot(bt_s[...], by_up).astype(bf16)
        acc_s[...] += dot(by_gate, wg_ref[:, gates], 1, 1) + dot(by_up, wg_ref[:, ups], 1, 1)

    @pl.when(i == pl.num_programs(0) - 1)
    def _():
        out_ref[...] = norm_back(h_ref[...], acc_s[...], dh_ref[...])


def mlp_back(dh, h, wd, wg, gu):
    (t, d), f = h.shape, wd.shape[0]
    rows = lambda: pl.BlockSpec((FF, d), lambda i: (i, 0))
    return call(mlp_back_body, "mlp_back", (f // FF,),
                [still((t, d)), still((t, d)), rows(), columns((d, 2 * FF)), columns((t, 2 * FF))],
                [still((t, d)), rows(), columns((d, 2 * FF))], [struct((t, d)), struct((f, d)), struct((d, 2 * f))],
                [pltpu.VMEM((d, t), bf16), pltpu.VMEM((t, d), f32)], 12 * t * d * f, (dh, h, wd, wg, gu))


def wo_back_body(dh_ref, w_ref, o_ref, do_ref, dw_ref):
    do_ref[...] = dot(dh_ref[...], w_ref[...], 1, 1).astype(bf16)
    dw_ref[...] = dot(o_ref[...].T, dh_ref[...]).astype(bf16)


def wo_back(dh, wa, o):
    (t, d), q = dh.shape, o.shape[1]
    return call(wo_back_body, "wo_back", (q // COLS,),
                [still((t, d)), pl.BlockSpec((COLS, d), lambda j: (j, 3)), columns((t, COLS))],
                [columns((t, COLS)), pl.BlockSpec((COLS, d), lambda j: (j, 3))], [struct((t, q)), struct((q, 4 * d))], (),
                4 * t * d * q, (dh, wa, o))


def attend_back_body(q_ref, k_ref, v_ref, do_ref, o_ref, lse_ref, cos_ref, sin_ref, out_ref, dq_s, *, scale):
    t, heads = q_ref.shape[0], q_ref.shape[1] // HEAD
    e = scale * LOG2E
    seen = lax.broadcasted_iota(jnp.int32, (BQ, BQ), 1) >= lax.broadcasted_iota(jnp.int32, (BQ, BQ), 0)

    def turned_back(x):
        x = x.astype(bf16).astype(f32)
        return x, pltpu.roll(x, HEAD // 2, 1)

    for n in range(heads):
        lanes = slice(n * HEAD, (n + 1) * HEAD)
        lse = lse_ref[0, n : n + 1, :] * LOG2E
        delta = (do_ref[:, lanes].astype(f32) * o_ref[:, lanes].astype(f32)).T.sum(axis=0, keepdims=True)
        for at in range(0, t, BQ):
            end = at + BQ
            k, v, q, do = k_ref[at:end, lanes], v_ref[at:end, lanes], q_ref[at:, lanes], do_ref[at:, lanes]
            s = dot(k, q, 1, 1)
            p = jnp.exp2(s * e - lse[:, at:])
            low = jnp.where(seen, p[:, :BQ], 0.0)
            p = low if end == t else jnp.concatenate([low, p[:, BQ:]], axis=1)
            ds = (p * (dot(v, do, 1, 1) - delta[:, at:])).astype(bf16)
            out_ref[2, at:end, lanes] = dot(p.astype(bf16), do).astype(bf16)
            x, y = turned_back(dot(ds, q) * scale)
            out_ref[1, at:end, lanes] = (x * cos_ref[at:end, :] - y * sin_ref[at:end, :]).astype(bf16)
            part = dot(k.T, ds)
            if at == 0:
                dq_s[n] = part
            else:
                dq_s[n, :, at:] += part
        x, y = turned_back((dq_s[n] * scale).T)
        out_ref[0, :, lanes] = (x * cos_ref[...] - y * sin_ref[...]).astype(bf16)


def attend_back(qkv, do, o, lse, cos, sin):
    t, q = o.shape
    w = 2 * HEAD
    blocks = q // w
    return call(functools.partial(attend_back_body, scale=HEAD**-0.5), "attend_back", (blocks,),
                [columns((t, w)), columns((t, w), blocks), columns((t, w), 2 * blocks), columns((t, w)), columns((t, w)),
                 pl.BlockSpec((1, 2, t), lambda j: (j, 0, 0)), still((t, HEAD)), still((t, HEAD))],
                pl.BlockSpec((3, t, w), lambda j: (0, 0, j)), struct((3, t, q)), [pltpu.VMEM((2, HEAD, t), f32)], 7 * t * t * q,
                (qkv, qkv, qkv, do, o, lse, cos, sin))


def qkv_back_body(dh_ref, h_ref, dqkv_ref, w_ref, _, out_ref, dw_ref, at_s, acc_s):
    j = pl.program_id(0)

    @pl.when(j == 0)
    def _():
        at_s[...] = normed(h_ref[...]).T
        acc_s[...] = jnp.zeros_like(acc_s)

    d = dqkv_ref[0]
    for at in range(0, d.shape[1], COLS):
        dw_ref[:, at : at + COLS] = dot(at_s[...], d[:, at : at + COLS]).astype(bf16)
    for at in range(0, acc_s.shape[1], COLS):
        acc_s[:, at : at + COLS] += dot(d, w_ref[at : at + COLS, :], 1, 1)

    @pl.when(j == pl.num_programs(0) - 1)
    def _():
        out_ref[...] = norm_back(h_ref[...], acc_s[...], dh_ref[...])


def qkv_back(dh, h, dqkv, wa, dwa):
    (t, d), q = h.shape, wa.shape[1] // 4
    return call(qkv_back_body, "qkv_back", (3,),
                [still((t, d)), still((t, d)), pl.BlockSpec((1, t, q), lambda j: (j, 0, 0)), columns((d, q)), pl.BlockSpec(memory_space=pl.ANY)],
                [still((t, d)), columns((d, q))], [struct((t, d)), struct(dwa.shape)],
                [pltpu.VMEM((d, t), bf16), pltpu.VMEM((t, d), f32)], 4 * t * d * 3 * q, (dh, h, dqkv, wa, dwa), {4: 1})


def layer(h, w, tables):
    wa, wg, wd = w
    qkv = qkv_of(h, wa, *tables)
    o, lse = attend(qkv)
    mid = added("wo", o, wa, h, 3 * wa.shape[1] // 4 // COLS)
    gu, p = gate_up(mid, wg)
    return added("down", p, wd, mid), (h, qkv, o, lse, mid, gu)


def layer_back(by_h, w, kept, tables):
    wa, wg, wd = w
    h, qkv, o, lse, mid, gu = kept
    by_mid, dwd, dwg = mlp_back(by_h, mid, wd, wg, gu)
    do, dwa = wo_back(by_mid, wa, o)
    dqkv = attend_back(qkv, do, o, lse, *tables)
    by_h, dwa = qkv_back(by_mid, h, dqkv, wa, dwa)
    return by_h, (dwa, dwg, dwd)


def tables_of(t):
    half = HEAD // 2
    angle = jnp.arange(t, dtype=f32)[:, None] * THETA ** (-jnp.arange(half, dtype=f32) / half)
    cos, sin = jnp.cos(angle), jnp.sin(angle)
    return jnp.concatenate([cos, cos], -1), jnp.concatenate([-sin, sin], -1)


def padded(rows):
    return -(-rows // 16) * 16


def pack(wq, wk, wv, wo, w_gate, w_up, w_down, n):
    rows = w_down.shape[0]
    more = padded(rows) - rows
    r = w_gate.shape[0]

    def spread(w):
        return jnp.pad(w.reshape(r, n, rows), ((0, 0), (0, 0), (0, more))).reshape(r, -1, FF)

    wg = jnp.stack([spread(w_gate), spread(w_up)], axis=2).reshape(r, -1)
    return jnp.concatenate([wq, wk, wv, wo], axis=1), wg, jnp.pad(w_down, ((0, more), (0, 0)))


def unpack(wa, wg, wd, n, rows):
    r = wa.shape[0]
    both = wg.reshape(r, -1, 2, FF)
    gate, up = (both[:, :, i].reshape(r, n, -1)[:, :, :rows].reshape(r, n * rows) for i in range(2))
    return *jnp.split(wa, 4, axis=1), gate, up, wd[:rows]


def solution(mesh):
    n = mesh.shape["dp"]

    def step(x, dy, *weights):
        layers = weights[0].shape[0]
        rows = weights[6].shape[1]
        tables = tables_of(x.shape[1])
        gathered = []
        for number in range(layers):
            parts = pack(*(w[number] for w in weights), n)
            gathered.append([lax.all_gather(p, "dp", axis=0, tiled=True) for p in parts])
        h, kept = x[0], []
        for number in range(layers):
            h, saved = layer(h, gathered[number], tables)
            kept.append(saved)
        by_h, mine = dy[0], [None] * layers
        for number in reversed(range(layers)):
            by_h, terms = layer_back(by_h, gathered[number], kept[number], tables)
            mine[number] = unpack(*(lax.psum_scatter(w, "dp", scatter_dimension=0, tiled=True) for w in terms), n, rows)
        return (by_h[None], *(jnp.stack([mine[number][i] for number in range(layers)]) for i in range(7)))

    states, cut = P(("rep", "dp"), None, None), P(None, "dp", None)
    return jax.shard_map(
        step,
        mesh=mesh,
        in_specs=(states, states) + (cut,) * 7,
        out_specs=(states,) + (P("rep", "dp", None),) * 7,
        check_vma=False,
    )
```

```python
import functools
import math

import jax
import jax.numpy as jnp
from jax import lax
from jax.experimental import pallas as pl
from jax.experimental.pallas import tpu as pltpu
from jax.sharding import PartitionSpec as P

HEAD = 128
THETA = 10000
EPS = 1e-6
LOG2E = 1.4426950408889634
HIDDEN = -2e30
VMEM = 62 * 2**20
FF = 512
COLS = 256
BQ = 256
INTERPRET = False

bf16, f32 = jnp.bfloat16, jnp.float32


def dot(a, b, ca=1, cb=0):
    return lax.dot_general(a, b, (((ca,), (cb,)), ((), ())), preferred_element_type=f32)


def call(body, name, grid, ins, outs, shapes, scratch=(), flops=0, args=(), alias=None):
    size = sum(a.size * a.dtype.itemsize for a in args)
    return pl.pallas_call(
        body,
        name=name,
        grid=grid,
        in_specs=ins,
        out_specs=outs,
        out_shape=shapes,
        scratch_shapes=list(scratch),
        input_output_aliases=alias or {},
        compiler_params=pltpu.CompilerParams(dimension_semantics=("arbitrary",) * len(grid), vmem_limit_bytes=VMEM),
        cost_estimate=pl.CostEstimate(flops=flops, bytes_accessed=size, transcendentals=0),
        interpret=INTERPRET,
    )(*args)


def still(shape):
    return pl.BlockSpec(shape, lambda *_: (0,) * len(shape), pipeline_mode=pl.Buffered(1))


def columns(shape, first=0):
    return pl.BlockSpec(shape, lambda j: (0, first + j))


def struct(shape, dtype=bf16):
    return jax.ShapeDtypeStruct(shape, dtype)


def scale_of(wide):
    return lax.rsqrt(jnp.mean(wide * wide, -1, keepdims=True) + EPS)


def normed(h):
    wide = h.astype(f32)
    return (wide * scale_of(wide)).astype(bf16)


def norm_back(h, by_a, by_h):
    wide = h.astype(f32)
    scale = scale_of(wide)
    by_a = by_a.astype(bf16).astype(f32)
    mine = scale * by_a - wide * (scale * scale * scale * jnp.mean(by_a * wide, -1, keepdims=True))
    return (by_h.astype(f32) + mine.astype(bf16).astype(f32)).astype(bf16)


def qkv_body(h_ref, w_ref, cos_ref, sin_ref, out_ref, a_s):
    j = pl.program_id(0)

    @pl.when(j == 0)
    def _():
        a_s[...] = normed(h_ref[...])

    def piece(at, turn):
        got = dot(a_s[...], w_ref[:, at : at + COLS]).astype(bf16)
        for n in range(0, COLS, HEAD):
            t = got[:, n : n + HEAD]
            if turn:
                t = t.astype(f32)
                t = (t * cos_ref[...] + pltpu.roll(t, HEAD // 2, 1) * sin_ref[...]).astype(bf16)
            out_ref[:, at + n : at + n + HEAD] = t

    @pl.when(j < 2)
    def _():
        for at in range(0, w_ref.shape[1], COLS):
            piece(at, True)

    @pl.when(j == 2)
    def _():
        for at in range(0, w_ref.shape[1], COLS):
            piece(at, False)


def qkv_of(h, wa, cos, sin):
    t, d = h.shape
    q = wa.shape[1] // 4
    return call(qkv_body, "qkv", (3,), [still((t, d)), columns((d, q)), still((t, HEAD)), still((t, HEAD))], columns((t, q)),
                struct((t, 3 * q)), [pltpu.VMEM((t, d), bf16)], 2 * t * d * 3 * q, (h, wa, cos, sin))


def attend_body(q_ref, k_ref, v_ref, o_ref, lse_ref, *, scale):
    t, heads = q_ref.shape[0], q_ref.shape[1] // HEAD
    e = scale * LOG2E
    seen = lax.broadcasted_iota(jnp.int32, (BQ, BQ), 1) >= lax.broadcasted_iota(jnp.int32, (BQ, BQ), 0)
    for n in range(heads):
        lanes = slice(n * HEAD, (n + 1) * HEAD)
        for at in range(0, t, BQ):
            end = at + BQ
            s = dot(k_ref[:end, lanes], q_ref[at:end, lanes], 1, 1)
            low = jnp.where(seen, s[at:], HIDDEN)
            s = low if at == 0 else jnp.concatenate([s[:at], low], axis=0)
            top = s.max(axis=0, keepdims=True)
            p = jnp.exp2((s - top) * e)
            total = p.sum(axis=0, keepdims=True)
            out = dot(v_ref[:end, lanes].T, p.astype(bf16), 1, 0)
            o_ref[at:end, lanes] = (out * (1 / total)).T.astype(bf16)
            lse_ref[0, n : n + 1, at:end] = top * scale + jnp.log(total)


def attend(qkv):
    t, q = qkv.shape[0], qkv.shape[1] // 3
    w = 2 * HEAD
    blocks = q // w
    return call(functools.partial(attend_body, scale=HEAD**-0.5), "attend", (blocks,),
                [columns((t, w)), columns((t, w), blocks), columns((t, w), 2 * blocks)],
                [columns((t, w)), pl.BlockSpec((1, 2, t), lambda j: (j, 0, 0))], [struct((t, q)), struct((blocks, 2, t), f32)], (),
                3 * t * t * q, (qkv, qkv, qkv))


def add_body(a_ref, w_ref, h_ref, out_ref, acc_s):
    j = pl.program_id(0)
    part = dot(a_ref[...], w_ref[...])

    @pl.when(j == 0)
    def _():
        acc_s[...] = part

    @pl.when(j > 0)
    def _():
        acc_s[...] += part

    @pl.when(j == pl.num_programs(0) - 1)
    def _():
        out_ref[...] = (h_ref[...].astype(f32) + acc_s[...].astype(bf16).astype(f32)).astype(bf16)


def added(name, a, w, h, rows, at=0):
    (t, k), d = a.shape, h.shape[1]
    return call(add_body, name, (k // rows,), [columns((t, rows)), pl.BlockSpec((rows, d), lambda j: (j, at)), still((t, d))], still((t, d)),
                struct((t, d)), [pltpu.VMEM((t, d), f32)], 2 * t * k * d, (a, w, h))


def up_body(h_ref, w_ref, gu_ref, p_ref, b_s):
    @pl.when(pl.program_id(0) == 0)
    def _():
        b_s[...] = normed(h_ref[...])

    for at in range(0, FF, COLS):
        got = dot(b_s[...], w_ref[:, 2 * at : 2 * at + 2 * COLS])
        gate, up = got[:, :COLS], got[:, COLS:]
        gu_ref[:, 2 * at : 2 * at + 2 * COLS] = got
        p_ref[:, at : at + COLS] = (gate * jax.nn.sigmoid(gate) * up).astype(bf16)


def gate_up(h, wg):
    (t, d), f = h.shape, wg.shape[1] // 2
    return call(up_body, "gate_up", (f // FF,), [still((t, d)), columns((d, 2 * FF))], [columns((t, 2 * FF)), columns((t, FF))],
                [struct((t, 2 * f), f32), struct((t, f))], [pltpu.VMEM((t, d), bf16)], 4 * t * d * f, (h, wg))


def place(side):
    me = lax.axis_index("dp")
    core, chip = me % 2, me // 2
    return core, chip // side, chip % side


def device(core, x, y, side):
    return {"dp": (((x + side) % side) * side + (y + side) % side) * 2 + core}


def remote(src, dst, send, recv, to):
    return pltpu.make_async_remote_copy(src_ref=src, dst_ref=dst, send_sem=send, recv_sem=recv, device_id=to, device_id_type=pl.DeviceIdType.MESH)


class Ring:
    def __init__(self, kind, axis, src, dim, first, width, came=None):
        self.kind, self.axis, self.src, self.dim, self.first, self.width, self.came = kind, axis, src, dim, first, width, came
        self.lead = src.shape[1 - dim]
        self.rows = src.shape[3]

    def given(self):
        return [self.src] + ([self.came] if self.kind == "mid" else [])

    def results(self):
        one = struct((self.lead, 2, self.rows, self.width))
        return [one] * {"raw": 2, "mid": 1, "ring": 3}[self.kind]

    def scratch(self):
        dma = pltpu.SemaphoreType.DMA
        got = [] if self.kind == "mid" else [dma((4,)), dma((4,))]
        if self.kind != "raw":
            got += [dma((2,)), dma((2,)), dma((3,)), pltpu.VMEM((2, self.lead, 2, self.rows, self.width), bf16)]
        return got

    def bind(self, given, results, scratch, side):
        core, x, y = place(side)
        self.side, self.at = side, x if self.axis == "x" else y
        step = lambda by: device(core, x + by, y, side) if self.axis == "x" else device(core, x, y + by, side)
        self.right, self.left = step(1), step(-1)
        self.src_ref = given[0]
        if self.kind == "mid":
            self.came_ref, (self.sums_ref,) = given[1], results
        elif self.kind == "raw":
            self.came_ref, self.raw_ref = results
        else:
            self.came_ref, self.raw_ref, self.sums_ref = results
        scratch = list(scratch)
        if self.kind != "mid":
            self.send, self.recv = scratch[:2]
            scratch = scratch[2:]
        if self.kind != "raw":
            self.send2, self.recv2, self.local, self.buf = scratch

    def part(self, by, half):
        k = (self.at + by + self.side) % self.side
        lanes = slice(self.first, self.first + self.width)
        return self.src_ref.at[k, :, half, :, lanes] if self.dim == 0 else self.src_ref.at[:, k, half, :, lanes]

    def raws(self):
        s, r = self.send, self.recv
        return [remote(self.part(2, 0), self.came_ref.at[:, 0], s.at[0], r.at[0], self.right),
                remote(self.part(2, 1), self.came_ref.at[:, 1], s.at[1], r.at[1], self.left),
                remote(self.part(1, 1), self.raw_ref.at[:, 1], s.at[2], r.at[2], self.right),
                remote(self.part(-1, 0), self.raw_ref.at[:, 0], s.at[3], r.at[3], self.left)]

    def mids(self):
        s, r = self.send2, self.recv2
        return [remote(self.buf.at[0, :, 0], self.sums_ref.at[:, 0], s.at[0], r.at[0], self.right),
                remote(self.buf.at[0, :, 1], self.sums_ref.at[:, 1], s.at[1], r.at[1], self.left)]

    def loads(self):
        return [pltpu.make_async_copy(self.part(1, 0), self.buf.at[0, :, 0], self.local.at[0]),
                pltpu.make_async_copy(self.part(-1, 1), self.buf.at[0, :, 1], self.local.at[1]),
                pltpu.make_async_copy(self.came_ref, self.buf.at[1], self.local.at[2])]

    def start(self):
        if self.kind != "mid":
            for copy in self.raws():
                copy.start()

    def load(self):
        if self.kind != "raw":
            if self.kind == "ring":
                for copy in self.raws()[:2]:
                    copy.wait_recv()
            for copy in self.loads():
                copy.start()

    def turn(self):
        if self.kind != "raw":
            for copy in self.loads():
                copy.wait()
            for i in range(self.lead):
                for half in range(2):
                    self.buf[0, i, half] = (self.buf[0, i, half].astype(f32) + self.buf[1, i, half].astype(f32)).astype(bf16)
            for copy in self.mids():
                copy.start()

    def finish(self):
        if self.kind != "mid":
            for n, copy in enumerate(self.raws()):
                copy.wait_send()
                if self.kind == "raw" or n >= 2:
                    copy.wait_recv()
        if self.kind != "raw":
            for copy in self.mids():
                copy.wait()


def barrier(side, rings, partner):
    core, x, y = place(side)
    near = [device(core, x + 1, y, side), device(core, x - 1, y, side), device(core, x, y + 1, side), device(core, x, y - 1, side)] if rings else []
    if partner:
        near.append(device(1 - core, x, y, side))
    sem = pltpu.get_barrier_semaphore()
    for to in near:
        pl.semaphore_signal(sem, inc=1, device_id=to, device_id_type=pl.DeviceIdType.MESH)
    pl.semaphore_wait(sem, len(near))


IDS = iter(range(1, 1000))


def host(body, name, side, steps, ins, outs, shapes, scratch=(), flops=0, args=(), rings=(), turn_at=0, partner=True):
    given = [x for r in rings for x in r.given()]
    results = [x for r in rings for x in r.results()]
    ends = [r.scratch() for r in rings]
    sizes = [len(ins), len(given), len(outs), len(results), len(scratch)]
    hbm = pl.BlockSpec(memory_space=pl.ANY)
    talks = bool(rings) or partner

    def kernel(*refs):
        groups, at = [], 0
        for n in sizes:
            groups.append(refs[at : at + n])
            at += n
        own_in, ring_in, own_out, ring_out, own_scratch = groups
        for r, scr in zip(rings, ends):
            n, m = len(r.given()), len(r.results())
            r.bind(ring_in[:n], ring_out[:m], refs[at : at + len(scr)], side)
            ring_in, ring_out, at = ring_in[n:], ring_out[m:], at + len(scr)
        i = pl.program_id(0)

        @pl.when(i == 0)
        def _():
            if talks:
                barrier(side, bool(rings), partner)
            for r in rings:
                r.start()

        if rings:

            @pl.when(i == turn_at)
            def _():
                for r in rings:
                    r.load()
                for r in rings:
                    r.turn()

        body(*own_in, *own_out, *own_scratch)

        if rings:

            @pl.when(i == steps - 1)
            def _():
                for r in rings:
                    r.finish()

    size = sum(a.size * a.dtype.itemsize for a in args)
    extra = dict(collective_id=next(IDS), has_side_effects=True) if talks else {}
    got = pl.pallas_call(
        kernel,
        name=name,
        grid=(steps,),
        in_specs=[*ins, *[hbm] * len(given)],
        out_specs=[*outs, *[hbm] * len(results)],
        out_shape=[*shapes, *results],
        scratch_shapes=[*scratch, *[s for e in ends for s in e]],
        compiler_params=pltpu.CompilerParams(dimension_semantics=("arbitrary",), vmem_limit_bytes=VMEM, **extra),
        cost_estimate=pl.CostEstimate(flops=flops, bytes_accessed=size, transcendentals=0),
        interpret=INTERPRET,
    )(*args, *given)
    mine, rest = got[: len(outs)], got[len(outs) :]
    per_ring = []
    for r in rings:
        n = len(r.results())
        per_ring.append(rest[:n])
        rest = rest[n:]
    return mine, per_ring


def first_rings(kind, u, came=(None, None)):
    w = u.shape[4] // 2
    return [Ring(kind, "x", u, 0, 0, w, came[0]), Ring(kind, "y", u, 1, w, w, came[1])]


def second_rings(kind, v):
    return [Ring(kind, "y", v[0], 0, 0, v[0].shape[4]), Ring(kind, "x", v[1], 0, 0, v[1].shape[4])]


def ended(ring, raw, sums, at):
    own = lax.dynamic_index_in_dim(ring.src, at, ring.dim, keepdims=False)[..., ring.first : ring.first + ring.width]
    return (own.astype(f32) + raw.astype(f32) + sums.astype(f32)).astype(bf16)


def mlp_back_body(dh_ref, h_ref, wd_ref, wg_ref, gu_ref, out_ref, ug_ref, ud_ref, bt_s, acc_s, send_g, send_d, got_g, got_d, send_sem, recv_sem, *, side):
    i = pl.program_id(0)
    half = pl.num_programs(0) // 2
    core, x, y = place(side)
    other = device(1 - core, x, y, side)

    def copies(n, slot):
        return [remote(send_g.at[slot], got_g.at[n], send_sem.at[n, 0], recv_sem.at[n, 0], other),
                remote(send_d.at[slot], got_d.at[n], send_sem.at[n, 1], recv_sem.at[n, 1], other)]

    @pl.when(i == 0)
    def _():
        bt_s[...] = normed(h_ref[...]).T
        acc_s[...] = jnp.zeros_like(acc_s)

    dp = dot(dh_ref[...], wd_ref[...], 1, 1).astype(bf16).astype(f32)
    gate, up = gu_ref[:, :COLS], gu_ref[:, COLS:]
    s = jax.nn.sigmoid(gate)
    silu = gate * s
    p = (silu * up).astype(bf16)
    by = jnp.concatenate([(dp * up * (s * (1 + gate * (1 - s)))).astype(bf16), (dp * silu).astype(bf16)], axis=1)
    acc_s[...] += dot(by, wg_ref[...], 1, 1)
    dwd = dot(p.T, dh_ref[...])
    dwg = dot(bt_s[...], by)

    @pl.when(i < half)
    def _():
        @pl.when(i >= 2)
        def _():
            for copy in copies(i - 2, i % 2):
                copy.wait_send()

        send_g[i % 2] = dwg.astype(bf16)
        send_d[i % 2] = dwd.astype(bf16)
        for copy in copies(i, i % 2):
            copy.start()

    @pl.when(i >= half)
    def _():
        @pl.when(i < half + 2)
        def _():
            for copy in copies(i - 2, i % 2):
                copy.wait_send()

        for copy in copies(i - half, 0):
            copy.wait_recv()
        ug_ref[...] = (dwg + got_g[i - half].astype(f32)).astype(bf16)
        ud_ref[...] = (dwd + got_d[i - half].astype(f32)).astype(bf16)

    @pl.when(i == pl.num_programs(0) - 1)
    def _():
        out_ref[...] = norm_back(h_ref[...], acc_s[...], dh_ref[...])


def mlp_back(dh, h, wd, wg, gu, side, rings):
    (t, d), f = h.shape, wd.shape[0]
    steps = f // COLS
    half = steps // 2

    def tile(i):
        core = lax.axis_index("dp") % 2
        return jnp.where(i < half, (1 - core) * half + i, core * half + i - half)

    wide = lambda rows: pl.BlockSpec((rows, 2 * COLS), lambda i: (0, tile(i)))
    dma = pltpu.SemaphoreType.DMA
    (out, ug, ud), per_ring = host(
        functools.partial(mlp_back_body, side=side), "mlp_back", side, steps,
        [still((t, d)), still((t, d)), pl.BlockSpec((COLS, d), lambda i: (tile(i), 0)), wide(d), wide(t)],
        [still((t, d)), pl.BlockSpec((d, 2 * COLS), lambda i: (0, jnp.maximum(i - half, 0))), pl.BlockSpec((COLS, d), lambda i: (jnp.maximum(i - half, 0), 0))],
        [struct((t, d)), struct((d, f)), struct((f // 2, d))],
        [pltpu.VMEM((d, t), bf16), pltpu.VMEM((t, d), f32), pltpu.VMEM((2, d, 2 * COLS), bf16), pltpu.VMEM((2, COLS, d), bf16),
         pltpu.VMEM((half, d, 2 * COLS), bf16), pltpu.VMEM((half, COLS, d), bf16), dma((half, 2)), dma((half, 2))],
        12 * t * d * f, (dh, h, wd, wg, gu), rings, turn_at=6)
    return out, cut(ug, side), cut(ud, side), per_ring


def cut(u, side):
    return u.reshape(side, side, 2, -1, u.shape[1])


def attend_back_body(dh_ref, w_ref, o_ref, q_ref, k_ref, v_ref, lse_ref, cos_ref, sin_ref, out_ref, u_ref, do_s, dq_s, keep_s, got_s, send_sem, recv_sem,
                     *, scale, side):
    i = pl.program_id(0)
    pairs = pl.num_programs(0) // 2
    core, x, y = place(side)
    other = device(1 - core, x, y, side)
    copy = lambda n: remote(keep_s.at[n], got_s.at[n], send_sem.at[n], recv_sem.at[n], other)

    @pl.when(i < pairs)
    def _():
        do_s[i] = dot(dh_ref[...], w_ref[...], 1, 1).astype(bf16)
        keep_s[i] = dot(o_ref[...].T, dh_ref[...]).astype(bf16)

        @pl.when(core == 0)
        def _():
            copy(i).start()

    @pl.when(i >= pairs)
    def _():
        n = i - pairs

        @pl.when(core == 0)
        def _():
            copy(n).wait_send()
            u_ref[...] = jnp.zeros_like(u_ref)

        @pl.when(core == 1)
        def _():
            copy(n).wait_recv()
            u_ref[...] = (keep_s[n].astype(f32) + got_s[n].astype(f32)).astype(bf16)

        heads_back(q_ref, k_ref, v_ref, do_s.at[n], o_ref, lse_ref, cos_ref, sin_ref, out_ref, dq_s, scale)


def heads_back(q_ref, k_ref, v_ref, do_ref, o_ref, lse_ref, cos_ref, sin_ref, out_ref, dq_s, scale):
    t, heads = q_ref.shape[0], q_ref.shape[1] // HEAD
    e = scale * LOG2E
    seen = lax.broadcasted_iota(jnp.int32, (BQ, BQ), 1) >= lax.broadcasted_iota(jnp.int32, (BQ, BQ), 0)

    def turned_back(x):
        x = x.astype(bf16).astype(f32)
        return x, pltpu.roll(x, HEAD // 2, 1)

    for n in range(heads):
        lanes = slice(n * HEAD, (n + 1) * HEAD)
        lse = lse_ref[0, n : n + 1, :] * LOG2E
        delta = (do_ref[:, lanes].astype(f32) * o_ref[:, lanes].astype(f32)).T.sum(axis=0, keepdims=True)
        for at in range(0, t, BQ):
            end = at + BQ
            k, v, q, do = k_ref[at:end, lanes], v_ref[at:end, lanes], q_ref[at:, lanes], do_ref[at:, lanes]
            s = dot(k, q, 1, 1)
            p = jnp.exp2(s * e - lse[:, at:])
            low = jnp.where(seen, p[:, :BQ], 0.0)
            p = low if end == t else jnp.concatenate([low, p[:, BQ:]], axis=1)
            ds = (p * (dot(v, do, 1, 1) - delta[:, at:])).astype(bf16)
            out_ref[2, at:end, lanes] = dot(p.astype(bf16), do).astype(bf16)
            x, y = turned_back(dot(ds, q) * scale)
            out_ref[1, at:end, lanes] = (x * cos_ref[at:end, :] - y * sin_ref[at:end, :]).astype(bf16)
            part = dot(k.T, ds)
            if at == 0:
                dq_s[n] = part
            else:
                dq_s[n, :, at:] += part
        x, y = turned_back((dq_s[n] * scale).T)
        out_ref[0, :, lanes] = (x * cos_ref[...] - y * sin_ref[...]).astype(bf16)


def attend_back(dh, wa, qkv, o, lse, cos, sin, side, rings):
    (t, d), q = dh.shape, o.shape[1]
    w = 2 * HEAD
    pairs = q // w
    late = lambda j: jnp.maximum(j - pairs, 0)
    head = lambda first: pl.BlockSpec((t, w), lambda j: (0, first + late(j)))
    dma = pltpu.SemaphoreType.DMA
    return host(
        functools.partial(attend_back_body, scale=HEAD**-0.5, side=side), "attend_back", side, 2 * pairs,
        [still((t, d)), pl.BlockSpec((w, d), lambda j: (jnp.minimum(j, pairs - 1), 3)), pl.BlockSpec((t, w), lambda j: (0, j % pairs)),
         head(0), head(pairs), head(2 * pairs), pl.BlockSpec((1, 2, t), lambda j: (late(j), 0, 0)), still((t, HEAD)), still((t, HEAD))],
        [pl.BlockSpec((3, t, w), lambda j: (0, 0, late(j))), pl.BlockSpec((w, d), lambda j: (late(j), 0))],
        [struct((3, t, q)), struct((q, d))],
        [pltpu.VMEM((pairs, t, w), bf16), pltpu.VMEM((2, HEAD, t), f32), pltpu.VMEM((pairs, w, d), bf16), pltpu.VMEM((pairs, w, d), bf16),
         dma((pairs,)), dma((pairs,))],
        4 * t * d * q + 7 * t * t * q, (dh, wa, o, qkv, qkv, qkv, lse, cos, sin), rings)


def qkv_back_body(dh_ref, h_ref, d_ref, w_ref, uo_ref, out_ref, u_ref, at_s, acc_s, send_s, got_s, send_sem, recv_sem, *, side):
    s = pl.program_id(0)
    rows = w_ref.shape[0]
    per = at_s.shape[0] // rows
    m, r = s // per, s % per
    core, x, y = place(side)
    other = device(1 - core, x, y, side)
    sends = jnp.where(core == 0, per, 2 * per)
    copy = lambda n, slot: remote(send_s.at[slot], got_s.at[n + (1 - core) * per], send_sem.at[n], recv_sem.at[n + (1 - core) * per], other)

    @pl.when(s == 0)
    def _():
        at_s[...] = normed(h_ref[...]).T

    lanes = pl.ds(pl.multiple_of(r * rows, rows), rows)
    part = dot(d_ref[0], w_ref[...], 1, 1)

    @pl.when(m == 0)
    def _():
        acc_s[:, lanes] = part

    @pl.when(m > 0)
    def _():
        acc_s[:, lanes] += part

    tile = dot(at_s[lanes, :], d_ref[0])

    @pl.when(s < sends)
    def _():
        @pl.when(s >= 2)
        def _():
            copy(s - 2, s % 2).wait_send()

        send_s[s % 2] = tile.astype(bf16)
        copy(s, s % 2).start()

    @pl.when(s >= sends)
    def _():
        @pl.when(s < sends + 2)
        def _():
            copy(s - 2, s % 2).wait_send()

    @pl.when((m == 1) & (core == 1))
    def _():
        u_ref[...] = uo_ref[...]

    @pl.when((m == 2) | ((m == 1) & (core == 0)))
    def _():
        n = s - per
        pltpu.make_async_copy(got_s.at[n], got_s.at[n], recv_sem.at[n]).wait()
        u_ref[...] = (tile + got_s[n].astype(f32)).astype(bf16)

    @pl.when(s == pl.num_programs(0) - 1)
    def _():
        out_ref[...] = norm_back(h_ref[...], acc_s[...], dh_ref[...])


def qkv_back(dh, h, dqkv, wa, uo, side, rings):
    (t, d), q = h.shape, wa.shape[1] // 4
    rows = 2 * HEAD
    per = d // rows
    matrix = lambda s: (s // per + 2 * (1 - lax.axis_index("dp") % 2)) % 3
    dma = pltpu.SemaphoreType.DMA
    (out, u), per_ring = host(
        functools.partial(qkv_back_body, side=side), "qkv_back", side, 3 * per,
        [still((t, d)), still((t, d)), pl.BlockSpec((1, t, q), lambda s: (matrix(s), 0, 0)), pl.BlockSpec((rows, q), lambda s: (s % per, matrix(s))),
         pl.BlockSpec((rows, q), lambda s: (jnp.clip(s - per, 0, per - 1), 0))],
        [still((t, d)), pl.BlockSpec((rows, q), lambda s: (jnp.where(s < per, 0, s % per), jnp.maximum(s // per - 1, 0)))],
        [struct((t, d)), struct((d, 2 * q))],
        [pltpu.VMEM((d, t), bf16), pltpu.VMEM((t, d), f32), pltpu.VMEM((2, rows, q), bf16), pltpu.VMEM((2 * per, rows, q), bf16), dma((2 * per,)), dma((2 * per,))],
        4 * t * d * 3 * q, (dh, h, dqkv, wa, uo), rings)
    return out, cut(u, side), per_ring


def idle_body(out_ref):
    out_ref[...] = jnp.zeros_like(out_ref)


def carry(name, side, rings):
    return host(idle_body, name, side, 1, [], [pl.BlockSpec((8, 128), lambda i: (0, 0))], [struct((8, 128), f32)], rings=rings, partner=False)[1]


def layer(h, w, tables):
    wa, wg, wd = w
    qkv = qkv_of(h, wa, *tables)
    o, lse = attend(qkv)
    mid = added("wo", o, wa, h, COLS, 3)
    gu, p = gate_up(mid, wg)
    return added("down", p, wd, mid, FF), (h, qkv, o, lse, mid, gu)


def tables_of(t):
    half = HEAD // 2
    angle = jnp.arange(t, dtype=f32)[:, None] * THETA ** (-jnp.arange(half, dtype=f32) / half)
    cos, sin = jnp.cos(angle), jnp.sin(angle)
    return jnp.concatenate([cos, cos], -1), jnp.concatenate([-sin, sin], -1)


def padded(rows):
    return -(-rows // 16) * 16


def pack(wq, wk, wv, wo, w_gate, w_up, w_down, n):
    rows = w_down.shape[0]
    more = padded(rows) - rows
    r = w_gate.shape[0]

    def spread(w):
        w = w.reshape(r, n // 2, 2, rows).swapaxes(1, 2)
        return jnp.pad(w, ((0, 0), (0, 0), (0, 0), (0, more))).reshape(r, -1, COLS)

    wg = jnp.stack([spread(w_gate), spread(w_up)], axis=2).reshape(r, -1)
    return jnp.concatenate([wq, wk, wv, wo], axis=1), wg, jnp.pad(w_down, ((0, more), (0, 0)))


def unpack(wq, wk, wv, wo, wg, wd, n, rows):
    r = wg.shape[0]
    both = wg.reshape(r, -1, 2, COLS)
    gate, up = (both[:, :, i].reshape(r, 2, n // 2, -1)[..., :rows].swapaxes(1, 2).reshape(r, n * rows) for i in range(2))
    return wq, wk, wv, wo, gate, up, wd[:rows]


def solution(mesh):
    n = mesh.shape["dp"]
    side = math.isqrt(n // 2)

    def step(x, dy, *weights):
        global IDS
        IDS = iter(range(1, 1000))
        layers = weights[0].shape[0]
        rows = weights[6].shape[1]
        core, px, py = place(side)
        tables = tables_of(x.shape[1])
        parts = [pack(*(w[number] for w in weights), n) for number in range(layers)]
        order = [((b % (n // 2)) * 2 + b // (n // 2), b) for b in range(n)]
        downs = lax.ppermute(jnp.stack([p[2] for p in parts]), "dp", order)
        gathered = [[lax.all_gather(p, "dp", axis=0, tiled=True) for p in (*parts[number][:2], downs[number])] for number in range(layers)]
        h, kept = x[0], []
        for number in range(layers):
            h, saved = layer(h, gathered[number], tables)
            kept.append(saved)

        def close(rings, got, axes):
            return [ended(r, raw, sums, px if axis == "x" else py)[:, None] for r, (_, raw, sums), axis in zip(rings, got, axes)]

        def whole(v):
            return jnp.concatenate([part[0, 0] for part in v], axis=-1)

        def swapped(z):
            mine = lax.dynamic_index_in_dim(z, core, 0, keepdims=False)
            got = lax.ppermute(lax.dynamic_index_in_dim(z, 1 - core, 0, keepdims=False), "dp", [(b, b ^ 1) for b in range(n)])
            return jnp.where(core == 0, mine, got), jnp.where(core == 0, got, mine)

        by_h = dy[0]
        sums = [None] * layers
        waiting = None
        first = ("x", "y")
        second = ("y", "x")
        seconds = None
        results = [[None] * 3 for _ in range(layers)]
        above = None
        for number in reversed(range(layers)):
            wa, wg, wd = gathered[number]
            hin, qkv, o, lse, mid, gu = kept[number]
            rings = []
            if seconds is not None:
                tail_g, tail_d, ring_a = second_rings("ring", seconds[0]), second_rings("ring", seconds[1]), first_rings("ring", waiting)
                rings = tail_g + tail_d + ring_a
            by_mid, ug, ud, got = mlp_back(by_h, mid, wd, wg, gu, side, rings)
            above_a = None
            if seconds is not None:
                results[number + 1][1] = whole(close(tail_g, got[:2], second))
                results[number + 1][2] = whole(close(tail_d, got[2:4], second))
                above_a = close(ring_a, got[4:], first)
            raw_g, raw_d = first_rings("raw", ug), first_rings("raw", ud)
            (dqkv, uo), got_raw = attend_back(by_mid, wa, qkv, o, lse, *tables, side, raw_g + raw_d)
            came = [g[0] for g in got_raw]
            mid_g, mid_d = first_rings("mid", ug, came[:2]), first_rings("mid", ud, came[2:])
            rings = mid_g + mid_d
            if above_a is not None:
                tail_a = second_rings("ring", above_a)
                rings = rings + tail_a
            by_h, ua, got = qkv_back(by_mid, hin, dqkv, wa, uo, side, rings)
            if above_a is not None:
                results[number + 1][0] = whole(close(tail_a, got[4:], second))
            both = [(None, got_raw[k][1], got[k][0]) for k in range(4)]
            seconds = close(mid_g, both[:2], first), close(mid_d, both[2:], first)
            waiting = ua
        tail_g, tail_d, ring_a = second_rings("ring", seconds[0]), second_rings("ring", seconds[1]), first_rings("ring", waiting)
        got = carry("tail_1", side, tail_g + tail_d + ring_a)
        results[0][1] = whole(close(tail_g, got[:2], second))
        results[0][2] = whole(close(tail_d, got[2:4], second))
        tail_a = second_rings("ring", close(ring_a, got[4:], first))
        got = carry("tail_2", side, tail_a)
        results[0][0] = whole(close(tail_a, got, second))
        mine = []
        for number in range(layers):
            za, zg, zd = results[number]
            (wq, wk), (wo, wv) = (jnp.split(s, 2, axis=-1) for s in swapped(za))
            mine.append(unpack(wq, wk, wv, wo, jnp.concatenate(swapped(zg), axis=-1), zd.reshape(-1, zd.shape[-1]), n, rows))
        return (by_h[None], *(jnp.stack([mine[number][i] for number in range(layers)]) for i in range(7)))

    states, cut_rows = P(("rep", "dp"), None, None), P(None, "dp", None)
    return jax.shard_map(
        step,
        mesh=mesh,
        in_specs=(states, states) + (cut_rows,) * 7,
        out_specs=(states,) + (P("rep", "dp", None),) * 7,
        check_vma=False,
    )
```

```python
import functools
import math

import jax
import jax.numpy as jnp
from jax import lax
from jax.experimental import pallas as pl
from jax.experimental.pallas import tpu as pltpu
from jax.sharding import PartitionSpec as P

HEAD = 128
THETA = 10000
EPS = 1e-6
LOG2E = 1.4426950408889634
HIDDEN = -2e30
VMEM = 62 * 2**20
COLS = 2 * HEAD
BQ = 256
HBM = pl.BlockSpec(memory_space=pl.ANY)
NONE, FIRST, SECOND, THIRD = None, 0, 1, 2

bf16, f32 = jnp.bfloat16, jnp.float32
dma = pltpu.SemaphoreType.DMA


def dot(a, b, ca=1, cb=0):
    return lax.dot_general(a, b, (((ca,), (cb,)), ((), ())), preferred_element_type=f32)


def dot_t(a, b):
    return dot(a, b, SECOND, SECOND)


def still(shape):
    return pl.BlockSpec(shape, lambda *_: (0,) * len(shape), pipeline_mode=pl.Buffered(SECOND))


def block(shape, where):
    return pl.BlockSpec(shape, where)


def struct(shape, dtype=bf16):
    return jax.ShapeDtypeStruct(shape, dtype)


def scale_of(wide):
    return lax.rsqrt(jnp.mean(wide * wide, -1, keepdims=True) + EPS)


def normed(h):
    wide = h.astype(f32)
    return (wide * scale_of(wide)).astype(bf16)


def norm_back(h, by_a, by_h):
    wide = h.astype(f32)
    scale = scale_of(wide)
    by_a = by_a.astype(bf16).astype(f32)
    mine = scale * by_a - wide * (scale * scale * scale * jnp.mean(by_a * wide, -1, keepdims=True))
    return (by_h.astype(f32) + mine.astype(bf16).astype(f32)).astype(bf16)


def plus(h, part):
    return (h.astype(f32) + part.astype(bf16).astype(f32)).astype(bf16)


def place(side):
    me = lax.axis_index("dp")
    core, chip = me % 2, me // 2
    return core, chip // side, chip % side


def number_of(core, x, y, side):
    return (((x + side) % side) * side + (y + side) % side) * 2 + core


def remote(src, dst, send, recv, to):
    return pltpu.make_async_remote_copy(src_ref=src, dst_ref=dst, send_sem=send, recv_sem=recv, device_id={"dp": to}, device_id_type=pl.DeviceIdType.MESH)


class Ring:
    def __init__(self, kind, axis, src, dim, first, width, came=None):
        self.kind, self.axis, self.src, self.dim, self.first, self.width, self.came = kind, axis, src, dim, first, width, came
        self.shape = (src.shape[FIRST], src.shape[3 - dim], 2, src.shape[-2], width)
        self.raw, self.mid = kind != "mid", kind != "raw"

    def given(self):
        return [self.src] + ([] if self.raw else [self.came])

    def results(self):
        return [struct(self.shape)] * (3 * self.raw + 2 * self.mid)

    def scratch(self):
        got = [dma((5,)), dma((4,))] if self.raw else []
        return got + ([dma((2,)), dma((2,)), dma((4,)), pltpu.VMEM((2, *self.shape), bf16)] if self.mid else [])

    def bind(self, given, results, scratch, side):
        core, x, y = place(side)
        self.side, self.at = side, x if self.axis == "x" else y
        near = lambda by: number_of(core, x + by, y, side) if self.axis == "x" else number_of(core, x, y + by, side)
        self.right, self.left = near(1), near(-1)
        results, scratch = list(results), list(scratch)
        self.src_ref = given[FIRST]
        if self.raw:
            self.came_ref, self.raw_ref, self.own_ref = results[:3]
            self.send, self.recv = scratch[:2]
        else:
            self.came_ref = given[SECOND]
        if self.mid:
            self.held_ref, self.sums_ref = results[-2:]
            self.send2, self.recv2, self.local, self.buf = scratch[-4:]

    def part(self, by, half):
        k = (self.at + by + self.side) % self.side
        lanes = slice(self.first, self.first + self.width)
        return self.src_ref.at[:, k, :, half, :, lanes] if self.dim == SECOND else self.src_ref.at[:, :, k, half, :, lanes]

    def raws(self, n):
        by, half, ref, to = ((2, FIRST, self.came_ref, self.right), (2, SECOND, self.came_ref, self.left),
                             (SECOND, SECOND, self.raw_ref, self.right), (-1, FIRST, self.raw_ref, self.left))[n]
        return remote(self.part(by, half), ref.at[:, :, half], self.send.at[n], self.recv.at[n], to)

    def mine(self, half):
        return pltpu.make_async_copy(self.part(FIRST, half), self.own_ref.at[:, :, half], self.send.at[4])

    def mids(self, half):
        return remote(self.held_ref.at[:, :, half], self.sums_ref.at[:, :, half], self.send2.at[half], self.recv2.at[half], self.left if half else self.right)

    def load(self, n):
        if n == THIRD:
            return pltpu.make_async_copy(self.came_ref, self.buf.at[SECOND], self.local.at[n])
        return pltpu.make_async_copy(self.part(-1 if n else SECOND, n), self.buf.at[FIRST, :, :, n], self.local.at[n])

    def hold(self):
        return pltpu.make_async_copy(self.buf.at[FIRST], self.held_ref, self.local.at[3])

    def start(self):
        if self.raw:
            for n in range(4):
                self.raws(n).start()
            self.mine(FIRST).start()

    def turn(self):
        if not self.mid:
            return
        if self.raw:
            for n in range(2):
                self.raws(n).wait_recv()
        for n in range(3):
            self.load(n).start()

    def add(self):
        if not self.mid:
            return
        for n in range(3):
            self.load(n).wait()
        for t in range(self.shape[FIRST]):
            for i in range(self.shape[SECOND]):
                self.buf[FIRST, t, i] = (self.buf[FIRST, t, i].astype(f32) + self.buf[SECOND, t, i].astype(f32)).astype(bf16)
        self.hold().start()

    def pass_on(self):
        if self.mid:
            self.hold().wait()
            for half in range(2):
                self.mids(half).start()

    def finish(self):
        if self.raw:
            self.mine(FIRST).wait()
            self.mine(SECOND).start()
            for n in range(4):
                self.raws(n).wait_send()
                if n >= 2 or not self.mid:
                    self.raws(n).wait_recv()
            self.mine(SECOND).wait()
        if self.mid:
            for half in range(2):
                self.mids(half).wait()

    def events(self):
        return self.start, self.turn, self.add, self.pass_on, self.finish


def first_rings(kind, u, came=(NONE, NONE)):
    w = u.shape[-1] // 2
    return [Ring(kind, "x", u, SECOND, FIRST, w, came[FIRST]), Ring(kind, "y", u, THIRD, w, w, came[SECOND])]


def second_rings(v):
    return [Ring("ring", axis, part, SECOND, FIRST, part.shape[-1]) for axis, part in zip("yx", v, strict=True)]


def ended(raw, own, sums):
    return (own.astype(f32) + raw.astype(f32) + sums.astype(f32)).astype(bf16)[:, :, NONE]


NEAR = (0, 1, -1, 2)


class Gather:
    def __init__(self, sources, shape):
        self.sources, self.shape = sources, shape

    def given(self):
        return list(self.sources)

    def results(self):
        return [struct(self.shape)]

    def scratch(self):
        return [dma((len(self.sources),)), dma((2, 36)), dma((2, 36))]

    def bind(self, given, results, scratch, side):
        self.side, self.me = side, place(side)
        self.from_refs, (self.full,), (self.local, self.send, self.recv) = given, results, scratch

    def spot(self, h, di, dj):
        _, x, y = self.me
        return (x + di, y + dj) if h == FIRST else (x + dj, y + di)

    def move(self, h, k, which, to, quarter=NONE, other=False):
        core = self.me[FIRST]
        share = self.view(number_of(core, *self.spot(h, *which), self.side), h, quarter)
        return remote(share, share, self.send.at[h, k], self.recv.at[h, k], number_of(1 - core if other else core, *self.spot(h, *to), self.side))

    def near(self, h):
        return [self.move(h, k, (0, 0), (1 - 2 * k, 0)) for k in range(2)]

    def far(self, h):
        return [self.move(h, 2 + k, (2 * k - 1, 0), (1 - 2 * k, 0), k) for k in range(2)]

    def side_ways(self, h, a):
        return [self.move(h, 4 + 2 * a + k, (NEAR[a], 0), (0, 1 - 2 * k)) for k in range(2)]

    def over(self, h, a):
        return [self.move(h, 12 + 2 * a + k, (NEAR[a], 2 * k - 1), (0, 1 - 2 * k), k) for k in range(2)]

    def twin(self, h, a, b):
        return [self.move(h, 20 + 4 * a + b, (NEAR[a], NEAR[b]), (0, 0), NONE, True)]

    def go(self, what, *places):
        for h in range(2):
            for a in places:
                for copy in what(h, *a):
                    copy.start()

    def come(self, what, *places):
        for h in range(2):
            for a in places:
                for copy in what(h, *a):
                    copy.wait_recv()

    def begin(self):
        own = [pltpu.make_async_copy(src, dst, self.local.at[n]) for n, (src, dst) in enumerate(self.own())]
        for copy in own:
            copy.start()
        for copy in own:
            copy.wait()
        self.go(self.near, ())
        self.go(self.side_ways, (0,))
        self.go(self.twin, (0, 0))

    def row(self):
        self.come(self.near, ())
        self.go(self.far, ())
        self.go(self.side_ways, (1,), (2,))
        self.go(self.twin, (1, 0), (2, 0))

    def row_end(self):
        self.come(self.far, ())
        self.go(self.side_ways, (3,))
        self.go(self.twin, (3, 0))

    def plane(self):
        all_of = [(a,) for a in range(4)]
        self.come(self.side_ways, *all_of)
        self.go(self.over, *all_of)
        self.go(self.twin, *((a, b) for a in range(4) for b in (1, 2)))

    def plane_end(self):
        self.come(self.over, *((a,) for a in range(4)))
        self.go(self.twin, *((a, 3) for a in range(4)))

    def finish(self):
        every = [(a, b) for a in range(4) for b in range(4)]
        self.come(self.twin, *every)
        for what, places in ((self.near, [()]), (self.far, [()]), (self.side_ways, [(a,) for a in range(4)]), (self.over, [(a,) for a in range(4)]), (self.twin, every)):
            for h in range(2):
                for a in places:
                    for copy in what(h, *a):
                        copy.wait_send()

    def events(self):
        return self.begin, self.row, self.row_end, self.plane, self.plane_end, self.finish


class GatherColumns(Gather):
    def __init__(self, sources, layer, n):
        super().__init__(sources, (sources[FIRST].shape[SECOND] * n, sources[FIRST].shape[THIRD] * len(sources)))
        self.layer, self.rows, self.width = layer, sources[FIRST].shape[SECOND], sources[FIRST].shape[THIRD]

    def view(self, device, h, quarter):
        lanes = pl.ds((2 * h + (quarter or 0)) * self.width, self.width * (2 if quarter is NONE else 1))
        return self.full.at[pl.ds(device * self.rows, self.rows), lanes]

    def own(self):
        me = number_of(*self.me, self.side)
        return [(src.at[self.layer], self.view(me, n // 2, n % 2)) for n, src in enumerate(self.from_refs)]


class GatherTiles(Gather):
    def __init__(self, source, layer, n):
        _, tiles, self.rows, width = source.shape
        super().__init__([source], (tiles, self.rows * n, width))
        self.layer, self.tiles = layer, tiles

    def view(self, device, h, quarter):
        half = self.tiles // 2
        cut = (half + 1) // 2
        first, count = ((0, half), (0, cut), (cut, half - cut))[0 if quarter is NONE else quarter + 1]
        return self.full.at[pl.ds(h * half + first, count), pl.ds(device * self.rows, self.rows)]

    def own(self):
        me = number_of(*self.me, self.side)
        return [(self.from_refs[FIRST].at[self.layer], self.full.at[:, pl.ds(me * self.rows, self.rows)])]


class GatherRows(Gather):
    def __init__(self, source, layer, n):
        _, self.rows, self.width = source.shape
        super().__init__([source], (self.rows * n, self.width))
        self.layer = layer

    def first_row(self, device):
        return ((device % 2) * self.side * self.side + device // 2) * self.rows

    def view(self, device, h, quarter):
        part = self.rows // 2
        rows = pl.ds(self.first_row(device) + (quarter or 0) * part, self.rows if quarter is NONE else part)
        return self.full.at[rows, pl.ds(h * (self.width // 2), self.width // 2)]

    def own(self):
        return [(self.from_refs[FIRST].at[self.layer], self.full.at[pl.ds(self.first_row(number_of(*self.me, self.side)), self.rows)])]


def barrier(side, far, partner):
    core, x, y = place(side)
    near = [number_of(core, x + a, y + b, side) for a, b in ((1, 0), (-1, 0), (0, 1), (0, -1))] if far else []
    if partner:
        near.append(number_of(1 - core, x, y, side))
    sem = pltpu.get_barrier_semaphore()
    for to in near:
        pl.semaphore_signal(sem, inc=1, device_id={"dp": to}, device_id_type=pl.DeviceIdType.MESH)
    pl.semaphore_wait(sem, len(near))


class Program:
    def __init__(self, side):
        self.side, self.count = side, 0

    def kernel(self, body, name, steps, ins, outs, shapes, scratch=(), flops=0, args=(), jobs=(), partner=False, alias=NONE):
        self.count += 1
        kinds = [j for j, _ in jobs]
        given = [x for j in kinds for x in j.given()]
        results = [x for j in kinds for x in j.results()]
        ends = [j.scratch() for j in kinds]
        sizes = [len(ins), len(given), len(outs), len(results), len(scratch)]
        talks = bool(jobs) or partner
        side = self.side

        def run(*refs):
            groups, at = [], 0
            for n in sizes:
                groups.append(refs[at : at + n])
                at += n
            own_in, job_in, own_out, job_out, own_scratch = groups
            todo = {}
            for (j, when), scr in zip(jobs, ends, strict=True):
                n, m = len(j.given()), len(j.results())
                j.bind(job_in[:n], job_out[:m], refs[at : at + len(scr)], side)
                job_in, job_out, at = job_in[n:], job_out[m:], at + len(scr)
                for event, step in zip(j.events(), (*when, steps), strict=True):
                    todo.setdefault((min(step, steps - 1), step == steps), []).append(event)
            i = pl.program_id(0)

            @pl.when(i == 0)
            def _():
                if talks:
                    barrier(side, bool(jobs), partner or any(isinstance(j, Gather) for j in kinds))

            def perform(last):
                for (step, late), events in sorted(todo.items(), key=lambda e: e[FIRST]):
                    if late == last:

                        @pl.when(i == step)
                        def _(events=events):
                            for event in events:
                                event()

            perform(False)
            body(*own_in, *own_out, *own_scratch)
            perform(True)

        size = sum(a.size * a.dtype.itemsize for a in args)
        extra = dict(collective_id=self.count, has_side_effects=True) if talks else {}
        got = pl.pallas_call(
            run,
            name=name,
            grid=(steps,),
            in_specs=[*ins, *[HBM] * len(given)],
            out_specs=[*outs, *[HBM] * len(results)],
            out_shape=[*shapes, *results],
            scratch_shapes=[*scratch, *[s for e in ends for s in e]],
            input_output_aliases=alias or {},
            compiler_params=pltpu.CompilerParams(dimension_semantics=("arbitrary",), vmem_limit_bytes=VMEM, **extra),
            cost_estimate=pl.CostEstimate(flops=flops, bytes_accessed=size, transcendentals=0),
        )(*args, *given)
        mine, rest = got[: len(outs)], got[len(outs) :]
        per_job = []
        for j in kinds:
            n = len(j.results())
            per_job.append(rest[:n])
            rest = rest[n:]
        return mine, per_job

    def carry(self, name, jobs):
        def body(out_ref):
            out_ref[...] = jnp.zeros_like(out_ref)

        spec = pl.BlockSpec((8, HEAD), lambda i: (0, 0))
        return self.kernel(body, name, 1, [], [spec], [struct((8, HEAD), f32)], jobs=[(j, [0] * (len(j.events()) - 1)) for j in jobs])[SECOND]


def front_body(h_ref, w_ref, wo_ref, cos_ref, sin_ref, qkv_ref, o_ref, lse_ref, mid_ref, a_s, qkv_s, acc_s, *, pairs):
    i = pl.program_id(0)

    @pl.when(i == 0)
    def _():
        a_s[...] = normed(h_ref[...])
        acc_s[...] = jnp.zeros_like(acc_s)

    def project(turn):
        for n in range(pairs):
            lanes = slice(n * COLS, (n + 1) * COLS)
            got = dot(a_s[...], w_ref[:, lanes]).astype(bf16)
            if turn:
                got = jnp.concatenate([turned(got[:, :HEAD], cos_ref, sin_ref), turned(got[:, HEAD:], cos_ref, sin_ref)], axis=1)
            qkv_ref[:, lanes] = got
            qkv_s[i * pairs + n] = got

    pl.when(i < 2)(lambda: project(True))
    pl.when(i == 2)(lambda: project(False))

    @pl.when(i > 2)
    def _():
        n = i - 3
        attend(qkv_s.at[n], qkv_s.at[pairs + n], qkv_s.at[2 * pairs + n], o_ref, lse_ref)
        acc_s[...] += dot(o_ref[...], wo_ref[...])

    @pl.when(i == pl.num_programs(0) - 1)
    def _():
        mid_ref[...] = plus(h_ref[...], acc_s[...])


def turned(t, cos_ref, sin_ref):
    t = t.astype(f32)
    return (t * cos_ref[...] + pltpu.roll(t, HEAD // 2, 1) * sin_ref[...]).astype(bf16)


def hides():
    return lax.broadcasted_iota(jnp.int32, (BQ, BQ), SECOND) >= lax.broadcasted_iota(jnp.int32, (BQ, BQ), FIRST)


def attend(q_ref, k_ref, v_ref, o_ref, lse_ref):
    t, heads = q_ref.shape[FIRST], q_ref.shape[SECOND] // HEAD
    scale = HEAD**-0.5
    e = scale * LOG2E
    seen = hides()
    for n in range(heads):
        lanes = slice(n * HEAD, (n + 1) * HEAD)
        for at in range(0, t, BQ):
            end = at + BQ
            s = dot_t(k_ref[:end, lanes], q_ref[at:end, lanes])
            low = jnp.where(seen, s[at:], HIDDEN)
            s = jnp.concatenate([s[:at], low], axis=0) if at else low
            top = s.max(axis=0, keepdims=True)
            p = jnp.exp2((s - top) * e)
            total = p.sum(axis=0, keepdims=True)
            out = dot(v_ref[:end, lanes].T, p.astype(bf16))
            o_ref[at:end, lanes] = (out * (1 / total)).T.astype(bf16)
            lse_ref[0, n : n + 1, at:end] = top * scale + jnp.log(total)


def front(program, h, wa, tables, jobs):
    t, d = h.shape
    q = wa.shape[SECOND] // 4
    pairs = q // COLS
    late = lambda i: jnp.maximum(i - 3, 0)
    first = lambda i: (0, jnp.minimum(i, 2))
    return program.kernel(
        functools.partial(front_body, pairs=pairs), "front", 3 + pairs,
        [still((t, d)), block((d, q), first), block((COLS, d), lambda i: (late(i), 3)), still((t, HEAD)), still((t, HEAD))],
        [block((t, q), first), block((t, COLS), lambda i: (0, late(i))), block((1, 2, t), lambda i: (late(i), 0, 0)), still((t, d))],
        [struct((t, 3 * q)), struct((t, q)), struct((pairs, 2, t), f32), struct((t, d))],
        [pltpu.VMEM((t, d), bf16), pltpu.VMEM((3 * pairs, t, COLS), bf16), pltpu.VMEM((t, d), f32)],
        8 * t * d * q + 3 * t * t * q, (h, wa, wa, *tables), jobs)


def mlp_body(h_ref, wg_ref, wd_ref, gu_ref, out_ref, b_s, acc_s):
    i = pl.program_id(0)

    @pl.when(i == 0)
    def _():
        b_s[...] = normed(h_ref[...])
        acc_s[...] = jnp.zeros_like(acc_s)

    p = []
    for n in range(wg_ref.shape[FIRST]):
        got = dot(b_s[...], wg_ref[n])
        gate, up = got[:, :COLS], got[:, COLS:]
        gu_ref[n] = got
        p.append((gate * jax.nn.sigmoid(gate) * up).astype(bf16))
    acc_s[...] += dot(jnp.concatenate(p, axis=1), wd_ref[...])

    @pl.when(i == pl.num_programs(0) - 1)
    def _():
        out_ref[...] = plus(h_ref[...], acc_s[...])


def mlp(program, h, wg, wd, jobs):
    (t, d), tiles = h.shape, wg.shape[FIRST]
    wide = lambda rows: block((2, rows, 2 * COLS), lambda i: (i, 0, 0))
    return program.kernel(
        mlp_body, "mlp", tiles // 2,
        [still((t, d)), wide(d), block((2 * COLS, d), lambda i: (i, 0))], [wide(t), still((t, d))],
        [struct((tiles, t, 2 * COLS), f32), struct((t, d))], [pltpu.VMEM((t, d), bf16), pltpu.VMEM((t, d), f32)],
        6 * t * d * tiles * COLS, (h, wg, wd), jobs)


def mlp_back_body(dh_ref, h_ref, wd_ref, wg_ref, gu_ref, out_ref, ug_ref, ud_ref, bt_s, acc_s, hold_g, hold_d, got_g, got_d, send_sem, recv_sem, *, side):
    i = pl.program_id(0)
    last = pl.num_programs(0) - 1
    half = pl.num_programs(0) // 2
    core, x, y = place(side)
    other = number_of(1 - core, x, y, side)

    def sends(n):
        return [remote(hold.at[n % 2], got.at[n], send_sem.at[n, k], recv_sem.at[n, k], other) for k, (hold, got) in enumerate(((hold_g, got_g), (hold_d, got_d)))]

    def stores(n):
        own = n - half
        return [pltpu.make_async_copy(hold_g.at[n % 2], ug_ref.at[own], send_sem.at[n, FIRST]),
                pltpu.make_async_copy(hold_d.at[n % 2], ud_ref.at[pl.ds(own * COLS, COLS)], send_sem.at[n, SECOND])]

    def left(n):
        @pl.when(n < half)
        def _():
            for copy in sends(n):
                copy.wait_send()

        @pl.when(n >= half)
        def _():
            for copy in stores(n):
                copy.wait()

    @pl.when(i == 0)
    def _():
        bt_s[...] = normed(h_ref[...]).T
        acc_s[...] = jnp.zeros_like(acc_s)
        got_g[half] = jnp.zeros(got_g.shape[1:], bf16)
        got_d[half] = jnp.zeros(got_d.shape[1:], bf16)

    pl.when(i >= 2)(lambda: left(i - 2))

    @pl.when(i >= half)
    def _():
        for copy in sends(i - half):
            copy.wait_recv()

    came = jnp.where(i < half, half, i - half)
    dp = dot_t(dh_ref[...], wd_ref[...]).astype(bf16).astype(f32)
    gate, up = gu_ref[0, :, :COLS], gu_ref[0, :, COLS:]
    s = jax.nn.sigmoid(gate)
    silu = gate * s
    p = (silu * up).astype(bf16)
    by = jnp.concatenate([(dp * up * (s * (1 + gate * (1 - s)))).astype(bf16), (dp * silu).astype(bf16)], axis=1)
    hold_d[i % 2] = (dot(p.T, dh_ref[...]) + got_d[came].astype(f32)).astype(bf16)
    hold_g[i % 2] = (dot(bt_s[...], by) + got_g[came].astype(f32)).astype(bf16)
    acc_s[...] += dot_t(by, wg_ref[0])

    @pl.when(i < half)
    def _():
        for copy in sends(i):
            copy.start()

    @pl.when(i >= half)
    def _():
        for copy in stores(i):
            copy.start()

    @pl.when(i == last)
    def _():
        out_ref[...] = norm_back(h_ref[...], acc_s[...], dh_ref[...])
        left(i - 1)
        left(i)


def mlp_back(program, dh, h, wd, wg, gu, jobs):
    (t, d), tiles = h.shape, wg.shape[FIRST]
    half = tiles // 2

    def tile(i):
        core = lax.axis_index("dp") % 2
        return jnp.where(i < half, (1 - core) * half + i, core * half + i - half)

    wide = lambda rows: block((1, rows, 2 * COLS), lambda i: (tile(i), 0, 0))
    vmem = lambda n: [pltpu.VMEM((n, d, 2 * COLS), bf16), pltpu.VMEM((n, COLS, d), bf16)]
    (out, ug, ud), got = program.kernel(
        functools.partial(mlp_back_body, side=program.side), "mlp_back", tiles,
        [still((t, d)), still((t, d)), block((COLS, d), lambda i: (tile(i), 0)), wide(d), wide(t)], [still((t, d)), HBM, HBM],
        [struct((t, d)), struct((half, d, 2 * COLS)), struct((half * COLS, d))],
        [pltpu.VMEM((d, t), bf16), pltpu.VMEM((t, d), f32), *vmem(2), *vmem(half + 1), dma((tiles, 2)), dma((half, 2))],
        12 * t * d * tiles * COLS, (dh, h, wd, wg, gu), jobs, True)
    return out, cut(ug, program.side), cut(ud[NONE], program.side), got


def cut(u, side):
    return u.reshape(u.shape[FIRST], side, side, 2, -1, u.shape[-1])


def attend_back_body(dh_ref, w_ref, o_ref, q_ref, k_ref, v_ref, lse_ref, cos_ref, sin_ref, out_ref, u_ref, do_s, dq_s, keep_s, got_s, send_sem, recv_sem, *, side):
    i = pl.program_id(0)
    pairs = pl.num_programs(0) // 2
    rows = keep_s.shape[SECOND]
    core, x, y = place(side)
    other = number_of(1 - core, x, y, side)
    copy = lambda n: remote(keep_s.at[n], got_s.at[n], send_sem.at[n], recv_sem.at[n], other)
    store = lambda n: pltpu.make_async_copy(keep_s.at[n], u_ref.at[FIRST, pl.ds(n * rows, rows)], send_sem.at[n])

    @pl.when(i < pairs)
    def _():
        do_s[i] = dot_t(dh_ref[...], w_ref[...]).astype(bf16)
        keep_s[i] = dot(o_ref[...].T, dh_ref[...]).astype(bf16)
        pl.when(core == 0)(lambda: copy(i).start())

    @pl.when(i >= pairs)
    def _():
        n = i - pairs
        pl.when(core == 0)(lambda: copy(n).wait_send())

        @pl.when(core == 1)
        def _():
            copy(n).wait_recv()
            keep_s[n] = (keep_s[n].astype(f32) + got_s[n].astype(f32)).astype(bf16)
            store(n).start()

        heads_back(q_ref, k_ref, v_ref, do_s.at[n], o_ref, lse_ref, cos_ref, sin_ref, out_ref, dq_s)
        pl.when(core == 1)(lambda: store(n).wait())


def heads_back(q_ref, k_ref, v_ref, do_ref, o_ref, lse_ref, cos_ref, sin_ref, out_ref, dq_s):
    t, heads = q_ref.shape[FIRST], q_ref.shape[SECOND] // HEAD
    scale = HEAD**-0.5
    e = scale * LOG2E
    seen = hides()

    def turned_back(x, rows):
        x = (x * scale).astype(bf16).astype(f32)
        return (x * cos_ref[rows, :] - pltpu.roll(x, HEAD // 2, 1) * sin_ref[rows, :]).astype(bf16)

    for n in range(heads):
        lanes = slice(n * HEAD, (n + 1) * HEAD)
        lse = lse_ref[0, n : n + 1, :] * LOG2E
        delta = (do_ref[:, lanes].astype(f32) * o_ref[:, lanes].astype(f32)).T.sum(axis=0, keepdims=True)
        for at in range(0, t, BQ):
            end = at + BQ
            k, v, q, do = k_ref[at:end, lanes], v_ref[at:end, lanes], q_ref[at:, lanes], do_ref[at:, lanes]
            p = jnp.exp2(dot_t(k, q) * e - lse[:, at:])
            low = jnp.where(seen, p[:, :BQ], 0.0)
            p = low if end == t else jnp.concatenate([low, p[:, BQ:]], axis=1)
            ds = (p * (dot_t(v, do) - delta[:, at:])).astype(bf16)
            out_ref[THIRD, at:end, lanes] = dot(p.astype(bf16), do).astype(bf16)
            out_ref[SECOND, at:end, lanes] = turned_back(dot(ds, q), slice(at, end))
            part = dot(k.T, ds)
            if at:
                dq_s[n, :, at:] += part
            else:
                dq_s[n] = part
        out_ref[FIRST, :, lanes] = turned_back(dq_s[n].T, slice(0, t))


def attend_back(program, dh, wa, qkv, o, lse, tables, jobs):
    (t, d), q = dh.shape, o.shape[SECOND]
    pairs = q // COLS
    late = lambda j: jnp.maximum(j - pairs, 0)
    head = lambda first: block((t, COLS), lambda j: (0, first + late(j)))
    tiles = [pltpu.VMEM((pairs, COLS, d), bf16)] * 2
    return program.kernel(
        functools.partial(attend_back_body, side=program.side), "attend_back", 2 * pairs,
        [still((t, d)), block((COLS, d), lambda j: (jnp.minimum(j, pairs - 1), 3)), block((t, COLS), lambda j: (0, j % pairs)),
         head(0), head(pairs), head(2 * pairs), block((1, 2, t), lambda j: (late(j), 0, 0)), still((t, HEAD)), still((t, HEAD))],
        [block((3, t, COLS), lambda j: (0, 0, late(j))), HBM], [struct((3, t, q)), struct((2, d, q))],
        [pltpu.VMEM((pairs, t, COLS), bf16), pltpu.VMEM((2, HEAD, t), f32), *tiles, dma((pairs,)), dma((pairs,))],
        4 * t * d * q + 7 * t * t * q, (dh, wa, o, qkv, qkv, qkv, lse, *tables), jobs, True)


def qkv_back_body(dh_ref, h_ref, d_ref, w_ref, _, out_ref, u_ref, at_s, acc_s, hold_s, got_s, send_sem, recv_sem, *, side):
    s = pl.program_id(0)
    last = pl.num_programs(0) - 1
    rows = w_ref.shape[FIRST]
    per = at_s.shape[FIRST] // rows
    r = s % per
    core, x, y = place(side)
    other = number_of(1 - core, x, y, side)
    sends = jnp.where(core == 0, per, 2 * per)
    zero = 2 * per

    def send(n):
        to = n + (1 - core) * per
        return remote(hold_s.at[n % 2], got_s.at[to], send_sem.at[n], recv_sem.at[to], other)

    def store(n):
        return pltpu.make_async_copy(hold_s.at[n % 2], u_ref.at[n // per - 1, pl.ds((n % per) * rows, rows)], send_sem.at[n])

    def left(n):
        pl.when(n < sends)(lambda: send(n).wait_send())
        pl.when(n >= sends)(lambda: store(n).wait())

    @pl.when(s == 0)
    def _():
        at_s[...] = normed(h_ref[...]).T
        acc_s[...] = jnp.zeros_like(acc_s)
        got_s[zero] = jnp.zeros(got_s.shape[1:], bf16)

    pl.when(s >= 2)(lambda: left(s - 2))

    @pl.when(s >= sends)
    def _():
        pltpu.make_async_copy(got_s.at[s - per], got_s.at[s - per], recv_sem.at[s - per]).wait()

    lanes = pl.ds(pl.multiple_of(r * rows, rows), rows)
    acc_s[:, lanes] += dot_t(d_ref[0], w_ref[...])
    came = jnp.where(s < sends, zero, s - per)
    hold_s[s % 2] = (dot(at_s[lanes, :], d_ref[0]) + got_s[came].astype(f32)).astype(bf16)
    pl.when(s < sends)(lambda: send(s).start())
    pl.when(s >= sends)(lambda: store(s).start())

    @pl.when(s == last)
    def _():
        out_ref[...] = norm_back(h_ref[...], acc_s[...], dh_ref[...])
        left(s - 1)
        left(s)


def qkv_back(program, dh, h, dqkv, wa, u, jobs):
    (t, d), q = h.shape, wa.shape[SECOND] // 4
    rows = COLS
    per = d // rows
    matrix = lambda s: (s // per + 2 * (1 - lax.axis_index("dp") % 2)) % 3
    (out, u), got = program.kernel(
        functools.partial(qkv_back_body, side=program.side), "qkv_back", 3 * per,
        [still((t, d)), still((t, d)), block((1, t, q), lambda s: (matrix(s), 0, 0)), block((rows, q), lambda s: (s % per, matrix(s))), HBM],
        [still((t, d)), HBM], [struct((t, d)), struct(u.shape)],
        [pltpu.VMEM((d, t), bf16), pltpu.VMEM((t, d), f32), pltpu.VMEM((2, rows, q), bf16), pltpu.VMEM((2 * per + 1, rows, q), bf16), dma((3 * per,)), dma((2 * per,))],
        12 * t * d * q, (dh, h, dqkv, wa, u), jobs, True, {4: 1})
    return out, cut(u, program.side), got


def tables_of(t):
    half = HEAD // 2
    angle = jnp.arange(t, dtype=f32)[:, None] * THETA ** (-jnp.arange(half, dtype=f32) / half)
    cos, sin = jnp.cos(angle), jnp.sin(angle)
    return jnp.concatenate([cos, cos], -1), jnp.concatenate([-sin, sin], -1)


def padded(rows):
    return -(-rows // 16) * 16


def pack(w_gate, w_up, w_down, n):
    rows = w_down.shape[SECOND]
    more = padded(rows) - rows

    def spread(w):
        layers, r = w.shape[:2]
        w = jnp.pad(w.reshape(layers, r, n // 2, 2, rows), ((0, 0),) * 4 + ((0, more),))
        return w.swapaxes(-2, -3).reshape(layers, r, -1, COLS).swapaxes(SECOND, THIRD)

    return jnp.concatenate([spread(w_gate), spread(w_up)], axis=-1), jnp.pad(w_down, ((0, 0), (0, more), (0, 0)))


def unpack(wg, n, rows):
    layers, r = wg.shape[FIRST], wg.shape[THIRD]

    def back(w):
        w = w.swapaxes(SECOND, THIRD).reshape(layers, r, 2, n // 2, -1)[..., :rows]
        return w.swapaxes(-2, -3).reshape(layers, r, n * rows)

    return back(wg[..., :COLS]), back(wg[..., COLS:])


def solution(mesh):
    n = mesh.shape["dp"]
    side = math.isqrt(n // 2)

    def step(x, dy, wq, wk, wv, wo, w_gate, w_up, w_down):
        program = Program(side)
        layers, rows = w_down.shape[:2]
        core = place(side)[FIRST]
        tables = tables_of(x.shape[SECOND])
        of_a = lambda number: GatherColumns([wq, wk, wv, wo], number, n)
        ((wa,),) = program.carry("first", [of_a(0)])
        tiles, downs = pack(w_gate, w_up, w_down, n)
        of_g, of_d = (lambda number: GatherTiles(tiles, number, n)), (lambda number: GatherRows(downs, number, n))
        h, kept, wd = x[0], [], None
        for number in range(layers):
            jobs = [(of_g(number), FRONT_G)] + ([] if number else [(of_d(number), FRONT_D)])
            (qkv, o, lse, mid), got = front(program, h, wa, tables, jobs)
            wg, wd = got[FIRST][FIRST], wd if number else got[SECOND][FIRST]
            jobs = [] if number == layers - 1 else [(of_a(number + 1), MLP_A), (of_d(number + 1), MLP_D)]
            (gu, out), got = mlp(program, mid, wg, wd, jobs)
            kept.append((wa, wg, wd, h, qkv, o, lse, mid, gu))
            h = out
            if jobs:
                (wa,), (wd,) = got

        def close(got):
            return [ended(raw, own, sums) for _, raw, own, _, sums in got]

        def whole(got):
            return jnp.concatenate([part[:, FIRST, FIRST] for part in close(got)], axis=-1)

        by_h, above = dy[0], None
        results = []
        for number in reversed(range(layers)):
            wa, wg, wd, hin, qkv, o, lse, mid, gu = kept[number]
            jobs = []
            if above:
                jobs = [(r, MLP_BACK) for part in above[:2] for r in second_rings(part)] + [(r, MLP_BACK) for r in first_rings("ring", above[THIRD])]
            by_mid, ug, ud, got = mlp_back(program, by_h, mid, wd, wg, gu, jobs)
            if above:
                done, tail = [whole(got[:2]), whole(got[2:4])], close(got[4:])
            (dqkv, u), raw = attend_back(program, by_mid, wa, qkv, o, lse, tables, [(r, [0] * 4) for part in (ug, ud) for r in first_rings("raw", part)])
            came = [r[FIRST] for r in raw]
            jobs = [(r, QKV_BACK) for r in first_rings("mid", ug, came[:2]) + first_rings("mid", ud, came[2:]) + (second_rings(tail) if above else [])]
            by_h, ua, got = qkv_back(program, by_mid, hin, dqkv, wa, u, jobs)
            if above:
                results.append([*done, whole(got[4:])])
            v = close([(*r, *s) for r, s in zip(raw, got[:4], strict=True)])
            above = v[:2], v[2:], ua
        got = program.carry("tail", [r for part in above[:2] for r in second_rings(part)] + first_rings("ring", above[THIRD]))
        done, tail = [whole(got[:2]), whole(got[2:4])], close(got[4:])
        results.append([*done, whole(program.carry("end", second_rings(tail)))])

        zg, zd, za = (jnp.stack(parts) for parts in zip(*reversed(results), strict=True))

        def swapped(z):
            mine, other = (lax.dynamic_index_in_dim(z, c, 2, keepdims=False) for c in (core, 1 - core))
            got = lax.ppermute(other, "dp", [(b, b ^ 1) for b in range(n)])
            return jnp.where(core == 0, mine, got), jnp.where(core == 0, got, mine)

        qk, ov = swapped(za)
        by_gate, by_up = unpack(jnp.concatenate(swapped(zg), axis=SECOND), n, rows)
        by_down = zd.reshape(layers, -1, zd.shape[-1])[:, :rows]
        return by_h[None], qk[:, FIRST], qk[:, SECOND], ov[:, SECOND], ov[:, FIRST], by_gate, by_up, by_down

    states, cut_rows = P(("rep", "dp"), None, None), P(None, "dp", None)
    return jax.shard_map(
        step,
        mesh=mesh,
        in_specs=(states, states) + (cut_rows,) * 7,
        out_specs=(states,) + (P("rep", "dp", None),) * 7,
        check_vma=False,
    )


FRONT_G = FRONT_D = (0, 2, 3, 7, 7)
MLP_A = MLP_D = (0, 1, 2, 5, 6)
MLP_BACK = (0, 6, 7, 8)
QKV_BACK = (0, 0, 1, 2)
```

```python
import functools
import math

import jax
import jax.numpy as jnp
from jax import lax
from jax.experimental import pallas as pl
from jax.experimental.pallas import tpu as pltpu
from jax.sharding import PartitionSpec as P

HEAD = 128
THETA = 10000
EPS = 1e-6
LOG2E = 1.4426950408889634
HIDDEN = -2e30
VMEM = 62 * 2**20
COLS = 2 * HEAD
BQ = 256
HBM = pl.BlockSpec(memory_space=pl.ANY)
NONE, FIRST, SECOND, THIRD = None, 0, 1, 2
BOTH, FOUR = range(2), range(4)
HERE = (0, 0)

bf16, f32 = jnp.bfloat16, jnp.float32
dma = pltpu.SemaphoreType.DMA


def dot(a, b, ca=1, cb=0):
    return lax.dot_general(a, b, (((ca,), (cb,)), ((), ())), preferred_element_type=f32)


def dot_t(a, b):
    return dot(a, b, SECOND, SECOND)


def still(shape):
    return pl.BlockSpec(shape, lambda *_: (0,) * len(shape), pipeline_mode=pl.Buffered(SECOND))


def block(shape, where):
    return pl.BlockSpec(shape, where)


def struct(shape, dtype=bf16):
    return jax.ShapeDtypeStruct(shape, dtype)


def scale_of(wide):
    return lax.rsqrt(jnp.mean(wide * wide, -1, keepdims=True) + EPS)


def normed(h):
    wide = h.astype(f32)
    return (wide * scale_of(wide)).astype(bf16)


def norm_back(h, by_a, by_h):
    wide = h.astype(f32)
    scale = scale_of(wide)
    by_a = by_a.astype(bf16).astype(f32)
    mine = scale * by_a - wide * (scale * scale * scale * jnp.mean(by_a * wide, -1, keepdims=True))
    return (by_h.astype(f32) + mine.astype(bf16).astype(f32)).astype(bf16)


def plus(h, part):
    return (h.astype(f32) + part.astype(bf16).astype(f32)).astype(bf16)


def place(side):
    me = lax.axis_index("dp")
    core, chip = me % 2, me // 2
    return core, chip // side, chip % side


def number_of(core, x, y, side):
    return (((x + side) % side) * side + (y + side) % side) * 2 + core


def remote(src, dst, send, recv, to):
    return pltpu.make_async_remote_copy(src_ref=src, dst_ref=dst, send_sem=send, recv_sem=recv, device_id={"dp": to}, device_id_type=pl.DeviceIdType.MESH)


class Ring:
    def __init__(self, kind, axis, src, dim, first, width, came=None):
        self.kind, self.axis, self.src, self.dim, self.first, self.width, self.came = kind, axis, src, dim, first, width, came
        self.rows = src.shape[3] // 2
        self.shape = (src.shape[FIRST], src.shape[3 - dim], 2, self.rows, width)
        self.raw, self.mid = kind != "mid", kind != "raw"

    def given(self):
        return [self.src] + ([] if self.raw else [self.came])

    def results(self):
        return [struct(self.shape)] * (2 * self.raw + 3 * self.mid)

    def scratch(self):
        got = [dma((4,)), dma((4,))] if self.raw else []
        return got + ([dma((2,)), dma((2,)), dma((7,)), pltpu.VMEM((3, *self.shape), bf16)] if self.mid else [])

    def bind(self, given, results, scratch, side):
        core, x, y = place(side)
        self.side, self.at = side, x if self.axis == "x" else y
        near = lambda by: number_of(core, x + by, y, side) if self.axis == "x" else number_of(core, x, y + by, side)
        self.right, self.left = near(1), near(-1)
        results, scratch = list(results), list(scratch)
        if given:
            self.src_ref = given[FIRST]
        if self.raw:
            self.came_ref, self.raw_ref = results[:2]
            self.send, self.recv = scratch[:2]
        else:
            self.came_ref = given[SECOND]
        if self.mid:
            self.held_ref, self.own_ref, self.sums_ref = results[-3:]
            self.send2, self.recv2, self.local, self.buf = scratch[-4:]

    def part(self, by, half, ts=slice(NONE)):
        k = (self.at + by + self.side) % self.side
        rows, lanes = slice(half * self.rows, (half + 1) * self.rows), slice(self.first, self.first + self.width)
        return self.src_ref.at[ts, k, :, rows, lanes] if self.dim == SECOND else self.src_ref.at[ts, :, k, rows, lanes]

    def raws(self, n, ts=slice(NONE), sem=()):
        by, half, ref, to = ((2, FIRST, self.came_ref, self.right), (2, SECOND, self.came_ref, self.left),
                             (SECOND, SECOND, self.raw_ref, self.right), (-1, FIRST, self.raw_ref, self.left))[n]
        return remote(self.part(by, half, ts), ref.at[ts, :, half], self.send.at[n, *sem], self.recv.at[n, *sem], to)

    def mids(self, half):
        return remote(self.held_ref.at[:, :, half], self.sums_ref.at[:, :, half], self.send2.at[half], self.recv2.at[half], self.left if half else self.right)

    def load(self, n):
        if n == THIRD:
            return pltpu.make_async_copy(self.came_ref, self.buf.at[SECOND], self.local.at[n])
        if n > THIRD:
            return pltpu.make_async_copy(self.part(FIRST, n - 3), self.buf.at[THIRD, :, :, n - 3], self.local.at[n])
        return pltpu.make_async_copy(self.part(-1 if n else SECOND, n), self.buf.at[FIRST, :, :, n], self.local.at[n])

    def stores(self):
        return [pltpu.make_async_copy(self.buf.at[FIRST], self.held_ref, self.local.at[5]), pltpu.make_async_copy(self.buf.at[THIRD], self.own_ref, self.local.at[6])]

    def start(self):
        if self.raw:
            for n in FOUR:
                self.raws(n).start()

    def turn(self):
        if self.raw and self.mid:
            for n in BOTH:
                self.raws(n).wait_recv()
        if self.mid:
            for n in range(5):
                self.load(n).start()

    def add(self):
        if not self.mid:
            return
        for n in range(5):
            self.load(n).wait()
        for t in range(self.shape[FIRST]):
            for i in range(self.shape[SECOND]):
                self.buf[FIRST, t, i] = (self.buf[FIRST, t, i].astype(f32) + self.buf[SECOND, t, i].astype(f32)).astype(bf16)
        for copy in self.stores():
            copy.start()

    def pass_on(self):
        if self.mid:
            for copy in self.stores():
                copy.wait()
            for half in BOTH:
                self.mids(half).start()

    def finish(self):
        if self.raw:
            for n in FOUR:
                self.raws(n).wait_send()
                if n >= 2 or not self.mid:
                    self.raws(n).wait_recv()
        if self.mid:
            for half in BOTH:
                self.mids(half).wait()

    def events(self):
        return self.start, self.turn, self.add, self.pass_on, self.finish


class TileRing(Ring):
    def given(self):
        return []

    def scratch(self):
        return [dma((4, self.shape[FIRST]))] * 2

    def go(self, t):
        for n in FOUR:
            self.raws(n, pl.ds(t, 1), (t,)).start()

    def finish(self):
        for t in range(self.shape[FIRST]):
            for n in FOUR:
                self.raws(n, pl.ds(t, 1), (t,)).wait()

    def events(self):
        return (self.finish,)


def first_rings(kind, u, came=(NONE, NONE), made=Ring):
    w = u.shape[-1] // 2
    return [made(kind, "x", u, SECOND, FIRST, w, came[FIRST]), made(kind, "y", u, THIRD, w, w, came[SECOND])]


def second_rings(v):
    return [Ring("ring", axis, part, SECOND, FIRST, part.shape[-1]) for axis, part in zip("yx", v, strict=True)]


def ended(raw, own, sums):
    got = (own.astype(f32) + raw.astype(f32) + sums.astype(f32)).astype(bf16)
    return got.reshape(*got.shape[:2], 1, -1, got.shape[-1])


NEAR = (0, 1, -1, 2)


class Gather:
    def __init__(self, source, layer, shape):
        self.source, self.layer, self.shape = source, layer, shape

    def given(self):
        return [self.source]

    def results(self):
        return [struct(self.shape)]

    def scratch(self):
        return [dma, dma((2, 36)), dma((2, 36))]

    def bind(self, given, results, scratch, side):
        self.side, self.me = side, place(side)
        (self.from_ref,), (self.full,), (self.local, self.send, self.recv) = given, results, scratch

    def own(self):
        return pltpu.make_async_copy(self.from_ref.at[self.layer], self.whole(number_of(*self.me, self.side)), self.local)

    def spot(self, h, di, dj):
        _, x, y = self.me
        return (x + di, y + dj) if h == FIRST else (x + dj, y + di)

    def move(self, h, k, which, to, quarter=NONE, other=False):
        core = self.me[FIRST]
        share = self.view(number_of(core, *self.spot(h, *which), self.side), h, quarter)
        return remote(share if any(which) else self.mine(h), share, self.send.at[h, k], self.recv.at[h, k], number_of(1 - core if other else core, *self.spot(h, *to), self.side))

    def near(self, h):
        return [self.move(h, k, HERE, (1 - 2 * k, 0)) for k in BOTH]

    def far(self, h):
        return [self.move(h, 2 + k, (2 * k - 1, 0), (1 - 2 * k, 0), k) for k in BOTH]

    def side_ways(self, h, a):
        return [self.move(h, 4 + 2 * a + k, (NEAR[a], 0), (0, 1 - 2 * k)) for k in BOTH]

    def over(self, h, a):
        return [self.move(h, 12 + 2 * a + k, (NEAR[a], 2 * k - 1), (0, 1 - 2 * k), k) for k in BOTH]

    def twin(self, h, a, b):
        return [self.move(h, 20 + 4 * a + b, (NEAR[a], NEAR[b]), HERE, NONE, True)]

    def go(self, what, *places):
        for h in BOTH:
            for a in places:
                for copy in what(h, *a):
                    copy.start()

    def come(self, what, *places):
        for h in BOTH:
            for a in places:
                for copy in what(h, *a):
                    copy.wait_recv()

    def begin(self):
        self.go(self.near, ())
        self.go(self.side_ways, (0,))
        self.go(self.twin, HERE)
        self.own().start()

    def row(self):
        self.come(self.near, ())
        self.go(self.far, ())
        self.go(self.side_ways, (1,), (2,))
        self.go(self.twin, (1, 0), (2, 0))

    def row_end(self):
        self.come(self.far, ())
        self.go(self.side_ways, (3,))
        self.go(self.twin, (3, 0))
        self.come(self.side_ways, (0,))
        self.go(self.over, (0,))

    def plane(self):
        rest = [(a,) for a in range(1, 4)]
        self.come(self.side_ways, *rest)
        self.go(self.over, *rest)
        self.go(self.twin, *((a, b) for a in FOUR for b in (1, 2)))

    def plane_end(self):
        self.come(self.over, *((a,) for a in FOUR))
        self.go(self.twin, *((a, 3) for a in FOUR))

    def finish(self):
        every = [(a, b) for a in FOUR for b in FOUR]
        self.come(self.twin, *every)
        self.own().wait()
        for what, places in ((self.near, [()]), (self.far, [()]), (self.side_ways, [(a,) for a in FOUR]), (self.over, [(a,) for a in FOUR]), (self.twin, every)):
            for h in BOTH:
                for a in places:
                    for copy in what(h, *a):
                        copy.wait_send()

    def events(self):
        return self.begin, self.row, self.row_end, self.plane, self.plane_end, self.finish


class GatherColumns(Gather):
    def __init__(self, source, layer, n):
        _, self.rows, self.width = source.shape
        super().__init__(source, layer, (self.rows * n, self.width))

    def lanes(self, h, quarter):
        part = self.width // 4
        return pl.ds((2 * h + (quarter or 0)) * part, part * (2 if quarter is NONE else 1))

    def view(self, device, h, quarter):
        return self.full.at[pl.ds(device * self.rows, self.rows), self.lanes(h, quarter)]

    def mine(self, h):
        return self.from_ref.at[self.layer, :, self.lanes(h, NONE)]

    def whole(self, device):
        return self.full.at[pl.ds(device * self.rows, self.rows)]


class GatherTiles(Gather):
    def __init__(self, source, layer, n):
        _, self.tiles, self.rows, width = source.shape
        super().__init__(source, layer, (self.tiles, self.rows * n, width))

    def range(self, h, quarter):
        half = self.tiles // 2
        cut = (half + 1) // 2
        first, count = ((0, half), (0, cut), (cut, half - cut))[0 if quarter is NONE else quarter + 1]
        return pl.ds(h * half + first, count)

    def view(self, device, h, quarter):
        return self.full.at[self.range(h, quarter), pl.ds(device * self.rows, self.rows)]

    def mine(self, h):
        return self.from_ref.at[self.layer, self.range(h, NONE)]

    def whole(self, device):
        return self.full.at[:, pl.ds(device * self.rows, self.rows)]


class GatherRows(Gather):
    def __init__(self, source, layer, n):
        _, self.rows, self.width = source.shape
        super().__init__(source, layer, (self.rows * n, self.width))

    def first_row(self, device):
        return ((device % 2) * self.side * self.side + device // 2) * self.rows

    def lanes(self, h):
        return pl.ds(h * (self.width // 2), self.width // 2)

    def view(self, device, h, quarter):
        part = self.rows // 2
        rows = pl.ds(self.first_row(device) + (quarter or 0) * part, self.rows if quarter is NONE else part)
        return self.full.at[rows, self.lanes(h)]

    def mine(self, h):
        return self.from_ref.at[self.layer, :, self.lanes(h)]

    def whole(self, device):
        return self.full.at[pl.ds(self.first_row(device), self.rows)]


def barrier(side, far, partner):
    core, x, y = place(side)
    near = [number_of(core, x + a, y + b, side) for a, b in ((1, 0), (-1, 0), (0, 1), (0, -1))] if far else []
    if partner:
        near.append(number_of(1 - core, x, y, side))
    sem = pltpu.get_barrier_semaphore()
    for to in near:
        pl.semaphore_signal(sem, inc=1, device_id={"dp": to}, device_id_type=pl.DeviceIdType.MESH)
    pl.semaphore_wait(sem, len(near))


class Program:
    def __init__(self, side):
        self.side, self.count = side, 0

    def kernel(self, body, name, steps, ins, outs, shapes, scratch=(), flops=0, args=(), jobs=(), partner=False, alias=NONE):
        self.count += 1
        kinds = [j for j, _ in jobs]
        given = [x for j in kinds for x in j.given()]
        results = [x for j in kinds for x in j.results()]
        ends = [j.scratch() for j in kinds]
        sizes = [len(ins), len(given), len(outs), len(results), len(scratch)]
        talks = bool(jobs) or partner
        side = self.side

        def run(*refs):
            groups, at = [], 0
            for n in sizes:
                groups.append(refs[at : at + n])
                at += n
            own_in, job_in, own_out, job_out, own_scratch = groups
            todo = {}
            for (j, when), scr in zip(jobs, ends, strict=True):
                n, m = len(j.given()), len(j.results())
                j.bind(job_in[:n], job_out[:m], refs[at : at + len(scr)], side)
                job_in, job_out, at = job_in[n:], job_out[m:], at + len(scr)
                for order, (event, step) in enumerate(zip(j.events(), (*when, steps), strict=True)):
                    todo.setdefault((min(step, steps - 1), step >= steps), []).append((order, event))
            i = pl.program_id(0)

            @pl.when(i == 0)
            def _():
                if talks:
                    barrier(side, bool(jobs), partner or any(isinstance(j, Gather) for j in kinds))

            def perform(last):
                for (step, late), events in sorted(todo.items(), key=lambda e: e[FIRST]):
                    if late == last:

                        @pl.when(i == step)
                        def _(events=events):
                            for _, event in sorted(events, key=lambda e: e[FIRST]):
                                event()

            perform(False)
            body(*own_in, *own_out, *own_scratch)
            perform(True)

        size = sum(a.size * a.dtype.itemsize for a in args)
        extra = dict(collective_id=self.count, has_side_effects=True) if talks else {}
        got = pl.pallas_call(
            run,
            name=name,
            grid=(steps,),
            in_specs=[*ins, *[HBM] * len(given)],
            out_specs=[*outs, *[HBM] * len(results)],
            out_shape=[*shapes, *results],
            scratch_shapes=[*scratch, *[s for e in ends for s in e]],
            input_output_aliases=alias or {},
            compiler_params=pltpu.CompilerParams(dimension_semantics=("arbitrary",), vmem_limit_bytes=VMEM, **extra),
            cost_estimate=pl.CostEstimate(flops=flops, bytes_accessed=size, transcendentals=0),
        )(*args, *given)
        mine, rest = got[: len(outs)], got[len(outs) :]
        per_job = []
        for j in kinds:
            n = len(j.results())
            per_job.append(rest[:n])
            rest = rest[n:]
        return mine, per_job

    def carry(self, name, jobs):
        def body(out_ref):
            out_ref[...] = jnp.zeros_like(out_ref)

        spec = pl.BlockSpec((8, HEAD), lambda i: (0, 0))
        return self.kernel(body, name, 1, [], [spec], [struct((8, HEAD), f32)], jobs=[(j, [0] * (len(j.events()) - 1)) for j in jobs])[SECOND]


def front_body(h_ref, w_ref, wo_ref, cos_ref, sin_ref, qkv_ref, o_ref, lse_ref, mid_ref, a_s, qkv_s, acc_s, *, pairs):
    i = pl.program_id(0)

    @pl.when(i == 0)
    def _():
        a_s[...] = normed(h_ref[...])
        acc_s[...] = jnp.zeros_like(acc_s)

    def project(turn):
        for n in range(pairs):
            lanes = slice(n * COLS, (n + 1) * COLS)
            got = dot(a_s[...], w_ref[:, lanes]).astype(bf16)
            if turn:
                got = jnp.concatenate([turned(got[:, :HEAD], cos_ref, sin_ref), turned(got[:, HEAD:], cos_ref, sin_ref)], axis=1)
            qkv_ref[:, lanes] = got
            qkv_s[i * pairs + n] = got

    pl.when(i < 2)(lambda: project(True))
    pl.when(i == 2)(lambda: project(False))

    @pl.when(i > 2)
    def _():
        n = i - 3
        attend(qkv_s.at[n], qkv_s.at[pairs + n], qkv_s.at[2 * pairs + n], o_ref, lse_ref)
        acc_s[...] += dot(o_ref[...], wo_ref[...])

    @pl.when(i == pl.num_programs(0) - 1)
    def _():
        mid_ref[...] = plus(h_ref[...], acc_s[...])


def turned(t, cos_ref, sin_ref):
    t = t.astype(f32)
    return (t * cos_ref[...] + pltpu.roll(t, HEAD // 2, 1) * sin_ref[...]).astype(bf16)


def hides():
    return lax.broadcasted_iota(jnp.int32, (BQ, BQ), SECOND) >= lax.broadcasted_iota(jnp.int32, (BQ, BQ), FIRST)


def attend(q_ref, k_ref, v_ref, o_ref, lse_ref):
    t, heads = q_ref.shape[FIRST], q_ref.shape[SECOND] // HEAD
    scale = HEAD**-0.5
    e = scale * LOG2E
    seen = hides()
    for n in range(heads):
        lanes = slice(n * HEAD, (n + 1) * HEAD)
        for at in range(0, t, BQ):
            end = at + BQ
            s = dot_t(k_ref[:end, lanes], q_ref[at:end, lanes])
            low = jnp.where(seen, s[at:], HIDDEN)
            s = jnp.concatenate([s[:at], low], axis=0) if at else low
            top = s.max(axis=0, keepdims=True)
            p = jnp.exp2((s - top) * e)
            total = p.sum(axis=0, keepdims=True)
            out = dot(v_ref[:end, lanes].T, p.astype(bf16))
            o_ref[at:end, lanes] = (out * (1 / total)).T.astype(bf16)
            lse_ref[0, n : n + 1, at:end] = top * scale + jnp.log(total)


def front(program, h, wa, tables, jobs):
    t, d = h.shape
    q = wa.shape[SECOND] // 4
    pairs = q // COLS
    late = lambda i: jnp.maximum(i - 3, 0)
    first = lambda i: (0, jnp.minimum(i, 2))
    return program.kernel(
        functools.partial(front_body, pairs=pairs), "front", 3 + pairs,
        [still((t, d)), block((d, q), first), block((COLS, d), lambda i: (late(i), 3)), still((t, HEAD)), still((t, HEAD))],
        [block((t, q), first), block((t, COLS), lambda i: (0, late(i))), block((1, 2, t), lambda i: (late(i), 0, 0)), still((t, d))],
        [struct((t, 3 * q)), struct((t, q)), struct((pairs, 2, t), f32), struct((t, d))],
        [pltpu.VMEM((t, d), bf16), pltpu.VMEM((3 * pairs, t, COLS), bf16), pltpu.VMEM((t, d), f32)],
        8 * t * d * q + 3 * t * t * q, (h, wa, wa, *tables), jobs)


def mlp_body(h_ref, wg_ref, wd_ref, gu_ref, out_ref, b_s, acc_s):
    i = pl.program_id(0)

    @pl.when(i == 0)
    def _():
        b_s[...] = normed(h_ref[...])
        acc_s[...] = jnp.zeros_like(acc_s)

    p = []
    for n in range(wg_ref.shape[FIRST]):
        got = dot(b_s[...], wg_ref[n])
        gate, up = got[:, :COLS], got[:, COLS:]
        gu_ref[n] = got
        p.append((gate * jax.nn.sigmoid(gate) * up).astype(bf16))
    acc_s[...] += dot(jnp.concatenate(p, axis=1), wd_ref[...])

    @pl.when(i == pl.num_programs(0) - 1)
    def _():
        out_ref[...] = plus(h_ref[...], acc_s[...])


def mlp(program, h, wg, wd, jobs):
    (t, d), tiles = h.shape, wg.shape[FIRST]
    wide = lambda rows: block((2, rows, 2 * COLS), lambda i: (i, 0, 0))
    return program.kernel(
        mlp_body, "mlp", tiles // 2,
        [still((t, d)), wide(d), block((2 * COLS, d), lambda i: (i, 0))], [wide(t), still((t, d))],
        [struct((tiles, t, 2 * COLS), f32), struct((t, d))], [pltpu.VMEM((t, d), bf16), pltpu.VMEM((t, d), f32)],
        6 * t * d * tiles * COLS, (h, wg, wd), jobs)


def mlp_back_body(dh_ref, h_ref, wd_ref, wg_ref, gu_ref, out_ref, ug_ref, ud_ref, bt_s, acc_s, hold_g, hold_d, got_g, got_d, send_sem, recv_sem, *, side, rings):
    i = pl.program_id(0)
    last = pl.num_programs(0) - 1
    half = pl.num_programs(0) // 2
    for ring in rings:
        ring.src_ref = ug_ref
    core, x, y = place(side)
    other = number_of(1 - core, x, y, side)

    def sends(n):
        return [remote(hold.at[n % 2], got.at[n], send_sem.at[n, k], recv_sem.at[n, k], other) for k, (hold, got) in enumerate(((hold_g, got_g), (hold_d, got_d)))]

    def stores(n):
        own = n - half
        return [pltpu.make_async_copy(hold_g.at[n % 2], ug_ref.at[own], send_sem.at[n, FIRST]),
                pltpu.make_async_copy(hold_d.at[n % 2], ud_ref.at[pl.ds(own * COLS, COLS)], send_sem.at[n, SECOND])]

    def left(n):
        @pl.when(n < half)
        def _():
            for copy in sends(n):
                copy.wait_send()

        @pl.when(n >= half)
        def _():
            for copy in stores(n):
                copy.wait()
            for ring in rings:
                ring.go(n - half)

    @pl.when(i == 0)
    def _():
        bt_s[...] = normed(h_ref[...]).T
        acc_s[...] = jnp.zeros_like(acc_s)
        got_g[half] = jnp.zeros(got_g.shape[1:], bf16)
        got_d[half] = jnp.zeros(got_d.shape[1:], bf16)

    pl.when((i >= 2) & (i < half + 2))(lambda: left(i - 2))
    pl.when(i > half)(lambda: left(i - 1))

    @pl.when(i >= half)
    def _():
        for copy in sends(i - half):
            copy.wait_recv()

    came = jnp.where(i < half, half, i - half)
    dp = dot_t(dh_ref[...], wd_ref[...]).astype(bf16).astype(f32)
    gate, up = gu_ref[0, :, :COLS], gu_ref[0, :, COLS:]
    s = jax.nn.sigmoid(gate)
    silu = gate * s
    p = (silu * up).astype(bf16)
    by = jnp.concatenate([(dp * up * (s * (1 + gate * (1 - s)))).astype(bf16), (dp * silu).astype(bf16)], axis=1)
    hold_d[i % 2] = (dot(p.T, dh_ref[...]) + got_d[came].astype(f32)).astype(bf16)
    there = got_g[came].reshape(bt_s.shape[FIRST], -1).astype(f32)
    hold_g[i % 2] = (dot(bt_s[...], by) + there).astype(bf16).reshape(hold_g.shape[1:])
    acc_s[...] += dot_t(by, wg_ref[0])

    @pl.when(i < half)
    def _():
        for copy in sends(i):
            copy.start()

    @pl.when(i >= half)
    def _():
        for copy in stores(i):
            copy.start()

    @pl.when(i == last)
    def _():
        left(i)
        out_ref[...] = norm_back(h_ref[...], acc_s[...], dh_ref[...])


def mlp_back(program, dh, h, wd, wg, gu, jobs):
    (t, d), tiles = h.shape, wg.shape[FIRST]
    half = tiles // 2

    def tile(i):
        core = lax.axis_index("dp") % 2
        return jnp.where(i < half, (1 - core) * half + i, core * half + i - half)

    wide = lambda rows: block((1, rows, 2 * COLS), lambda i: (tile(i), 0, 0))
    side = program.side
    by_chip = (side, side, d // side // side, 2 * COLS)
    vmem = lambda n: [pltpu.VMEM((n, *by_chip), bf16), pltpu.VMEM((n, COLS, d), bf16)]
    rings = first_rings("raw", struct((half, *by_chip)), made=TileRing)
    (out, ug, ud), got = program.kernel(
        functools.partial(mlp_back_body, side=side, rings=rings), "mlp_back", tiles,
        [still((t, d)), still((t, d)), block((COLS, d), lambda i: (tile(i), 0)), wide(d), wide(t)], [still((t, d)), HBM, HBM],
        [struct((t, d)), struct((half, *by_chip)), struct((half * COLS, d))],
        [pltpu.VMEM((d, t), bf16), pltpu.VMEM((t, d), f32), *vmem(2), *vmem(half + 1), dma((tiles, 2)), dma((half, 2))],
        12 * t * d * tiles * COLS, (dh, h, wd, wg, gu), [*jobs, *((r, ()) for r in rings)], True)
    return out, ug, cut(ud[NONE], side), got[: len(jobs)], got[len(jobs) :]


def cut(u, side):
    return u.reshape(u.shape[FIRST], side, side, -1, u.shape[-1])


def attend_back_body(dh_ref, w_ref, o_ref, q_ref, k_ref, v_ref, lse_ref, cos_ref, sin_ref, out_ref, u_ref, do_s, dq_s, keep_s, got_s, send_sem, recv_sem, *, side):
    i = pl.program_id(0)
    pairs = pl.num_programs(0) // 2
    rows = keep_s.shape[SECOND]
    core, x, y = place(side)
    other = number_of(1 - core, x, y, side)
    copy = lambda n: remote(keep_s.at[n], got_s.at[n], send_sem.at[n], recv_sem.at[n], other)
    store = lambda n: pltpu.make_async_copy(keep_s.at[n], u_ref.at[FIRST, pl.ds(n * rows, rows)], send_sem.at[n])

    @pl.when(i < pairs)
    def _():
        do_s[i] = dot_t(dh_ref[...], w_ref[...]).astype(bf16)
        keep_s[i] = dot(o_ref[...].T, dh_ref[...]).astype(bf16)
        pl.when(core == 0)(lambda: copy(i).start())

    @pl.when(i >= pairs)
    def _():
        n = i - pairs
        pl.when(core == 0)(lambda: copy(n).wait_send())

        @pl.when(core == 1)
        def _():
            copy(n).wait_recv()
            keep_s[n] = (keep_s[n].astype(f32) + got_s[n].astype(f32)).astype(bf16)
            store(n).start()

        heads_back(q_ref, k_ref, v_ref, do_s.at[n], o_ref, lse_ref, cos_ref, sin_ref, out_ref, dq_s)
        pl.when(core == 1)(lambda: store(n).wait())


def heads_back(q_ref, k_ref, v_ref, do_ref, o_ref, lse_ref, cos_ref, sin_ref, out_ref, dq_s):
    t, heads = q_ref.shape[FIRST], q_ref.shape[SECOND] // HEAD
    scale = HEAD**-0.5
    e = scale * LOG2E
    seen = hides()

    def turned_back(x, rows):
        x = (x * scale).astype(bf16).astype(f32)
        return (x * cos_ref[rows, :] - pltpu.roll(x, HEAD // 2, 1) * sin_ref[rows, :]).astype(bf16)

    for n in range(heads):
        lanes = slice(n * HEAD, (n + 1) * HEAD)
        lse = lse_ref[0, n : n + 1, :] * LOG2E
        delta = (do_ref[:, lanes].astype(f32) * o_ref[:, lanes].astype(f32)).T.sum(axis=0, keepdims=True)
        for at in range(0, t, BQ):
            end = at + BQ
            k, v, q, do = k_ref[at:end, lanes], v_ref[at:end, lanes], q_ref[at:, lanes], do_ref[at:, lanes]
            p = jnp.exp2(dot_t(k, q) * e - lse[:, at:])
            low = jnp.where(seen, p[:, :BQ], 0.0)
            p = low if end == t else jnp.concatenate([low, p[:, BQ:]], axis=1)
            ds = (p * (dot_t(v, do) - delta[:, at:])).astype(bf16)
            out_ref[THIRD, at:end, lanes] = dot(p.astype(bf16), do).astype(bf16)
            out_ref[SECOND, at:end, lanes] = turned_back(dot(ds, q), slice(at, end))
            part = dot(k.T, ds)
            if at:
                dq_s[n, :, at:] += part
            else:
                dq_s[n] = part
        out_ref[FIRST, :, lanes] = turned_back(dq_s[n].T, slice(0, t))


def attend_back(program, dh, wa, qkv, o, lse, tables, jobs):
    (t, d), q = dh.shape, o.shape[SECOND]
    pairs = q // COLS
    late = lambda j: jnp.maximum(j - pairs, 0)
    head = lambda first: block((t, COLS), lambda j: (0, first + late(j)))
    tiles = [pltpu.VMEM((pairs, COLS, d), bf16)] * 2
    return program.kernel(
        functools.partial(attend_back_body, side=program.side), "attend_back", 2 * pairs,
        [still((t, d)), block((COLS, d), lambda j: (jnp.minimum(j, pairs - 1), 3)), block((t, COLS), lambda j: (0, j % pairs)),
         head(0), head(pairs), head(2 * pairs), block((1, 2, t), lambda j: (late(j), 0, 0)), still((t, HEAD)), still((t, HEAD))],
        [block((3, t, COLS), lambda j: (0, 0, late(j))), HBM], [struct((3, t, q)), struct((2, d, q))],
        [pltpu.VMEM((pairs, t, COLS), bf16), pltpu.VMEM((2, HEAD, t), f32), *tiles, dma((pairs,)), dma((pairs,))],
        4 * t * d * q + 7 * t * t * q, (dh, wa, o, qkv, qkv, qkv, lse, *tables), jobs, True)


def qkv_back_body(dh_ref, h_ref, d_ref, w_ref, _, out_ref, u_ref, at_s, acc_s, hold_s, got_s, send_sem, recv_sem, *, side):
    s = pl.program_id(0)
    last = pl.num_programs(0) - 1
    rows = w_ref.shape[FIRST]
    per = at_s.shape[FIRST] // rows
    r = s % per
    core, x, y = place(side)
    other = number_of(1 - core, x, y, side)
    sends = jnp.where(core == 0, per, 2 * per)
    zero = 2 * per

    def send(n):
        to = n + (1 - core) * per
        return remote(hold_s.at[n % 2], got_s.at[to], send_sem.at[n], recv_sem.at[to], other)

    def store(n):
        return pltpu.make_async_copy(hold_s.at[n % 2], u_ref.at[n // per - 1, pl.ds((n % per) * rows, rows)], send_sem.at[n])

    def left(n):
        pl.when(n < sends)(lambda: send(n).wait_send())
        pl.when(n >= sends)(lambda: store(n).wait())

    @pl.when(s == 0)
    def _():
        at_s[...] = normed(h_ref[...]).T
        acc_s[...] = jnp.zeros_like(acc_s)
        got_s[zero] = jnp.zeros(got_s.shape[1:], bf16)

    pl.when(s >= 2)(lambda: left(s - 2))

    @pl.when(s >= sends)
    def _():
        pltpu.make_async_copy(got_s.at[s - per], got_s.at[s - per], recv_sem.at[s - per]).wait()

    lanes = pl.ds(pl.multiple_of(r * rows, rows), rows)
    acc_s[:, lanes] += dot_t(d_ref[0], w_ref[...])
    came = jnp.where(s < sends, zero, s - per)
    hold_s[s % 2] = (dot(at_s[lanes, :], d_ref[0]) + got_s[came].astype(f32)).astype(bf16)
    pl.when(s < sends)(lambda: send(s).start())
    pl.when(s >= sends)(lambda: store(s).start())

    @pl.when(s == last)
    def _():
        out_ref[...] = norm_back(h_ref[...], acc_s[...], dh_ref[...])
        left(s - 1)
        left(s)


def qkv_back(program, dh, h, dqkv, wa, u, jobs):
    (t, d), q = h.shape, wa.shape[SECOND] // 4
    rows = COLS
    per = d // rows
    matrix = lambda s: (s // per + 2 * (1 - lax.axis_index("dp") % 2)) % 3
    (out, u), got = program.kernel(
        functools.partial(qkv_back_body, side=program.side), "qkv_back", 3 * per,
        [still((t, d)), still((t, d)), block((1, t, q), lambda s: (matrix(s), 0, 0)), block((rows, q), lambda s: (s % per, matrix(s))), HBM],
        [still((t, d)), HBM], [struct((t, d)), struct(u.shape)],
        [pltpu.VMEM((d, t), bf16), pltpu.VMEM((t, d), f32), pltpu.VMEM((2, rows, q), bf16), pltpu.VMEM((2 * per + 1, rows, q), bf16), dma((3 * per,)), dma((2 * per,))],
        12 * t * d * q, (dh, h, dqkv, wa, u), jobs, True, {4: 1})
    return out, cut(u, program.side), got


def tables_of(t):
    half = HEAD // 2
    angle = jnp.arange(t, dtype=f32)[:, None] * THETA ** (-jnp.arange(half, dtype=f32) / half)
    cos, sin = jnp.cos(angle), jnp.sin(angle)
    return jnp.concatenate([cos, cos], -1), jnp.concatenate([-sin, sin], -1)


def padded(rows):
    return -(-rows // 16) * 16


def pack(w_gate, w_up, w_down, n):
    rows = w_down.shape[SECOND]
    more = padded(rows) - rows

    def spread(w):
        layers, r = w.shape[:2]
        w = jnp.pad(w.reshape(layers, r, n // 2, 2, rows), ((0, 0),) * 4 + ((0, more),))
        return w.swapaxes(-2, -3).reshape(layers, r, -1, COLS).swapaxes(SECOND, THIRD)

    return jnp.concatenate([spread(w_gate), spread(w_up)], axis=-1), jnp.pad(w_down, ((0, 0), (0, more), (0, 0)))


def unpack(wg, n, rows):
    layers, r = wg.shape[FIRST], wg.shape[THIRD]

    def back(w):
        w = w.swapaxes(SECOND, THIRD).reshape(layers, r, 2, n // 2, -1)[..., :rows]
        return w.swapaxes(-2, -3).reshape(layers, r, n * rows)

    return back(wg[..., :COLS]), back(wg[..., COLS:])


def solution(mesh):
    n = mesh.shape["dp"]
    side = math.isqrt(n // 2)

    def step(x, dy, wq, wk, wv, wo, w_gate, w_up, w_down):
        program = Program(side)
        layers, rows = w_down.shape[:2]
        core = place(side)[FIRST]
        tables = tables_of(x.shape[SECOND])
        columns = jnp.concatenate([wq, wk, wv, wo], axis=-1)
        of_a = lambda number: GatherColumns(columns, number, n)
        ((wa,),) = program.carry("first", [of_a(0)])
        tiles, downs = pack(w_gate, w_up, w_down, n)
        of_g, of_d = (lambda number: GatherTiles(tiles, number, n)), (lambda number: GatherRows(downs, number, n))
        h, kept, wd = x[0], [], NONE
        for number in range(layers):
            jobs = [(of_g(number), FRONT)] if number else [(of_g(number), FRONT_BOTH), (of_d(number), FRONT_BOTH)]
            (qkv, o, lse, mid), got = front(program, h, wa, tables, jobs)
            wg, wd = got[FIRST][FIRST], wd if number else got[SECOND][FIRST]
            jobs = [] if number == layers - 1 else [(of_a(number + 1), MLP), (of_d(number + 1), MLP)]
            (gu, out), got = mlp(program, mid, wg, wd, jobs)
            kept.append((wa, wg, wd, h, qkv, o, lse, mid, gu))
            h = out
            if jobs:
                (wa,), (wd,) = got

        def close(got):
            return [ended(raw, own, sums) for _, raw, _, own, sums in got]

        def both(raw, mid):
            return close([(*r, *m) for r, m in zip(raw, mid, strict=True)])

        def whole(got):
            return jnp.concatenate([part[:, FIRST, FIRST] for part in close(got)], axis=-1)

        came = lambda raw: [r[FIRST] for r in raw]
        at = lambda steps, rings: [(r, steps) for r in rings]
        by_h, above = dy[0], NONE
        results = []
        for number in reversed(range(layers)):
            wa, wg, wd, hin, qkv, o, lse, mid, gu = kept[number]
            jobs = at(MLP_BACK, second_rings(above[FIRST]) + first_rings("ring", above[SECOND])) if above else []
            by_mid, ug, ud, got, raw_g = mlp_back(program, by_h, mid, wd, wg, gu, jobs)
            done_d, tail = (whole(got[:2]), second_rings(close(got[2:]))) if above else (NONE, [])
            jobs = at(ATTEND_BACK, first_rings("raw", ud) + first_rings("mid", ug, came(raw_g)))
            (dqkv, u), got = attend_back(program, by_mid, wa, qkv, o, lse, tables, jobs)
            raw_d, second_g = got[:2], second_rings(both(raw_g, got[2:]))
            jobs = at(QKV_BACK, first_rings("mid", ud, came(raw_d))) + at(QKV_BACK_RINGS, second_g + tail)
            by_h, ua, got = qkv_back(program, by_mid, hin, dqkv, wa, u, jobs)
            if above:
                results[-1] += [whole(got[4:]), done_d]
            results.append([whole(got[2:4])])
            above = both(raw_d, got[:2]), ua
        got = program.carry("tail", second_rings(above[FIRST]) + first_rings("ring", above[SECOND]))
        done_d, tail = whole(got[:2]), second_rings(close(got[2:]))
        results[-1] += [whole(program.carry("end", tail)), done_d]

        zg, za, zd = (jnp.stack(parts) for parts in zip(*reversed(results), strict=True))

        def swapped(z):
            z = z.reshape(*z.shape[:2], 2, -1, z.shape[-1])
            mine, other = (lax.dynamic_index_in_dim(z, c, 2, keepdims=False) for c in (core, 1 - core))
            got = lax.ppermute(other, "dp", [(b, b ^ 1) for b in range(n)])
            return jnp.where(core == 0, mine, got), jnp.where(core == 0, got, mine)

        qk, ov = swapped(za)
        by_gate, by_up = unpack(jnp.concatenate(swapped(zg), axis=SECOND), n, rows)
        by_down = zd.reshape(layers, -1, zd.shape[-1])[:, :rows]
        return by_h[None], qk[:, FIRST], qk[:, SECOND], ov[:, SECOND], ov[:, FIRST], by_gate, by_up, by_down

    states, cut_rows = P(("rep", "dp"), None, None), P(None, "dp", None)
    return jax.shard_map(
        step,
        mesh=mesh,
        in_specs=(states, states) + (cut_rows,) * 7,
        out_specs=(states,) + (P("rep", "dp", None),) * 7,
        check_vma=False,
    )


FRONT = (0, 2, 3, 7, 8)
FRONT_BOTH = (0, 2, 4, 8, 8)
MLP = (0, 2, 3, 7, 7)
MLP_BACK = (0, 5, 6, 7)
ATTEND_BACK = (0, 0, 1, 2)
QKV_BACK = (0, 0, 1, 2)
QKV_BACK_RINGS = (0, 7, 8, 9)
```

```python
import functools
import math

import jax
import jax.numpy as jnp
from jax import lax
from jax.experimental import pallas as pl
from jax.experimental.pallas import tpu as pltpu
from jax.sharding import PartitionSpec as P

HEAD = 128
THETA = 10000
EPS = 1e-6
LOG2E = 1.4426950408889634
HIDDEN = -2e30
VMEM = 62 * 2**20
COLS = 2 * HEAD
BQ = 256
HBM = pl.BlockSpec(memory_space=pl.ANY)
NONE, FIRST, SECOND, THIRD = None, 0, 1, 2
BOTH, FOUR = range(2), range(4)
HERE = (0, 0)

bf16, f32 = jnp.bfloat16, jnp.float32
dma = pltpu.SemaphoreType.DMA


def dot(a, b, ca=1, cb=0):
    return lax.dot_general(a, b, (((ca,), (cb,)), ((), ())), preferred_element_type=f32)


def dot_t(a, b):
    return dot(a, b, SECOND, SECOND)


def still(shape):
    return pl.BlockSpec(shape, lambda *_: (0,) * len(shape), pipeline_mode=pl.Buffered(SECOND))


def block(shape, where):
    return pl.BlockSpec(shape, where)


def struct(shape, dtype=bf16):
    return jax.ShapeDtypeStruct(shape, dtype)


def now():
    return pl.program_id(FIRST)


def count():
    return pl.num_programs(FIRST)


def scale_of(wide):
    return lax.rsqrt(jnp.mean(wide * wide, -1, keepdims=True) + EPS)


def normed(h):
    wide = h.astype(f32)
    return (wide * scale_of(wide)).astype(bf16)


def norm_back(h, by_a, by_h):
    wide = h.astype(f32)
    scale = scale_of(wide)
    by_a = by_a.astype(bf16).astype(f32)
    mine = scale * by_a - wide * (scale * scale * scale * jnp.mean(by_a * wide, -1, keepdims=True))
    return (by_h.astype(f32) + mine.astype(bf16).astype(f32)).astype(bf16)


def plus(h, part):
    return (h.astype(f32) + part.astype(bf16).astype(f32)).astype(bf16)


def place(side):
    me = lax.axis_index("dp")
    core, chip = me % 2, me // 2
    return core, chip // side, chip % side


def number_of(core, x, y, side):
    return (((x + side) % side) * side + (y + side) % side) * 2 + core


def remote(src, dst, send, recv, to):
    return pltpu.make_async_remote_copy(src_ref=src, dst_ref=dst, send_sem=send, recv_sem=recv, device_id={"dp": to}, device_id_type=pl.DeviceIdType.MESH)


class Ring:
    def __init__(self, kind, axis, src, dim, came=NONE, tiles=NONE, lanes=NONE):
        self.kind, self.axis, self.src, self.dim, self.came = kind, axis, src, dim, came
        self.tiles, lanes = tiles or (FIRST, src.shape[FIRST]), lanes or (FIRST, src.shape[-1])
        self.rows, self.lanes = src.shape[3] // 2, pl.ds(*lanes)
        self.shape = (self.tiles[SECOND], src.shape[3 - dim], 2, self.rows, lanes[SECOND])
        self.raw, self.mid = kind != "mid", kind != "raw"

    def given(self):
        return [self.src] + ([] if self.raw else [self.came])

    def results(self):
        return [struct(self.shape)] * (2 * self.raw + 3 * self.mid)

    def scratch(self):
        got = [dma((4,)), dma((4,))] if self.raw else []
        return got + ([dma((2,)), dma((2,)), dma((7,)), pltpu.VMEM((3, *self.shape), bf16)] if self.mid else [])

    def bind(self, given, results, scratch, side):
        core, x, y = place(side)
        self.side, self.at = side, x if self.axis == "x" else y
        near = lambda by: number_of(core, x + by, y, side) if self.axis == "x" else number_of(core, x, y + by, side)
        self.right, self.left = near(1), near(-1)
        results, scratch = list(results), list(scratch)
        if given:
            self.src_ref = given[FIRST]
        if self.raw:
            self.came_ref, self.raw_ref = results[:2]
            self.send, self.recv = scratch[:2]
        else:
            self.came_ref = given[SECOND]
        if self.mid:
            self.held_ref, self.own_ref, self.sums_ref = results[-3:]
            self.send2, self.recv2, self.local, self.buf = scratch[-4:]

    def part(self, by, half, t=NONE):
        k = (self.at + by + self.side) % self.side
        ts = pl.ds(*self.tiles) if t is NONE else pl.ds(self.tiles[FIRST] + t, 1)
        rows = pl.ds(half * self.rows, self.rows)
        return self.src_ref.at[ts, k, :, rows, self.lanes] if self.dim == SECOND else self.src_ref.at[ts, :, k, rows, self.lanes]

    def raws(self, n, t=NONE):
        by, half, ref, to = ((2, FIRST, self.came_ref, self.right), (2, SECOND, self.came_ref, self.left),
                             (SECOND, SECOND, self.raw_ref, self.right), (-1, FIRST, self.raw_ref, self.left))[n]
        ts, sem = (slice(NONE), ()) if t is NONE else (pl.ds(t, 1), (t,))
        return remote(self.part(by, half, t), ref.at[ts, :, half], self.send.at[n, *sem], self.recv.at[n, *sem], to)

    def mids(self, half):
        return remote(self.held_ref.at[:, :, half], self.sums_ref.at[:, :, half], self.send2.at[half], self.recv2.at[half], self.left if half else self.right)

    def load(self, n):
        if n == THIRD:
            return pltpu.make_async_copy(self.came_ref, self.buf.at[SECOND], self.local.at[n])
        if n > THIRD:
            return pltpu.make_async_copy(self.part(FIRST, n - 3), self.buf.at[THIRD, :, :, n - 3], self.local.at[n])
        return pltpu.make_async_copy(self.part(-1 if n else SECOND, n), self.buf.at[FIRST, :, :, n], self.local.at[n])

    def stores(self):
        return [pltpu.make_async_copy(self.buf.at[FIRST], self.held_ref, self.local.at[5]), pltpu.make_async_copy(self.buf.at[THIRD], self.own_ref, self.local.at[6])]

    def start(self):
        if self.raw:
            for n in FOUR:
                self.raws(n).start()

    def turn(self):
        if self.raw and self.mid:
            for n in BOTH:
                self.raws(n).wait_recv()
        if self.mid:
            for n in range(5):
                self.load(n).start()

    def add(self):
        if not self.mid:
            return
        for n in range(5):
            self.load(n).wait()
        for t in range(self.shape[FIRST]):
            for i in range(self.shape[SECOND]):
                self.buf[FIRST, t, i] = (self.buf[FIRST, t, i].astype(f32) + self.buf[SECOND, t, i].astype(f32)).astype(bf16)
        for copy in self.stores():
            copy.start()

    def pass_on(self):
        if self.mid:
            for copy in self.stores():
                copy.wait()
            for half in BOTH:
                self.mids(half).start()

    def finish(self):
        if self.raw:
            for n in FOUR:
                self.raws(n).wait_send()
                if n >= 2 or not self.mid:
                    self.raws(n).wait_recv()
        if self.mid:
            for half in BOTH:
                self.mids(half).wait()

    def events(self):
        return self.start, self.turn, self.add, self.pass_on, self.finish


class OwnRing(Ring):
    def given(self):
        return []

    def events(self):
        return self.start, self.finish


class TileRing(OwnRing):
    def scratch(self):
        return [dma((4, self.shape[FIRST]))] * 2

    def go(self, t):
        for n in FOUR:
            self.raws(n, t).start()

    def finish(self):
        for t in range(self.shape[FIRST]):
            for n in FOUR:
                self.raws(n, t).wait()

    def events(self):
        return (self.finish,)


def first_rings(kind, u, came=(NONE, NONE), made=Ring):
    if isinstance(u, tuple):
        return [made(kind, "x", u[FIRST], SECOND, came[FIRST]), made(kind, "y", u[SECOND], THIRD, came[SECOND])]
    t, w = u.shape[FIRST], u.shape[-1] // 2
    cut = (t + 1) // 2
    parts = [dict(tiles=(FIRST, cut)), dict(tiles=(cut, t - cut))] if t > cut else [dict(lanes=(FIRST, w)), dict(lanes=(w, w))]
    return [made(kind, axis, u, dim, c, **part) for axis, dim, c, part in zip("xy", (SECOND, THIRD), came, parts, strict=True)]


def second_rings(v):
    return [Ring("ring", axis, part, SECOND) for axis, part in zip("yx", v, strict=True)]


def ended(raw, own, sums):
    got = (own.astype(f32) + raw.astype(f32) + sums.astype(f32)).astype(bf16)
    return got.reshape(*got.shape[:2], 1, -1, got.shape[-1])


NEAR = (0, 1, -1, 2)


class Gather:
    def __init__(self, source, layer, shape):
        self.source, self.layer, self.shape = source, layer, shape

    def given(self):
        return [self.source]

    def results(self):
        return [struct(self.shape)]

    def scratch(self):
        return [dma, dma((2, 36)), dma((2, 36))]

    def bind(self, given, results, scratch, side):
        self.side, self.me = side, place(side)
        (self.from_ref,), (self.full,), (self.local, self.send, self.recv) = given, results, scratch

    def own(self):
        return pltpu.make_async_copy(self.from_ref.at[self.layer], self.whole(number_of(*self.me, self.side)), self.local)

    def spot(self, h, di, dj):
        _, x, y = self.me
        return (x + di, y + dj) if h == FIRST else (x + dj, y + di)

    def move(self, h, k, which, to, quarter=NONE, other=False):
        core = self.me[FIRST]
        share = self.view(number_of(core, *self.spot(h, *which), self.side), h, quarter)
        return remote(share if any(which) else self.mine(h), share, self.send.at[h, k], self.recv.at[h, k], number_of(1 - core if other else core, *self.spot(h, *to), self.side))

    def near(self, h):
        return [self.move(h, k, HERE, (1 - 2 * k, 0)) for k in BOTH]

    def far(self, h):
        return [self.move(h, 2 + k, (2 * k - 1, 0), (1 - 2 * k, 0), k) for k in BOTH]

    def side_ways(self, h, a):
        return [self.move(h, 4 + 2 * a + k, (NEAR[a], 0), (0, 1 - 2 * k)) for k in BOTH]

    def over(self, h, a):
        return [self.move(h, 12 + 2 * a + k, (NEAR[a], 2 * k - 1), (0, 1 - 2 * k), k) for k in BOTH]

    def twin(self, h, a, b):
        return [self.move(h, 20 + 4 * a + b, (NEAR[a], NEAR[b]), HERE, NONE, True)]

    def go(self, what, *places):
        for h in BOTH:
            for a in places:
                for copy in what(h, *a):
                    copy.start()

    def come(self, what, *places):
        for h in BOTH:
            for a in places:
                for copy in what(h, *a):
                    copy.wait_recv()

    def begin(self):
        self.go(self.near, ())
        self.go(self.side_ways, (0,))
        self.go(self.twin, HERE)
        self.own().start()

    def row(self):
        self.come(self.near, ())
        self.go(self.far, ())
        self.go(self.side_ways, (1,), (2,))
        self.go(self.twin, (1, 0), (2, 0))

    def row_end(self):
        self.come(self.far, ())
        self.go(self.side_ways, (3,))
        self.go(self.twin, (3, 0))
        self.come(self.side_ways, (0,))
        self.go(self.over, (0,))

    def plane(self):
        self.come(self.side_ways, (1,), (2,))
        self.go(self.over, (1,), (2,))
        self.go(self.twin, *((a, b) for a in (0, 1, 2) for b in (1, 2)))

    def plane_rest(self):
        self.come(self.side_ways, (3,))
        self.go(self.over, (3,))
        self.go(self.twin, (3, 1), (3, 2))

    def plane_end(self):
        self.come(self.over, *((a,) for a in FOUR))
        self.go(self.twin, *((a, 3) for a in FOUR))

    def finish(self):
        every = [(a, b) for a in FOUR for b in FOUR]
        self.come(self.twin, *every)
        self.own().wait()
        for what, places in ((self.near, [()]), (self.far, [()]), (self.side_ways, [(a,) for a in FOUR]), (self.over, [(a,) for a in FOUR]), (self.twin, every)):
            for h in BOTH:
                for a in places:
                    for copy in what(h, *a):
                        copy.wait_send()

    def events(self):
        return self.begin, self.row, self.row_end, self.plane, self.plane_rest, self.plane_end, self.finish


class GatherColumns(Gather):
    def __init__(self, source, layer, n):
        _, self.rows, self.width = source.shape
        super().__init__(source, layer, (self.rows * n, self.width))

    def lanes(self, h, quarter):
        part = self.width // 4
        return pl.ds((2 * h + (quarter or 0)) * part, part * (2 if quarter is NONE else 1))

    def view(self, device, h, quarter):
        return self.full.at[pl.ds(device * self.rows, self.rows), self.lanes(h, quarter)]

    def mine(self, h):
        return self.from_ref.at[self.layer, :, self.lanes(h, NONE)]

    def whole(self, device):
        return self.full.at[pl.ds(device * self.rows, self.rows)]


class GatherTiles(Gather):
    def __init__(self, source, layer, n):
        _, self.tiles, self.rows, width = source.shape
        super().__init__(source, layer, (self.tiles, self.rows * n, width))

    def range(self, h, quarter):
        half = self.tiles // 2
        cut = (half + 1) // 2
        first, count = ((0, half), (0, cut), (cut, half - cut))[0 if quarter is NONE else quarter + 1]
        return pl.ds(h * half + first, count)

    def view(self, device, h, quarter):
        return self.full.at[self.range(h, quarter), pl.ds(device * self.rows, self.rows)]

    def mine(self, h):
        return self.from_ref.at[self.layer, self.range(h, NONE)]

    def whole(self, device):
        return self.full.at[:, pl.ds(device * self.rows, self.rows)]


class GatherRows(Gather):
    def __init__(self, source, layer, n):
        _, self.rows, self.width = source.shape
        super().__init__(source, layer, (self.rows * n, self.width))

    def first_row(self, device):
        return ((device % 2) * self.side * self.side + device // 2) * self.rows

    def lanes(self, h):
        return pl.ds(h * (self.width // 2), self.width // 2)

    def view(self, device, h, quarter):
        part = self.rows // 2
        rows = pl.ds(self.first_row(device) + (quarter or 0) * part, self.rows if quarter is NONE else part)
        return self.full.at[rows, self.lanes(h)]

    def mine(self, h):
        return self.from_ref.at[self.layer, :, self.lanes(h)]

    def whole(self, device):
        return self.full.at[pl.ds(self.first_row(device), self.rows)]


def barrier(side, far, partner):
    core, x, y = place(side)
    near = [number_of(core, x + a, y + b, side) for a, b in ((1, 0), (-1, 0), (0, 1), (0, -1))] if far else []
    if partner:
        near.append(number_of(1 - core, x, y, side))
    sem = pltpu.get_barrier_semaphore()
    for to in near:
        pl.semaphore_signal(sem, inc=1, device_id={"dp": to}, device_id_type=pl.DeviceIdType.MESH)
    pl.semaphore_wait(sem, len(near))


class Program:
    def __init__(self, side):
        self.side, self.count = side, 0

    def kernel(self, body, name, steps, ins, outs, shapes, scratch=(), flops=0, args=(), jobs=(), partner=False, alias=NONE):
        self.count += 1
        kinds = [j for j, _ in jobs]
        given = [x for j in kinds for x in j.given()]
        results = [x for j in kinds for x in j.results()]
        ends = [j.scratch() for j in kinds]
        sizes = [len(ins), len(given), len(outs), len(results), len(scratch)]
        talks = bool(jobs) or partner
        side = self.side

        def run(*refs):
            groups, at = [], 0
            for n in sizes:
                groups.append(refs[at : at + n])
                at += n
            own_in, job_in, own_out, job_out, own_scratch = groups
            todo = {}
            for (j, when), scr in zip(jobs, ends, strict=True):
                n, m = len(j.given()), len(j.results())
                j.bind(job_in[:n], job_out[:m], refs[at : at + len(scr)], side)
                job_in, job_out, at = job_in[n:], job_out[m:], at + len(scr)
                if isinstance(j, OwnRing):
                    j.src_ref = own_out[j.source]
                for order, (event, step) in enumerate(zip(j.events(), (*when, steps), strict=True)):
                    todo.setdefault((min(step, steps - 1), step >= steps), []).append((order, event))
            i = now()

            @pl.when(i == FIRST)
            def _():
                if talks:
                    barrier(side, bool(jobs), partner or any(isinstance(j, Gather) for j in kinds))

            def perform(last):
                for (step, late), events in sorted(todo.items(), key=lambda e: e[FIRST]):
                    if late == last:

                        @pl.when(i == step)
                        def _(events=events):
                            for _, event in sorted(events, key=lambda e: e[FIRST]):
                                event()

            perform(False)
            body(*own_in, *own_out, *own_scratch)
            perform(True)

        size = sum(a.size * a.dtype.itemsize for a in args)
        extra = dict(collective_id=self.count, has_side_effects=True) if talks else {}
        got = pl.pallas_call(
            run,
            name=name,
            grid=(steps,),
            in_specs=[*ins, *[HBM] * len(given)],
            out_specs=[*outs, *[HBM] * len(results)],
            out_shape=[*shapes, *results],
            scratch_shapes=[*scratch, *[s for e in ends for s in e]],
            input_output_aliases=alias or {},
            compiler_params=pltpu.CompilerParams(dimension_semantics=("arbitrary",), vmem_limit_bytes=VMEM, **extra),
            cost_estimate=pl.CostEstimate(flops=flops, bytes_accessed=size, transcendentals=0),
        )(*args, *given)
        mine, rest = got[: len(outs)], got[len(outs) :]
        per_job = []
        for j in kinds:
            n = len(j.results())
            per_job.append(rest[:n])
            rest = rest[n:]
        return mine, per_job

    def carry(self, name, jobs):
        def body(out_ref):
            out_ref[...] = jnp.zeros_like(out_ref)

        spec = pl.BlockSpec((8, HEAD), lambda i: (0, 0))
        return self.kernel(body, name, 1, [], [spec], [struct((8, HEAD), f32)], jobs=[(j, [0] * (len(j.events()) - 1)) for j in jobs])[SECOND]


def front_body(h_ref, w_ref, wo_ref, cos_ref, sin_ref, qkv_ref, o_ref, lse_ref, mid_ref, a_s, qkv_s, acc_s, *, pairs):
    i = now()

    @pl.when(i == FIRST)
    def _():
        a_s[...] = normed(h_ref[...])
        acc_s[...] = jnp.zeros_like(acc_s)

    def project(turn):
        for n in range(pairs):
            lanes = slice(n * COLS, (n + 1) * COLS)
            got = dot(a_s[...], w_ref[:, lanes]).astype(bf16)
            if turn:
                got = jnp.concatenate([turned(got[:, :HEAD], cos_ref, sin_ref), turned(got[:, HEAD:], cos_ref, sin_ref)], axis=1)
            qkv_ref[:, lanes] = got
            qkv_s[i * pairs + n] = got

    pl.when(i < 2)(lambda: project(True))
    pl.when(i == 2)(lambda: project(False))

    @pl.when(i > 2)
    def _():
        n = i - 3
        attend(qkv_s.at[n], qkv_s.at[pairs + n], qkv_s.at[2 * pairs + n], o_ref, lse_ref)
        acc_s[...] += dot(o_ref[...], wo_ref[...])

    @pl.when(i == count() - 1)
    def _():
        mid_ref[...] = plus(h_ref[...], acc_s[...])


def turned(t, cos_ref, sin_ref):
    t = t.astype(f32)
    return (t * cos_ref[...] + pltpu.roll(t, HEAD // 2, 1) * sin_ref[...]).astype(bf16)


def hides():
    return lax.broadcasted_iota(jnp.int32, (BQ, BQ), SECOND) >= lax.broadcasted_iota(jnp.int32, (BQ, BQ), FIRST)


def attend(q_ref, k_ref, v_ref, o_ref, lse_ref):
    t, heads = q_ref.shape[FIRST], q_ref.shape[SECOND] // HEAD
    scale = HEAD**-0.5
    e = scale * LOG2E
    seen = hides()
    for n in range(heads):
        lanes = slice(n * HEAD, (n + 1) * HEAD)
        for at in range(0, t, BQ):
            end = at + BQ
            s = dot_t(k_ref[:end, lanes], q_ref[at:end, lanes])
            low = jnp.where(seen, s[at:], HIDDEN)
            s = jnp.concatenate([s[:at], low], axis=0) if at else low
            top = s.max(axis=0, keepdims=True)
            p = jnp.exp2((s - top) * e)
            total = p.sum(axis=0, keepdims=True)
            out = dot(v_ref[:end, lanes].T, p.astype(bf16))
            o_ref[at:end, lanes] = (out * (1 / total)).T.astype(bf16)
            lse_ref[0, n : n + 1, at:end] = top * scale + jnp.log(total)


def front(program, h, wa, tables, jobs):
    t, d = h.shape
    q = wa.shape[SECOND] // 4
    pairs = q // COLS
    late = lambda i: jnp.maximum(i - 3, 0)
    first = lambda i: (0, jnp.minimum(i, 2))
    return program.kernel(
        functools.partial(front_body, pairs=pairs), "front", 3 + pairs,
        [still((t, d)), block((d, q), first), block((COLS, d), lambda i: (late(i), 3)), still((t, HEAD)), still((t, HEAD))],
        [block((t, q), first), block((t, COLS), lambda i: (0, late(i))), block((1, 2, t), lambda i: (late(i), 0, 0)), still((t, d))],
        [struct((t, 3 * q)), struct((t, q)), struct((pairs, 2, t), f32), struct((t, d))],
        [pltpu.VMEM((t, d), bf16), pltpu.VMEM((3 * pairs, t, COLS), bf16), pltpu.VMEM((t, d), f32)],
        8 * t * d * q + 3 * t * t * q, (h, wa, wa, *tables), jobs)


def mlp_body(h_ref, wg_ref, wd_ref, gu_ref, out_ref, b_s, acc_s):
    i = now()

    @pl.when(i == FIRST)
    def _():
        b_s[...] = normed(h_ref[...])
        acc_s[...] = jnp.zeros_like(acc_s)

    p = []
    for n in range(wg_ref.shape[FIRST]):
        got = dot(b_s[...], wg_ref[n])
        gate, up = got[:, :COLS], got[:, COLS:]
        gu_ref[n] = got
        p.append((gate * jax.nn.sigmoid(gate) * up).astype(bf16))
    acc_s[...] += dot(jnp.concatenate(p, axis=1), wd_ref[...])

    @pl.when(i == count() - 1)
    def _():
        out_ref[...] = plus(h_ref[...], acc_s[...])


def mlp(program, h, wg, wd, jobs):
    (t, d), tiles = h.shape, wg.shape[FIRST]
    wide = lambda rows: block((2, rows, 2 * COLS), lambda i: (i, 0, 0))
    return program.kernel(
        mlp_body, "mlp", tiles // 2,
        [still((t, d)), wide(d), block((2 * COLS, d), lambda i: (i, 0))], [wide(t), still((t, d))],
        [struct((tiles, t, 2 * COLS), f32), struct((t, d))], [pltpu.VMEM((t, d), bf16), pltpu.VMEM((t, d), f32)],
        6 * t * d * tiles * COLS, (h, wg, wd), jobs)


def mlp_back_body(dh_ref, h_ref, wd_ref, wg_ref, gu_ref, out_ref, ug_ref, ud_ref, bt_s, acc_s, hold_g, hold_d, got_g, got_d, send_sem, recv_sem, *, side, rings):
    i = now()
    last = count() - 1
    half = count() // 2
    core, x, y = place(side)
    other = number_of(1 - core, x, y, side)

    def sends(n):
        return [remote(hold.at[n % 2], got.at[n], send_sem.at[n, k], recv_sem.at[n, k], other) for k, (hold, got) in enumerate(((hold_g, got_g), (hold_d, got_d)))]

    def stores(n):
        own = turn_of(n - half, half)
        return [pltpu.make_async_copy(hold_g.at[n % 2], ug_ref.at[own], send_sem.at[n, FIRST]),
                pltpu.make_async_copy(hold_d.at[n % 2], ud_ref.at[pl.ds(own * COLS, COLS)], send_sem.at[n, SECOND])]

    def left(n):
        @pl.when(n < half)
        def _():
            for copy in sends(n):
                copy.wait_send()

        @pl.when(n >= half)
        def _():
            for copy in stores(n):
                copy.wait()
            for k, ring in enumerate(rings):
                pl.when((n - half) % 2 == k)(functools.partial(ring.go, (n - half) // 2))

    @pl.when(i == FIRST)
    def _():
        bt_s[...] = normed(h_ref[...]).T
        acc_s[...] = jnp.zeros_like(acc_s)
        got_g[half] = jnp.zeros(got_g.shape[1:], bf16)
        got_d[half] = jnp.zeros(got_d.shape[1:], bf16)

    pl.when((i >= 2) & (i < half + 2))(lambda: left(i - 2))
    pl.when(i > half)(lambda: left(i - 1))

    @pl.when(i >= half)
    def _():
        for copy in sends(i - half):
            copy.wait_recv()

    came = jnp.where(i < half, half, i - half)
    dp = dot_t(dh_ref[...], wd_ref[...]).astype(bf16).astype(f32)
    gate, up = gu_ref[0, :, :COLS], gu_ref[0, :, COLS:]
    s = jax.nn.sigmoid(gate)
    silu = gate * s
    p = (silu * up).astype(bf16)
    by = jnp.concatenate([(dp * up * (s * (1 + gate * (1 - s)))).astype(bf16), (dp * silu).astype(bf16)], axis=1)
    hold_d[i % 2] = (dot(p.T, dh_ref[...]) + got_d[came].astype(f32)).astype(bf16)
    there = got_g[came].reshape(bt_s.shape[FIRST], -1).astype(f32)
    hold_g[i % 2] = (dot(bt_s[...], by) + there).astype(bf16).reshape(hold_g.shape[1:])
    acc_s[...] += dot_t(by, wg_ref[0])

    @pl.when(i < half)
    def _():
        for copy in sends(i):
            copy.start()

    @pl.when(i >= half)
    def _():
        for copy in stores(i):
            copy.start()

    @pl.when(i == last)
    def _():
        left(i)
        out_ref[...] = norm_back(h_ref[...], acc_s[...], dh_ref[...])


def turn_of(n, tiles):
    return n // 2 + (n % 2) * ((tiles + 1) // 2)


def mlp_back(program, dh, h, wd, wg, gu, jobs):
    (t, d), tiles = h.shape, wg.shape[FIRST]
    half = tiles // 2

    def tile(i):
        core = lax.axis_index("dp") % 2
        return jnp.where(i < half, (1 - core) * half + turn_of(i, half), core * half + turn_of(i - half, half))

    wide = lambda rows: block((1, rows, 2 * COLS), lambda i: (tile(i), 0, 0))
    side = program.side
    by_chip = (side, side, d // side // side, 2 * COLS)
    vmem = lambda n: [pltpu.VMEM((n, *by_chip), bf16), pltpu.VMEM((n, COLS, d), bf16)]
    rings = first_rings("raw", struct((half, *by_chip)), made=TileRing)
    for ring in rings:
        ring.source = SECOND
    (out, ug, ud), got = program.kernel(
        functools.partial(mlp_back_body, side=side, rings=rings), "mlp_back", tiles,
        [still((t, d)), still((t, d)), block((COLS, d), lambda i: (tile(i), 0)), wide(d), wide(t)], [still((t, d)), HBM, HBM],
        [struct((t, d)), struct((half, *by_chip)), struct((half * COLS, d))],
        [pltpu.VMEM((d, t), bf16), pltpu.VMEM((t, d), f32), *vmem(2), *vmem(half + 1), dma((tiles, 2)), dma((half, 2))],
        12 * t * d * tiles * COLS, (dh, h, wd, wg, gu), [*jobs, *((r, ()) for r in rings)], True)
    return out, ug, cut(ud, side), got[: len(jobs)], got[len(jobs) :]


def cut(u, side):
    return u.reshape(1, side, side, -1, u.shape[-1])


def attend_back_body(dh_ref, w_ref, o_ref, q_ref, k_ref, v_ref, lse_ref, cos_ref, sin_ref, out_ref, u_ref, do_s, dq_s, keep_s, got_s, send_sem, recv_sem, *, side):
    i = now()
    pairs = count() // 2
    rows = keep_s.shape[SECOND]
    core, x, y = place(side)
    other = number_of(1 - core, x, y, side)
    copy = lambda n: remote(keep_s.at[n], got_s.at[n], send_sem.at[n], recv_sem.at[n], other)
    store = lambda n: pltpu.make_async_copy(keep_s.at[n], u_ref.at[pl.ds(n * rows, rows)], send_sem.at[n])

    @pl.when(i < pairs)
    def _():
        do_s[i] = dot_t(dh_ref[...], w_ref[...]).astype(bf16)
        keep_s[i] = dot(o_ref[...].T, dh_ref[...]).astype(bf16)
        pl.when(core == FIRST)(lambda: copy(i).start())

    @pl.when(i >= pairs)
    def _():
        n = i - pairs
        pl.when(core == FIRST)(lambda: copy(n).wait_send())

        @pl.when(core == SECOND)
        def _():
            copy(n).wait_recv()
            keep_s[n] = (keep_s[n].astype(f32) + got_s[n].astype(f32)).astype(bf16)
            store(n).start()

        heads_back(q_ref, k_ref, v_ref, do_s.at[n], o_ref, lse_ref, cos_ref, sin_ref, out_ref, dq_s)
        pl.when(core == SECOND)(lambda: store(n).wait())


def heads_back(q_ref, k_ref, v_ref, do_ref, o_ref, lse_ref, cos_ref, sin_ref, out_ref, dq_s):
    t, heads = q_ref.shape[FIRST], q_ref.shape[SECOND] // HEAD
    scale = HEAD**-0.5
    e = scale * LOG2E
    seen = hides()

    def turned_back(x, rows):
        x = (x * scale).astype(bf16).astype(f32)
        return (x * cos_ref[rows, :] - pltpu.roll(x, HEAD // 2, 1) * sin_ref[rows, :]).astype(bf16)

    for n in range(heads):
        lanes = slice(n * HEAD, (n + 1) * HEAD)
        lse = lse_ref[0, n : n + 1, :] * LOG2E
        delta = (do_ref[:, lanes].astype(f32) * o_ref[:, lanes].astype(f32)).T.sum(axis=0, keepdims=True)
        for at in range(0, t, BQ):
            end = at + BQ
            k, v, q, do = k_ref[at:end, lanes], v_ref[at:end, lanes], q_ref[at:, lanes], do_ref[at:, lanes]
            p = jnp.exp2(dot_t(k, q) * e - lse[:, at:])
            low = jnp.where(seen, p[:, :BQ], 0.0)
            p = low if end == t else jnp.concatenate([low, p[:, BQ:]], axis=1)
            ds = (p * (dot_t(v, do) - delta[:, at:])).astype(bf16)
            out_ref[THIRD, at:end, lanes] = dot(p.astype(bf16), do).astype(bf16)
            out_ref[SECOND, at:end, lanes] = turned_back(dot(ds, q), slice(at, end))
            part = dot(k.T, ds)
            if at:
                dq_s[n, :, at:] += part
            else:
                dq_s[n] = part
        out_ref[FIRST, :, lanes] = turned_back(dq_s[n].T, slice(0, t))


def attend_back(program, dh, wa, qkv, o, lse, tables, jobs):
    (t, d), q = dh.shape, o.shape[SECOND]
    pairs = q // COLS
    late = lambda j: jnp.maximum(j - pairs, 0)
    head = lambda first: block((t, COLS), lambda j: (0, first + late(j)))
    tiles = [pltpu.VMEM((pairs, COLS, d), bf16)] * 2
    return program.kernel(
        functools.partial(attend_back_body, side=program.side), "attend_back", 2 * pairs,
        [still((t, d)), block((COLS, d), lambda j: (jnp.minimum(j, pairs - 1), 3)), block((t, COLS), lambda j: (0, j % pairs)),
         head(0), head(pairs), head(2 * pairs), block((1, 2, t), lambda j: (late(j), 0, 0)), still((t, HEAD)), still((t, HEAD))],
        [block((3, t, COLS), lambda j: (0, 0, late(j))), HBM], [struct((3, t, q)), struct((q, d))],
        [pltpu.VMEM((pairs, t, COLS), bf16), pltpu.VMEM((2, HEAD, t), f32), *tiles, dma((pairs,)), dma((pairs,))],
        4 * t * d * q + 7 * t * t * q, (dh, wa, o, qkv, qkv, qkv, lse, *tables), jobs, True)


def qkv_back_body(dh_ref, h_ref, d_ref, wq_ref, wk_ref, wv_ref, _, out_ref, u0_ref, u1_ref, at_s, acc_s, hold_s, got_s, send_sem, recv_sem, *, side):
    s = now()
    last = count() - 1
    per = side
    rows = at_s.shape[FIRST] // per
    core, x, y = place(side)
    other = number_of(1 - core, x, y, side)
    sends = jnp.where(core == FIRST, per, 2 * per)
    zero, tiles = 2 * per, 3 * per

    def send(n):
        to = n + (1 - core) * per
        return remote(hold_s.at[n % 2], got_s.at[to], send_sem.at[n], recv_sem.at[to], other)

    def store(n, ref):
        return pltpu.make_async_copy(hold_s.at[n % 2], ref.at[0, n % per], send_sem.at[n])

    def stored(n, do):
        pl.when((n >= sends) & (n < 2 * per))(lambda: do(store(n, u0_ref)))
        pl.when(n >= 2 * per)(lambda: do(store(n, u1_ref)))

    def left(n):
        pl.when(n < sends)(lambda: send(n).wait_send())
        stored(n, lambda copy: copy.wait())

    @pl.when(s == FIRST)
    def _():
        at_s[...] = normed(h_ref[...]).T
        got_s[zero] = jnp.zeros(got_s.shape[1:], bf16)

    pl.when((s >= 2) & (s < tiles))(lambda: left(s - 2))

    @pl.when((s >= sends) & (s < tiles))
    def _():
        pltpu.make_async_copy(got_s.at[s - per], got_s.at[s - per], recv_sem.at[s - per]).wait()

    @pl.when(s < tiles)
    def _():
        came = jnp.where(s < sends, zero, s - per)
        m = (s // per + 2 * (1 - core)) % 3
        there = got_s[came].reshape(rows, -1).astype(f32)
        mine = at_s[pl.ds(pl.multiple_of((s % per) * rows, HEAD // 2), rows), :]
        hold_s[s % 2] = (dot(mine, d_ref[m]) + there).astype(bf16).reshape(hold_s.shape[1:])
        pl.when(s < sends)(lambda: send(s).start())
        stored(s, lambda copy: copy.start())

    @pl.when(s == tiles)
    def _():
        left(s - 2)
        left(s - 1)

    @pl.when(s >= tiles)
    def _():
        wide = wq_ref.shape[FIRST]
        lanes = pl.ds(pl.multiple_of((s - tiles) * wide, wide), wide)
        acc_s[:, lanes] = dot_t(d_ref[FIRST], wq_ref[...]) + dot_t(d_ref[SECOND], wk_ref[...]) + dot_t(d_ref[THIRD], wv_ref[...])

    @pl.when(s == last)
    def _():
        out_ref[...] = norm_back(h_ref[...], acc_s[...], dh_ref[...])


def qkv_back(program, dh, h, dqkv, wa, uo, jobs):
    (t, d), q = h.shape, wa.shape[SECOND] // 4
    side = program.side
    tiles, per_chip = 3 * side, d // side // side
    u = struct((1, side, side, per_chip, q))
    rings = first_rings("raw", (u, u), made=OwnRing)
    for n, ring in enumerate(rings):
        ring.source = n + 1
    matrix = lambda m: block((COLS, q), lambda s: (jnp.maximum(s - tiles, 0), m))
    vmem = lambda n: pltpu.VMEM((n, side, per_chip, q), bf16)
    (out, *us), got = program.kernel(
        functools.partial(qkv_back_body, side=side), "qkv_back", tiles + d // COLS,
        [still((t, d)), still((t, d)), still((3, t, q)), *map(matrix, range(3)), HBM], [still((t, d)), HBM, HBM], [struct((t, d)), u, u],
        [pltpu.VMEM((d, t), bf16), pltpu.VMEM((t, d), f32), vmem(2), vmem(2 * side + 1), dma((tiles,)), dma((2 * side,))],
        12 * t * d * q, (dh, h, dqkv, wa, wa, wa, uo), [*jobs, *((r, (tiles + 1,)) for r in rings)], True, {6: 1})
    return out, tuple(us), got[: len(jobs)], got[len(jobs) :]


def tables_of(t):
    half = HEAD // 2
    angle = jnp.arange(t, dtype=f32)[:, None] * THETA ** (-jnp.arange(half, dtype=f32) / half)
    cos, sin = jnp.cos(angle), jnp.sin(angle)
    return jnp.concatenate([cos, cos], -1), jnp.concatenate([-sin, sin], -1)


def padded(rows):
    return -(-rows // 16) * 16


def pack(w_gate, w_up, w_down, n):
    rows = w_down.shape[SECOND]
    more = padded(rows) - rows

    def spread(w):
        layers, r = w.shape[:2]
        w = jnp.pad(w.reshape(layers, r, n // 2, 2, rows), ((0, 0),) * 4 + ((0, more),))
        return w.swapaxes(-2, -3).reshape(layers, r, -1, COLS).swapaxes(SECOND, THIRD)

    return jnp.concatenate([spread(w_gate), spread(w_up)], axis=-1), jnp.pad(w_down, ((0, 0), (0, more), (0, 0)))


def unpack(wg, n, rows):
    layers, r = wg.shape[FIRST], wg.shape[THIRD]

    def back(w):
        w = w.swapaxes(SECOND, THIRD).reshape(layers, r, 2, n // 2, -1)[..., :rows]
        return w.swapaxes(-2, -3).reshape(layers, r, n * rows)

    return back(wg[..., :COLS]), back(wg[..., COLS:])


def solution(mesh):
    n = mesh.shape["dp"]
    side = math.isqrt(n // 2)

    def step(x, dy, wq, wk, wv, wo, w_gate, w_up, w_down):
        program = Program(side)
        layers, rows = w_down.shape[:2]
        core = place(side)[FIRST]
        tables = tables_of(x.shape[SECOND])
        columns = jnp.concatenate([wq, wk, wv, wo], axis=-1)
        of_a = lambda number: GatherColumns(columns, number, n)
        ((wa,),) = program.carry("first", [of_a(0)])
        tiles, downs = pack(w_gate, w_up, w_down, n)
        of_g, of_d = (lambda number: GatherTiles(tiles, number, n)), (lambda number: GatherRows(downs, number, n))
        h, kept, wd = x[0], [], NONE
        for number in range(layers):
            jobs = [(of_g(number), FRONT)] if number else [(of_g(number), FRONT_BOTH), (of_d(number), FRONT_BOTH)]
            (qkv, o, lse, mid), got = front(program, h, wa, tables, jobs)
            wg, wd = got[FIRST][FIRST], wd if number else got[SECOND][FIRST]
            jobs = [] if number == layers - 1 else [(of_a(number + 1), MLP), (of_d(number + 1), MLP)]
            (gu, out), got = mlp(program, mid, wg, wd, jobs)
            kept.append((wa, wg, wd, h, qkv, o, lse, mid, gu))
            h = out
            if jobs:
                (wa,), (wd,) = got

        def close(got):
            return [ended(raw, own, sums) for _, raw, _, own, sums in got]

        def both(raw, mid):
            return close([(*r, *m) for r, m in zip(raw, mid, strict=True)])

        def whole(got, axis=FIRST):
            return jnp.concatenate([part[:, FIRST, FIRST] for part in close(got)], axis=axis)

        came = lambda raw: [r[FIRST] for r in raw]
        at = lambda steps, rings: [(r, steps) for r in rings]
        by_h, above = dy[0], NONE
        results = []
        for number in reversed(range(layers)):
            wa, wg, wd, hin, qkv, o, lse, mid, gu = kept[number]
            jobs = at(MLP_BACK, second_rings(above[FIRST]) + first_rings("mid", above[SECOND], came(above[THIRD]))) if above else []
            by_mid, ug, ud, got, raw_g = mlp_back(program, by_h, mid, wd, wg, gu, jobs)
            done_d, tail = (whole(got[:2], -1), second_rings(both(above[THIRD], got[2:]))) if above else (NONE, [])
            jobs = at(MIDS, first_rings("raw", ud) + first_rings("mid", ug, came(raw_g))) + at(ATTEND_BACK_RINGS, tail)
            (dqkv, u), got = attend_back(program, by_mid, wa, qkv, o, lse, tables, jobs)
            raw_d, second_g = got[:2], second_rings(both(raw_g, got[2:4]))
            if above:
                results[-1] += [whole(got[4:]), done_d]
            jobs = at(MIDS, first_rings("mid", ud, came(raw_d))) + at(QKV_BACK_RINGS, second_g)
            by_h, us, got, raw_a = qkv_back(program, by_mid, hin, dqkv, wa, cut(u, side), jobs)
            results.append([whole(got[2:])])
            above = both(raw_d, got[:2]), us, raw_a
        got = program.carry("tail", second_rings(above[FIRST]) + first_rings("mid", above[SECOND], came(above[THIRD])))
        done_d, tail = whole(got[:2], -1), second_rings(both(above[THIRD], got[2:]))
        results[-1] += [whole(program.carry("end", tail)), done_d]

        zg, za, zd = (jnp.stack(parts) for parts in zip(*reversed(results), strict=True))

        def swapped(z):
            z = z.reshape(*z.shape[:2], 2, -1, z.shape[-1])
            mine, other = (lax.dynamic_index_in_dim(z, c, 2, keepdims=False) for c in (core, 1 - core))
            got = lax.ppermute(other, "dp", [(b, b ^ 1) for b in range(n)])
            return jnp.where(core == FIRST, mine, got), jnp.where(core == FIRST, got, mine)

        qk, ov = swapped(za)
        by_gate, by_up = unpack(jnp.concatenate(swapped(zg), axis=SECOND), n, rows)
        by_down = zd.reshape(layers, -1, zd.shape[-1])[:, :rows]
        return by_h[None], qk[:, FIRST], qk[:, SECOND], ov[:, SECOND], ov[:, FIRST], by_gate, by_up, by_down

    states, cut_rows = P(("rep", "dp"), None, None), P(None, "dp", None)
    return jax.shard_map(
        step,
        mesh=mesh,
        in_specs=(states, states) + (cut_rows,) * 7,
        out_specs=(states,) + (P("rep", "dp", None),) * 7,
        check_vma=False,
    )


AFTER = (100,) * 3
FRONT = (0, 2, 3, 6, 7, 8)
FRONT_BOTH = MLP = (0, 2, 4, *AFTER)
MIDS = (0, 0, 1, 2)
MLP_BACK = (0, 4, 5, 6)
ATTEND_BACK_RINGS = (0, 7, 8, 9)
QKV_BACK_RINGS = (0, 10, 11, 12)
```

```python
import functools
import math

import jax
import jax.numpy as jnp
from jax import lax
from jax.experimental import pallas as pl
from jax.experimental.pallas import tpu as pltpu
from jax.sharding import PartitionSpec as P

HEAD = 128
THETA = 10000
EPS = 1e-6
LOG2E = 1.4426950408889634
HIDDEN = -2e30
VMEM = 62 * 2**20
COLS = 2 * HEAD
BQ = 256
HBM = pl.BlockSpec(memory_space=pl.ANY)
NONE, FIRST, SECOND, THIRD = None, 0, 1, 2
BOTH, FOUR = range(2), range(4)
HERE = (0, 0)

bf16, f32 = jnp.bfloat16, jnp.float32
dma = pltpu.SemaphoreType.DMA


def dot(a, b, ca=1, cb=0):
    return lax.dot_general(a, b, (((ca,), (cb,)), ((), ())), preferred_element_type=f32)


def dot_t(a, b):
    return dot(a, b, SECOND, SECOND)


def still(shape):
    return pl.BlockSpec(shape, lambda *_: (0,) * len(shape), pipeline_mode=pl.Buffered(SECOND))


def block(shape, where):
    return pl.BlockSpec(shape, where)


def struct(shape, dtype=bf16):
    return jax.ShapeDtypeStruct(shape, dtype)


def now():
    return pl.program_id(FIRST)


def count():
    return pl.num_programs(FIRST)


def scale_of(wide):
    return lax.rsqrt(jnp.mean(wide * wide, -1, keepdims=True) + EPS)


def by_rows(count, do):
    lax.fori_loop(FIRST, count // HEAD, lambda n, _: do(pl.ds(pl.multiple_of(n * HEAD, HEAD), HEAD)), NONE)


def normed(h_ref, out_ref, turn=False):
    def do(rows):
        wide = h_ref[rows, :].astype(f32)
        got = (wide * scale_of(wide)).astype(bf16)
        if turn:
            out_ref[:, rows] = got.T
        else:
            out_ref[rows, :] = got

    by_rows(h_ref.shape[FIRST], do)


def norm_back(h_ref, by_a_ref, by_h_ref, out_ref):
    def do(rows):
        wide = h_ref[rows, :].astype(f32)
        scale = scale_of(wide)
        by_a = by_a_ref[rows, :].astype(bf16).astype(f32)
        mine = scale * by_a - wide * (scale * scale * scale * jnp.mean(by_a * wide, -1, keepdims=True))
        out_ref[rows, :] = plus(by_h_ref[rows, :], mine)

    by_rows(h_ref.shape[FIRST], do)


def plus(h, part):
    return (h.astype(f32) + part.astype(bf16).astype(f32)).astype(bf16)


def place(side):
    me = lax.axis_index("dp")
    core, chip = me % 2, me // 2
    return core, chip // side, chip % side


def number_of(core, x, y, side):
    return (((x + side) % side) * side + (y + side) % side) * 2 + core


def remote(src, dst, send, recv, to):
    return pltpu.make_async_remote_copy(src_ref=src, dst_ref=dst, send_sem=send, recv_sem=recv, device_id={"dp": to}, device_id_type=pl.DeviceIdType.MESH)


class Ring:
    def __init__(self, kind, axis, src, dim, came=NONE, lanes=NONE):
        self.kind, self.axis, self.src, self.dim, self.came = kind, axis, src, dim, came
        lanes = lanes or (FIRST, src.shape[-1])
        self.rows, self.lanes = src.shape[3] // 2, pl.ds(*lanes)
        self.shape = (src.shape[FIRST], src.shape[3 - dim], 2, self.rows, lanes[SECOND])
        self.raw, self.mid = kind != "mid", kind != "raw"

    def given(self):
        return [self.src] + ([] if self.raw else [self.came])

    def results(self):
        return [struct(self.shape)] * (2 * self.raw + 3 * self.mid)

    def scratch(self):
        got = [dma((4,)), dma((4,))] if self.raw else []
        return got + ([dma((2,)), dma((2,)), dma((7,)), pltpu.VMEM((3, *self.shape), bf16)] if self.mid else [])

    def bind(self, given, results, scratch, side):
        core, x, y = place(side)
        self.side, self.at = side, x if self.axis == "x" else y
        near = lambda by: number_of(core, x + by, y, side) if self.axis == "x" else number_of(core, x, y + by, side)
        self.right, self.left = near(1), near(-1)
        results, scratch = list(results), list(scratch)
        self.src_ref = given[FIRST]
        if self.raw:
            self.came_ref, self.raw_ref = results[:2]
            self.send, self.recv = scratch[:2]
        else:
            self.came_ref = given[SECOND]
        if self.mid:
            self.held_ref, self.own_ref, self.sums_ref = results[-3:]
            self.send2, self.recv2, self.local, self.buf = scratch[-4:]

    def part(self, by, half):
        k = (self.at + by + self.side) % self.side
        rows = pl.ds(half * self.rows, self.rows)
        return self.src_ref.at[:, k, :, rows, self.lanes] if self.dim == SECOND else self.src_ref.at[:, :, k, rows, self.lanes]

    def raws(self, n):
        by, half, ref, to = ((2, FIRST, self.came_ref, self.right), (2, SECOND, self.came_ref, self.left),
                             (SECOND, SECOND, self.raw_ref, self.right), (-1, FIRST, self.raw_ref, self.left))[n]
        return remote(self.part(by, half), ref.at[:, :, half], self.send.at[n], self.recv.at[n], to)

    def mids(self, half):
        return remote(self.held_ref.at[:, :, half], self.sums_ref.at[:, :, half], self.send2.at[half], self.recv2.at[half], self.left if half else self.right)

    def load(self, n):
        if n == THIRD:
            return pltpu.make_async_copy(self.came_ref, self.buf.at[SECOND], self.local.at[n])
        if n > THIRD:
            return pltpu.make_async_copy(self.part(FIRST, n - 3), self.buf.at[THIRD, :, :, n - 3], self.local.at[n])
        return pltpu.make_async_copy(self.part(-1 if n else SECOND, n), self.buf.at[FIRST, :, :, n], self.local.at[n])

    def stores(self):
        return [pltpu.make_async_copy(self.buf.at[FIRST], self.held_ref, self.local.at[5]), pltpu.make_async_copy(self.buf.at[THIRD], self.own_ref, self.local.at[6])]

    def start(self):
        if self.raw:
            for n in FOUR:
                self.raws(n).start()

    def turn(self):
        if self.raw and self.mid:
            for n in BOTH:
                self.raws(n).wait_recv()
        if self.mid:
            for n in range(5):
                self.load(n).start()

    def add(self):
        if not self.mid:
            return
        for n in range(5):
            self.load(n).wait()
        for t in range(self.shape[FIRST]):
            for i in range(self.shape[SECOND]):
                self.buf[FIRST, t, i] = (self.buf[FIRST, t, i].astype(f32) + self.buf[SECOND, t, i].astype(f32)).astype(bf16)
        for copy in self.stores():
            copy.start()

    def pass_on(self):
        if self.mid:
            for copy in self.stores():
                copy.wait()
            for half in BOTH:
                self.mids(half).start()

    def finish(self):
        if self.raw:
            for n in FOUR:
                self.raws(n).wait_send()
                if n >= 2 or not self.mid:
                    self.raws(n).wait_recv()
        if self.mid:
            for half in BOTH:
                self.mids(half).wait()

    def events(self):
        return self.start, self.turn, self.add, self.pass_on, self.finish


def first_rings(kind, u, came=(NONE, NONE)):
    if isinstance(u, tuple):
        return [Ring(kind, "x", u[FIRST], SECOND, came[FIRST]), Ring(kind, "y", u[SECOND], THIRD, came[SECOND])]
    w = u.shape[-1] // 2
    return [Ring(kind, axis, u, dim, c, (n * w, w)) for n, (axis, dim, c) in enumerate(zip("xy", (SECOND, THIRD), came, strict=True))]


def second_rings(v):
    return [Ring("ring", axis, part, SECOND) for axis, part in zip("yx", v, strict=True)]


def ended(raw, own, sums):
    got = (own.astype(f32) + raw.astype(f32) + sums.astype(f32)).astype(bf16)
    return got.reshape(*got.shape[:2], 1, -1, got.shape[-1])


NEAR = (0, 1, -1, 2)


class Gather:
    def __init__(self, source, layer, shape):
        self.source, self.layer, self.shape = source, layer, shape

    def given(self):
        return [self.source]

    def results(self):
        return [struct(self.shape)]

    def scratch(self):
        return [dma, dma((2, 36)), dma((2, 36))]

    def bind(self, given, results, scratch, side):
        self.side, self.me = side, place(side)
        (self.from_ref,), (self.full,), (self.local, self.send, self.recv) = given, results, scratch

    def own(self):
        return pltpu.make_async_copy(self.from_ref.at[self.layer], self.whole(number_of(*self.me, self.side)), self.local)

    def spot(self, h, di, dj):
        _, x, y = self.me
        return (x + di, y + dj) if h == FIRST else (x + dj, y + di)

    def move(self, h, k, which, to, quarter=NONE, other=False):
        core = self.me[FIRST]
        share = self.view(number_of(core, *self.spot(h, *which), self.side), h, quarter)
        return remote(share if any(which) else self.mine(h), share, self.send.at[h, k], self.recv.at[h, k], number_of(1 - core if other else core, *self.spot(h, *to), self.side))

    def near(self, h):
        return [self.move(h, k, HERE, (1 - 2 * k, 0)) for k in BOTH]

    def far(self, h):
        return [self.move(h, 2 + k, (2 * k - 1, 0), (1 - 2 * k, 0), k) for k in BOTH]

    def side_ways(self, h, a):
        return [self.move(h, 4 + 2 * a + k, (NEAR[a], 0), (0, 1 - 2 * k)) for k in BOTH]

    def over(self, h, a):
        return [self.move(h, 12 + 2 * a + k, (NEAR[a], 2 * k - 1), (0, 1 - 2 * k), k) for k in BOTH]

    def twin(self, h, a, b):
        return [self.move(h, 20 + 4 * a + b, (NEAR[a], NEAR[b]), HERE, NONE, True)]

    def go(self, what, *places):
        for h in BOTH:
            for a in places:
                for copy in what(h, *a):
                    copy.start()

    def come(self, what, *places):
        for h in BOTH:
            for a in places:
                for copy in what(h, *a):
                    copy.wait_recv()

    def begin(self):
        self.go(self.near, ())
        self.go(self.side_ways, (0,))
        self.go(self.twin, HERE)
        self.own().start()

    def row(self):
        self.come(self.near, ())
        self.go(self.far, ())
        self.go(self.side_ways, (1,), (2,))
        self.go(self.twin, (1, 0), (2, 0))

    def row_end(self):
        self.come(self.far, ())
        self.go(self.side_ways, (3,))
        self.go(self.twin, (3, 0))
        self.come(self.side_ways, (0,))
        self.go(self.over, (0,))

    def plane(self):
        for a in (1, 2):
            self.come(self.side_ways, (a,))
            self.go(self.over, (a,))
        self.go(self.twin, *((a, b) for a in (0, 1, 2) for b in (1, 2)))

    def plane_rest(self):
        self.come(self.side_ways, (3,))
        self.go(self.over, (3,))
        self.go(self.twin, (3, 1), (3, 2))

    def plane_end(self):
        for a in FOUR:
            self.come(self.over, (a,))
            self.go(self.twin, (a, 3))

    def finish(self):
        every = [(a, b) for a in FOUR for b in FOUR]
        self.come(self.twin, *every)
        self.own().wait()
        for what, places in ((self.near, [()]), (self.far, [()]), (self.side_ways, [(a,) for a in FOUR]), (self.over, [(a,) for a in FOUR]), (self.twin, every)):
            for h in BOTH:
                for a in places:
                    for copy in what(h, *a):
                        copy.wait_send()

    def events(self):
        return self.begin, self.row, self.row_end, self.plane, self.plane_rest, self.plane_end, self.finish


class GatherColumns(Gather):
    def __init__(self, source, layer, n):
        _, self.rows, self.width = source.shape
        super().__init__(source, layer, (self.rows * n, self.width))

    def lanes(self, h, quarter):
        part = self.width // 4
        return pl.ds((2 * h + (quarter or 0)) * part, part * (2 if quarter is NONE else 1))

    def view(self, device, h, quarter):
        return self.full.at[pl.ds(device * self.rows, self.rows), self.lanes(h, quarter)]

    def mine(self, h):
        return self.from_ref.at[self.layer, :, self.lanes(h, NONE)]

    def whole(self, device):
        return self.full.at[pl.ds(device * self.rows, self.rows)]


class GatherTiles(Gather):
    def __init__(self, source, layer, n):
        _, self.tiles, self.rows, width = source.shape
        super().__init__(source, layer, (self.tiles, self.rows * n, width))

    def range(self, h, quarter):
        half = self.tiles // 2
        cut = (half + 1) // 2
        first, count = ((0, half), (0, cut), (cut, half - cut))[0 if quarter is NONE else quarter + 1]
        return pl.ds(h * half + first, count)

    def view(self, device, h, quarter):
        return self.full.at[self.range(h, quarter), pl.ds(device * self.rows, self.rows)]

    def mine(self, h):
        return self.from_ref.at[self.layer, self.range(h, NONE)]

    def whole(self, device):
        return self.full.at[:, pl.ds(device * self.rows, self.rows)]


class GatherRows(Gather):
    def __init__(self, source, layer, n):
        _, self.rows, self.width = source.shape
        super().__init__(source, layer, (self.rows * n, self.width))

    def first_row(self, device):
        return ((device % 2) * self.side * self.side + device // 2) * self.rows

    def lanes(self, h):
        return pl.ds(h * (self.width // 2), self.width // 2)

    def view(self, device, h, quarter):
        part = self.rows // 2
        rows = pl.ds(self.first_row(device) + (quarter or 0) * part, self.rows if quarter is NONE else part)
        return self.full.at[rows, self.lanes(h)]

    def mine(self, h):
        return self.from_ref.at[self.layer, :, self.lanes(h)]

    def whole(self, device):
        return self.full.at[pl.ds(self.first_row(device), self.rows)]


def barrier(side, far, partner):
    core, x, y = place(side)
    near = [number_of(core, x + a, y + b, side) for a, b in ((1, 0), (-1, 0), (0, 1), (0, -1))] if far else []
    if partner:
        near.append(number_of(1 - core, x, y, side))
    sem = pltpu.get_barrier_semaphore()
    for to in near:
        pl.semaphore_signal(sem, inc=1, device_id={"dp": to}, device_id_type=pl.DeviceIdType.MESH)
    pl.semaphore_wait(sem, len(near))


class Program:
    def __init__(self, side):
        self.side, self.count = side, 0

    def kernel(self, body, name, steps, ins, outs, shapes, scratch=(), flops=0, args=(), jobs=(), partner=False, alias=NONE):
        self.count += 1
        kinds = [j for j, _ in jobs]
        given = [x for j in kinds for x in j.given()]
        results = [x for j in kinds for x in j.results()]
        ends = [j.scratch() for j in kinds]
        sizes = [len(ins), len(given), len(outs), len(results), len(scratch)]
        talks = bool(jobs) or partner
        side = self.side

        def run(*refs):
            groups, at = [], 0
            for n in sizes:
                groups.append(refs[at : at + n])
                at += n
            own_in, job_in, own_out, job_out, own_scratch = groups
            todo = {}
            for (j, when), scr in zip(jobs, ends, strict=True):
                n, m = len(j.given()), len(j.results())
                j.bind(job_in[:n], job_out[:m], refs[at : at + len(scr)], side)
                job_in, job_out, at = job_in[n:], job_out[m:], at + len(scr)
                for order, (event, step) in enumerate(zip(j.events(), (*when, steps), strict=True)):
                    todo.setdefault((min(step, steps - 1), step >= steps), []).append((order, event))
            i = now()

            @pl.when(i == FIRST)
            def _():
                if talks:
                    barrier(side, bool(jobs), partner or any(isinstance(j, Gather) for j in kinds))

            def perform(last):
                for (step, late), events in sorted(todo.items(), key=lambda e: e[FIRST]):
                    if late == last:

                        @pl.when(i == step)
                        def _(events=events):
                            for _, event in sorted(events, key=lambda e: e[FIRST]):
                                event()

            perform(False)
            body(*own_in, *own_out, *own_scratch)
            perform(True)

        size = sum(a.size * a.dtype.itemsize for a in args)
        extra = dict(collective_id=self.count, has_side_effects=True) if talks else {}
        got = pl.pallas_call(
            run,
            name=name,
            grid=(steps,),
            in_specs=[*ins, *[HBM] * len(given)],
            out_specs=[*outs, *[HBM] * len(results)],
            out_shape=[*shapes, *results],
            scratch_shapes=[*scratch, *[s for e in ends for s in e]],
            input_output_aliases=alias or {},
            compiler_params=pltpu.CompilerParams(dimension_semantics=("arbitrary",), vmem_limit_bytes=VMEM, **extra),
            cost_estimate=pl.CostEstimate(flops=flops, bytes_accessed=size, transcendentals=0),
        )(*args, *given)
        mine, rest = got[: len(outs)], got[len(outs) :]
        per_job = []
        for j in kinds:
            n = len(j.results())
            per_job.append(rest[:n])
            rest = rest[n:]
        return mine, per_job

    def carry(self, name, jobs):
        def body(out_ref):
            out_ref[...] = jnp.zeros_like(out_ref)

        spec = pl.BlockSpec((8, HEAD), lambda i: (0, 0))
        return self.kernel(body, name, 1, [], [spec], [struct((8, HEAD), f32)], jobs=[(j, [0] * (len(j.events()) - 1)) for j in jobs])[SECOND]


def front_body(h_ref, w_ref, wo_ref, cos_ref, sin_ref, qkv_ref, o_ref, lse_ref, mid_ref, a_s, qkv_s, acc_s, *, pairs):
    i = now()

    @pl.when(i == FIRST)
    def _():
        normed(h_ref, a_s)
        acc_s[...] = jnp.zeros_like(acc_s)

    def project(turn):
        for n in range(pairs):
            lanes = slice(n * COLS, (n + 1) * COLS)
            got = dot(a_s[...], w_ref[:, lanes]).astype(bf16)
            if turn:
                got = jnp.concatenate([turned(got[:, :HEAD], cos_ref, sin_ref), turned(got[:, HEAD:], cos_ref, sin_ref)], axis=1)
            qkv_ref[:, lanes] = got
            qkv_s[i * pairs + n] = got

    pl.when(i < 2)(lambda: project(True))
    pl.when(i == 2)(lambda: project(False))

    @pl.when(i > 2)
    def _():
        n = i - 3
        attend(qkv_s.at[n], qkv_s.at[pairs + n], qkv_s.at[2 * pairs + n], o_ref, lse_ref)
        acc_s[...] += dot(o_ref[...], wo_ref[...])

    @pl.when(i == count() - 1)
    def _():
        mid_ref[...] = plus(h_ref[...], acc_s[...])


def turned(t, cos_ref, sin_ref):
    t = t.astype(f32)
    return (t * cos_ref[...] + pltpu.roll(t, HEAD // 2, 1) * sin_ref[...]).astype(bf16)


def hides():
    return lax.broadcasted_iota(jnp.int32, (BQ, BQ), SECOND) >= lax.broadcasted_iota(jnp.int32, (BQ, BQ), FIRST)


def attend(q_ref, k_ref, v_ref, o_ref, lse_ref):
    t, heads = q_ref.shape[FIRST], q_ref.shape[SECOND] // HEAD
    scale = HEAD**-0.5
    e = scale * LOG2E
    seen = hides()
    for n in range(heads):
        lanes = slice(n * HEAD, (n + 1) * HEAD)
        for at in range(0, t, BQ):
            end = at + BQ
            s = dot_t(k_ref[:end, lanes], q_ref[at:end, lanes])
            low = jnp.where(seen, s[at:], HIDDEN)
            s = jnp.concatenate([s[:at], low], axis=0) if at else low
            top = s.max(axis=0, keepdims=True)
            p = jnp.exp2((s - top) * e)
            total = p.sum(axis=0, keepdims=True)
            out = dot(v_ref[:end, lanes].T, p.astype(bf16))
            o_ref[at:end, lanes] = (out * (1 / total)).T.astype(bf16)
            lse_ref[0, n : n + 1, at:end] = top * scale + jnp.log(total)


def front(program, h, wa, tables, jobs):
    t, d = h.shape
    q = wa.shape[SECOND] // 4
    pairs = q // COLS
    late = lambda i: jnp.maximum(i - 3, 0)
    first = lambda i: (0, jnp.minimum(i, 2))
    return program.kernel(
        functools.partial(front_body, pairs=pairs), "front", 3 + pairs,
        [still((t, d)), block((d, q), first), block((COLS, d), lambda i: (late(i), 3)), still((t, HEAD)), still((t, HEAD))],
        [block((t, q), first), block((t, COLS), lambda i: (0, late(i))), block((1, 2, t), lambda i: (late(i), 0, 0)), still((t, d))],
        [struct((t, 3 * q)), struct((t, q)), struct((pairs, 2, t), f32), struct((t, d))],
        [pltpu.VMEM((t, d), bf16), pltpu.VMEM((3 * pairs, t, COLS), bf16), pltpu.VMEM((t, d), f32)],
        8 * t * d * q + 3 * t * t * q, (h, wa, wa, *tables), jobs)


def mlp_body(h_ref, wg_ref, wd_ref, gu_ref, out_ref, b_s, acc_s):
    i = now()

    @pl.when(i == FIRST)
    def _():
        normed(h_ref, b_s)
        acc_s[...] = jnp.zeros_like(acc_s)

    p = []
    for n in range(wg_ref.shape[FIRST]):
        got = dot(b_s[...], wg_ref[n])
        gate, up = got[:, :COLS], got[:, COLS:]
        gu_ref[n] = got
        p.append((gate * jax.nn.sigmoid(gate) * up).astype(bf16))
    acc_s[...] += dot(jnp.concatenate(p, axis=1), wd_ref[...])

    @pl.when(i == count() - 1)
    def _():
        out_ref[...] = plus(h_ref[...], acc_s[...])


def mlp(program, h, wg, wd, jobs):
    (t, d), tiles = h.shape, wg.shape[FIRST]
    wide = lambda rows: block((2, rows, 2 * COLS), lambda i: (i, 0, 0))
    return program.kernel(
        mlp_body, "mlp", tiles // 2,
        [still((t, d)), wide(d), block((2 * COLS, d), lambda i: (i, 0))], [wide(t), still((t, d))],
        [struct((tiles, t, 2 * COLS), f32), struct((t, d))], [pltpu.VMEM((t, d), bf16), pltpu.VMEM((t, d), f32)],
        6 * t * d * tiles * COLS, (h, wg, wd), jobs)


def mlp_back_body(dh_ref, h_ref, wd_ref, wg_ref, gu_ref, out_ref, ug_ref, ud_ref, bt_s, acc_s, hold_g, hold_d, got_g, got_d, send_sem, recv_sem, *, side):
    i = now()
    last = count() - 1
    half = count() // 2
    core, x, y = place(side)
    other = number_of(1 - core, x, y, side)

    def sends(n):
        return [remote(hold.at[n % 2], got.at[n], send_sem.at[n, k], recv_sem.at[n, k], other) for k, (hold, got) in enumerate(((hold_g, got_g), (hold_d, got_d)))]

    def stores(n):
        own = n - half
        return [pltpu.make_async_copy(hold_g.at[n % 2], ug_ref.at[own], send_sem.at[n, FIRST]),
                pltpu.make_async_copy(hold_d.at[n % 2], ud_ref.at[pl.ds(own * COLS, COLS)], send_sem.at[n, SECOND])]

    def left(n):
        @pl.when(n < half)
        def _():
            for copy in sends(n):
                copy.wait_send()

        @pl.when(n >= half)
        def _():
            for copy in stores(n):
                copy.wait()

    @pl.when(i == FIRST)
    def _():
        normed(h_ref, bt_s, True)
        acc_s[...] = jnp.zeros_like(acc_s)
        got_g[half] = jnp.zeros(got_g.shape[1:], bf16)
        got_d[half] = jnp.zeros(got_d.shape[1:], bf16)

    pl.when(i >= 2)(lambda: left(i - 2))

    @pl.when(i >= half)
    def _():
        for copy in sends(i - half):
            copy.wait_recv()

    came = jnp.where(i < half, half, i - half)
    dp = dot_t(dh_ref[...], wd_ref[...]).astype(bf16).astype(f32)
    gate, up = gu_ref[0, :, :COLS], gu_ref[0, :, COLS:]
    s = jax.nn.sigmoid(gate)
    silu = gate * s
    p = (silu * up).astype(bf16)
    by = jnp.concatenate([(dp * up * (s * (1 + gate * (1 - s)))).astype(bf16), (dp * silu).astype(bf16)], axis=1)
    hold_d[i % 2] = (dot(p.T, dh_ref[...]) + got_d[came].astype(f32)).astype(bf16)
    there = got_g[came].reshape(bt_s.shape[FIRST], -1).astype(f32)
    hold_g[i % 2] = (dot(bt_s[...], by) + there).astype(bf16).reshape(hold_g.shape[1:])
    acc_s[...] += dot_t(by, wg_ref[0])

    @pl.when(i < half)
    def _():
        for copy in sends(i):
            copy.start()

    @pl.when(i >= half)
    def _():
        for copy in stores(i):
            copy.start()

    @pl.when(i == last)
    def _():
        norm_back(h_ref, acc_s, dh_ref, out_ref)
        left(i - 1)
        left(i)


def mlp_back(program, dh, h, wd, wg, gu, jobs):
    (t, d), tiles = h.shape, wg.shape[FIRST]
    half = tiles // 2

    def tile(i):
        core = lax.axis_index("dp") % 2
        return jnp.where(i < half, (1 - core) * half + i, core * half + i - half)

    wide = lambda rows: block((1, rows, 2 * COLS), lambda i: (tile(i), 0, 0))
    side = program.side
    by_chip = (side, side, d // side // side, 2 * COLS)
    vmem = lambda n: [pltpu.VMEM((n, *by_chip), bf16), pltpu.VMEM((n, COLS, d), bf16)]
    (out, ug, ud), got = program.kernel(
        functools.partial(mlp_back_body, side=side), "mlp_back", tiles,
        [still((t, d)), still((t, d)), block((COLS, d), lambda i: (tile(i), 0)), wide(d), wide(t)], [still((t, d)), HBM, HBM],
        [struct((t, d)), struct((half, *by_chip)), struct((half * COLS, d))],
        [pltpu.VMEM((d, t), bf16), pltpu.VMEM((t, d), f32), *vmem(2), *vmem(half + 1), dma((tiles, 2)), dma((half, 2))],
        12 * t * d * tiles * COLS, (dh, h, wd, wg, gu), jobs, True)
    return out, ug, cut(ud, side), got


def cut(u, side):
    return u.reshape(1, side, side, -1, u.shape[-1])


def attend_back_body(dh_ref, w_ref, o_ref, q_ref, k_ref, v_ref, lse_ref, cos_ref, sin_ref, out_ref, u_ref, do_s, dq_s, keep_s, got_s, send_sem, recv_sem, *, side):
    i = now()
    pairs = count() // 2
    rows = keep_s.shape[SECOND]
    core, x, y = place(side)
    other = number_of(1 - core, x, y, side)
    copy = lambda n: remote(keep_s.at[n], got_s.at[n], send_sem.at[n], recv_sem.at[n], other)
    store = lambda n: pltpu.make_async_copy(keep_s.at[n], u_ref.at[pl.ds(n * rows, rows)], send_sem.at[n])

    @pl.when(i < pairs)
    def _():
        do_s[i] = dot_t(dh_ref[...], w_ref[...]).astype(bf16)
        keep_s[i] = dot(o_ref[...].T, dh_ref[...]).astype(bf16)
        pl.when(core == FIRST)(lambda: copy(i).start())

    @pl.when(i >= pairs)
    def _():
        n = i - pairs
        pl.when(core == FIRST)(lambda: copy(n).wait_send())

        @pl.when(core == SECOND)
        def _():
            copy(n).wait_recv()
            keep_s[n] = (keep_s[n].astype(f32) + got_s[n].astype(f32)).astype(bf16)
            store(n).start()

        heads_back(q_ref, k_ref, v_ref, do_s.at[n], o_ref, lse_ref, cos_ref, sin_ref, out_ref, dq_s)
        pl.when(core == SECOND)(lambda: store(n).wait())


def heads_back(q_ref, k_ref, v_ref, do_ref, o_ref, lse_ref, cos_ref, sin_ref, out_ref, dq_s):
    t, heads = q_ref.shape[FIRST], q_ref.shape[SECOND] // HEAD
    scale = HEAD**-0.5
    e = scale * LOG2E
    seen = hides()

    def turned_back(x, rows):
        x = (x * scale).astype(bf16).astype(f32)
        return (x * cos_ref[rows, :] - pltpu.roll(x, HEAD // 2, 1) * sin_ref[rows, :]).astype(bf16)

    for n in range(heads):
        lanes = slice(n * HEAD, (n + 1) * HEAD)
        lse = lse_ref[0, n : n + 1, :] * LOG2E
        delta = (do_ref[:, lanes].astype(f32) * o_ref[:, lanes].astype(f32)).T.sum(axis=0, keepdims=True)
        for at in range(0, t, BQ):
            end = at + BQ
            k, v, q, do = k_ref[at:end, lanes], v_ref[at:end, lanes], q_ref[at:, lanes], do_ref[at:, lanes]
            p = jnp.exp2(dot_t(k, q) * e - lse[:, at:])
            low = jnp.where(seen, p[:, :BQ], 0.0)
            p = low if end == t else jnp.concatenate([low, p[:, BQ:]], axis=1)
            ds = (p * (dot_t(v, do) - delta[:, at:])).astype(bf16)
            out_ref[THIRD, at:end, lanes] = dot(p.astype(bf16), do).astype(bf16)
            out_ref[SECOND, at:end, lanes] = turned_back(dot(ds, q), slice(at, end))
            part = dot(k.T, ds)
            if at:
                dq_s[n, :, at:] += part
            else:
                dq_s[n] = part
        out_ref[FIRST, :, lanes] = turned_back(dq_s[n].T, slice(0, t))


def attend_back(program, dh, wa, qkv, o, lse, tables, jobs):
    (t, d), q = dh.shape, o.shape[SECOND]
    pairs = q // COLS
    late = lambda j: jnp.maximum(j - pairs, 0)
    head = lambda first: block((t, COLS), lambda j: (0, first + late(j)))
    tiles = [pltpu.VMEM((pairs, COLS, d), bf16)] * 2
    return program.kernel(
        functools.partial(attend_back_body, side=program.side), "attend_back", 2 * pairs,
        [still((t, d)), block((COLS, d), lambda j: (jnp.minimum(j, pairs - 1), 3)), block((t, COLS), lambda j: (0, j % pairs)),
         head(0), head(pairs), head(2 * pairs), block((1, 2, t), lambda j: (late(j), 0, 0)), still((t, HEAD)), still((t, HEAD))],
        [block((3, t, COLS), lambda j: (0, 0, late(j))), HBM], [struct((3, t, q)), struct((q, d))],
        [pltpu.VMEM((pairs, t, COLS), bf16), pltpu.VMEM((2, HEAD, t), f32), *tiles, dma((pairs,)), dma((pairs,))],
        4 * t * d * q + 7 * t * t * q, (dh, wa, o, qkv, qkv, qkv, lse, *tables), jobs, True)


def qkv_back_body(dh_ref, h_ref, d_ref, wq_ref, wk_ref, wv_ref, _, out_ref, u0_ref, u1_ref, at_s, acc_s, hold_s, got_s, send_sem, recv_sem, *, side):
    s = now()
    last = count() - 1
    per = side
    rows = at_s.shape[FIRST] // per
    core, x, y = place(side)
    other = number_of(1 - core, x, y, side)
    sends = jnp.where(core == FIRST, per, 2 * per)
    zero, tiles = 2 * per, 3 * per

    def send(n):
        to = n + (1 - core) * per
        return remote(hold_s.at[n % 2], got_s.at[to], send_sem.at[n], recv_sem.at[to], other)

    def store(n, ref):
        return pltpu.make_async_copy(hold_s.at[n % 2], ref.at[0, n % per], send_sem.at[n])

    def stored(n, do):
        pl.when((n >= sends) & (n < 2 * per))(lambda: do(store(n, u0_ref)))
        pl.when(n >= 2 * per)(lambda: do(store(n, u1_ref)))

    def left(n):
        pl.when(n < sends)(lambda: send(n).wait_send())
        stored(n, lambda copy: copy.wait())

    @pl.when(s == FIRST)
    def _():
        normed(h_ref, at_s, True)
        got_s[zero] = jnp.zeros(got_s.shape[1:], bf16)

    pl.when((s >= 2) & (s < tiles))(lambda: left(s - 2))

    @pl.when((s >= sends) & (s < tiles))
    def _():
        pltpu.make_async_copy(got_s.at[s - per], got_s.at[s - per], recv_sem.at[s - per]).wait()

    @pl.when(s < tiles)
    def _():
        came = jnp.where(s < sends, zero, s - per)
        m = (s // per + 2 * (1 - core)) % 3
        there = got_s[came].reshape(rows, -1).astype(f32)
        mine = at_s[pl.ds(pl.multiple_of((s % per) * rows, HEAD // 2), rows), :]
        hold_s[s % 2] = (dot(mine, d_ref[m]) + there).astype(bf16).reshape(hold_s.shape[1:])
        pl.when(s < sends)(lambda: send(s).start())
        stored(s, lambda copy: copy.start())

    @pl.when(s == tiles)
    def _():
        left(s - 2)
        left(s - 1)

    @pl.when(s >= tiles)
    def _():
        wide = wq_ref.shape[FIRST]
        lanes = pl.ds(pl.multiple_of((s - tiles) * wide, wide), wide)
        acc_s[:, lanes] = dot_t(d_ref[FIRST], wq_ref[...]) + dot_t(d_ref[SECOND], wk_ref[...]) + dot_t(d_ref[THIRD], wv_ref[...])

    @pl.when(s == last)
    def _():
        norm_back(h_ref, acc_s, dh_ref, out_ref)


def qkv_back(program, dh, h, dqkv, wa, uo, jobs):
    (t, d), q = h.shape, wa.shape[SECOND] // 4
    side = program.side
    tiles, per_chip = 3 * side, d // side // side
    u = struct((1, side, side, per_chip, q))
    matrix = lambda m: block((COLS, q), lambda s: (jnp.maximum(s - tiles, 0), m))
    vmem = lambda n: pltpu.VMEM((n, side, per_chip, q), bf16)
    (out, *us), got = program.kernel(
        functools.partial(qkv_back_body, side=side), "qkv_back", tiles + d // COLS,
        [still((t, d)), still((t, d)), still((3, t, q)), *map(matrix, range(3)), HBM], [still((t, d)), HBM, HBM], [struct((t, d)), u, u],
        [pltpu.VMEM((d, t), bf16), pltpu.VMEM((t, d), f32), vmem(2), vmem(2 * side + 1), dma((tiles,)), dma((2 * side,))],
        12 * t * d * q, (dh, h, dqkv, wa, wa, wa, uo), jobs, True, {6: 1})
    return out, tuple(us), got


def tables_of(t):
    half = HEAD // 2
    angle = jnp.arange(t, dtype=f32)[:, None] * THETA ** (-jnp.arange(half, dtype=f32) / half)
    cos, sin = jnp.cos(angle), jnp.sin(angle)
    return jnp.concatenate([cos, cos], -1), jnp.concatenate([-sin, sin], -1)


def padded(rows):
    return -(-rows // 16) * 16


def pack(w_gate, w_up, w_down, n):
    rows = w_down.shape[SECOND]
    more = padded(rows) - rows

    def spread(w):
        layers, r = w.shape[:2]
        w = jnp.pad(w.reshape(layers, r, n // 2, 2, rows), ((0, 0),) * 4 + ((0, more),))
        return w.swapaxes(-2, -3).reshape(layers, r, -1, COLS).swapaxes(SECOND, THIRD)

    return jnp.concatenate([spread(w_gate), spread(w_up)], axis=-1), jnp.pad(w_down, ((0, 0), (0, more), (0, 0)))


def unpack(wg, n, rows):
    layers, r = wg.shape[FIRST], wg.shape[THIRD]

    def back(w):
        w = w.swapaxes(SECOND, THIRD).reshape(layers, r, 2, n // 2, -1)[..., :rows]
        return w.swapaxes(-2, -3).reshape(layers, r, n * rows)

    return back(wg[..., :COLS]), back(wg[..., COLS:])


def solution(mesh):
    n = mesh.shape["dp"]
    side = math.isqrt(n // 2)

    def step(x, dy, wq, wk, wv, wo, w_gate, w_up, w_down):
        program = Program(side)
        layers, rows = w_down.shape[:2]
        core = place(side)[FIRST]
        tables = tables_of(x.shape[SECOND])
        columns = jnp.concatenate([wq, wk, wv, wo], axis=-1)
        of_a = lambda number: GatherColumns(columns, number, n)
        ((wa,),) = program.carry("first", [of_a(0)])
        tiles, downs = pack(w_gate, w_up, w_down, n)
        of_g, of_d = (lambda number: GatherTiles(tiles, number, n)), (lambda number: GatherRows(downs, number, n))
        h, kept, wd = x[0], [], NONE
        for number in range(layers):
            jobs = [(of_g(number), FRONT)] if number else [(of_g(number), FRONT_BOTH), (of_d(number), FRONT_BOTH)]
            (qkv, o, lse, mid), got = front(program, h, wa, tables, jobs)
            wg, wd = got[FIRST][FIRST], wd if number else got[SECOND][FIRST]
            jobs = [] if number == layers - 1 else [(of_a(number + 1), MLP), (of_d(number + 1), MLP)]
            (gu, out), got = mlp(program, mid, wg, wd, jobs)
            kept.append((wa, wg, wd, h, qkv, o, lse, mid, gu))
            h = out
            if jobs:
                (wa,), (wd,) = got

        def close(got):
            return [ended(raw, own, sums) for _, raw, _, own, sums in got]

        def both(raw, mid):
            return close([(*r, *m) for r, m in zip(raw, mid, strict=True)])

        def whole(got, axis=FIRST):
            return jnp.concatenate([part[:, FIRST, FIRST] for part in close(got)], axis=axis)

        came = lambda raw: [r[FIRST] for r in raw]
        at = lambda steps, rings: [(r, steps) for r in rings]
        by_h, above = dy[0], NONE
        results = []

        def late(above):
            (g, d), us = above
            return second_rings(g) + second_rings(d) + first_rings("ring", us)

        def done(got):
            return [whole(got[:2], -1), whole(got[2:4], -1)], second_rings(close(got[4:]))

        for number in reversed(range(layers)):
            wa, wg, wd, hin, qkv, o, lse, mid, gu = kept[number]
            by_mid, ug, ud, got = mlp_back(program, by_h, mid, wd, wg, gu, at(MLP_BACK, late(above)) if above else [])
            parts, tail = done(got) if above else ([], [])
            jobs = at(MIDS, first_rings("raw", ug) + first_rings("raw", ud))
            (dqkv, u), raw = attend_back(program, by_mid, wa, qkv, o, lse, tables, jobs)
            sent = came(raw)
            jobs = at(MIDS, first_rings("mid", ug, sent[:2]) + first_rings("mid", ud, sent[2:])) + at(QKV_BACK_RINGS, tail)
            by_h, us, got = qkv_back(program, by_mid, hin, dqkv, wa, cut(u, side), jobs)
            if above:
                results.append([*parts, whole(got[4:])])
            above = (both(raw[:2], got[:2]), both(raw[2:], got[2:4])), us
        parts, tail = done(program.carry("tail", late(above)))
        results.append([*parts, whole(program.carry("end", tail))])

        zg, zd, za = (jnp.stack(parts) for parts in zip(*reversed(results), strict=True))

        def swapped(z):
            z = z.reshape(*z.shape[:2], 2, -1, z.shape[-1])
            mine, other = (lax.dynamic_index_in_dim(z, c, 2, keepdims=False) for c in (core, 1 - core))
            got = lax.ppermute(other, "dp", [(b, b ^ 1) for b in range(n)])
            return jnp.where(core == FIRST, mine, got), jnp.where(core == FIRST, got, mine)

        qk, ov = swapped(za)
        by_gate, by_up = unpack(jnp.concatenate(swapped(zg), axis=SECOND), n, rows)
        by_down = zd.reshape(layers, -1, zd.shape[-1])[:, :rows]
        return by_h[None], qk[:, FIRST], qk[:, SECOND], ov[:, SECOND], ov[:, FIRST], by_gate, by_up, by_down

    states, cut_rows = P(("rep", "dp"), None, None), P(None, "dp", None)
    return jax.shard_map(
        step,
        mesh=mesh,
        in_specs=(states, states) + (cut_rows,) * 7,
        out_specs=(states,) + (P("rep", "dp", None),) * 7,
        check_vma=False,
    )


AFTER = (100,) * 3
FRONT = (0, 2, 3, 6, 7, 8)
FRONT_BOTH = MLP = (0, 2, 4, *AFTER)
MIDS = (0, 0, 1, 2)
MLP_BACK = (0, 6, 7, 8)
QKV_BACK_RINGS = (0, 10, 11, 12)
```

```python
import functools
import math

import jax
import jax.numpy as jnp
from jax import lax
from jax.experimental import pallas as pl
from jax.experimental.pallas import tpu as pltpu
from jax.sharding import PartitionSpec as P

HEAD = 128
THETA = 10000
EPS = 1e-6
LOG2E = 1.4426950408889634
HIDDEN = -2e30
VMEM = 62 * 2**20
COLS = 2 * HEAD
BQ = 256
HBM = pl.BlockSpec(memory_space=pl.ANY)
NONE, FIRST, SECOND, THIRD = None, 0, 1, 2
BOTH, FOUR = range(2), range(4)
HERE = (0, 0)

bf16, f32 = jnp.bfloat16, jnp.float32
dma = pltpu.SemaphoreType.DMA


def dot(a, b, ca=1, cb=0):
    return lax.dot_general(a, b, (((ca,), (cb,)), ((), ())), preferred_element_type=f32)


def dot_t(a, b):
    return dot(a, b, SECOND, SECOND)


def still(shape):
    return pl.BlockSpec(shape, lambda *_: (0,) * len(shape), pipeline_mode=pl.Buffered(SECOND))


def block(shape, where):
    return pl.BlockSpec(shape, where)


def struct(shape, dtype=bf16):
    return jax.ShapeDtypeStruct(shape, dtype)


def now():
    return pl.program_id(FIRST)


def count():
    return pl.num_programs(FIRST)


def scale_of(wide):
    return lax.rsqrt(jnp.mean(wide * wide, -1, keepdims=True) + EPS)


def normed(h):
    wide = h.astype(f32)
    return (wide * scale_of(wide)).astype(bf16)


def norm_back(h, by_a, by_h):
    wide = h.astype(f32)
    scale = scale_of(wide)
    by_a = by_a.astype(bf16).astype(f32)
    mine = scale * by_a - wide * (scale * scale * scale * jnp.mean(by_a * wide, -1, keepdims=True))
    return (by_h.astype(f32) + mine.astype(bf16).astype(f32)).astype(bf16)


def plus(h, part):
    return (h.astype(f32) + part.astype(bf16).astype(f32)).astype(bf16)


def place(side):
    me = lax.axis_index("dp")
    core, chip = me % 2, me // 2
    return core, chip // side, chip % side


def number_of(core, x, y, side):
    return (((x + side) % side) * side + (y + side) % side) * 2 + core


def remote(src, dst, send, recv, to):
    return pltpu.make_async_remote_copy(src_ref=src, dst_ref=dst, send_sem=send, recv_sem=recv, device_id={"dp": to}, device_id_type=pl.DeviceIdType.MESH)


class Ring:
    def __init__(self, kind, axis, src, dim, first, width, came=NONE, tiles=NONE):
        self.kind, self.axis, self.src, self.dim, self.first, self.width, self.came = kind, axis, src, dim, first, width, came
        self.rows, self.tiles = src.shape[3] // 2, tiles or (FIRST, src.shape[FIRST])
        self.shape = (self.tiles[SECOND], src.shape[3 - dim], 2, self.rows, width)
        self.raw, self.mid = kind != "mid", kind != "raw"

    def given(self):
        return [self.src] + ([] if self.raw else [self.came])

    def results(self):
        return [struct(self.shape)] * (2 * self.raw + 3 * self.mid)

    def scratch(self):
        got = [dma((4,)), dma((4,))] if self.raw else []
        return got + ([dma((2,)), dma((2,)), dma((7,)), pltpu.VMEM((3, *self.shape), bf16)] if self.mid else [])

    def bind(self, given, results, scratch, side):
        core, x, y = place(side)
        self.side, self.at = side, x if self.axis == "x" else y
        near = lambda by: number_of(core, x + by, y, side) if self.axis == "x" else number_of(core, x, y + by, side)
        self.right, self.left = near(1), near(-1)
        results, scratch = list(results), list(scratch)
        if given:
            self.src_ref = given[FIRST]
        if self.raw:
            self.came_ref, self.raw_ref = results[:2]
            self.send, self.recv = scratch[:2]
        else:
            self.came_ref = given[SECOND]
        if self.mid:
            self.held_ref, self.own_ref, self.sums_ref = results[-3:]
            self.send2, self.recv2, self.local, self.buf = scratch[-4:]

    def part(self, by, half, ts=NONE):
        ts = ts or pl.ds(*self.tiles)
        k = (self.at + by + self.side) % self.side
        rows, lanes = slice(half * self.rows, (half + 1) * self.rows), slice(self.first, self.first + self.width)
        return self.src_ref.at[ts, k, :, rows, lanes] if self.dim == SECOND else self.src_ref.at[ts, :, k, rows, lanes]

    def raws(self, n, ts=NONE, sem=()):
        by, half, ref, to = ((2, FIRST, self.came_ref, self.right), (2, SECOND, self.came_ref, self.left),
                             (SECOND, SECOND, self.raw_ref, self.right), (-1, FIRST, self.raw_ref, self.left))[n]
        return remote(self.part(by, half, ts), ref.at[ts or slice(NONE), :, half], self.send.at[n, *sem], self.recv.at[n, *sem], to)

    def mids(self, half):
        return remote(self.held_ref.at[:, :, half], self.sums_ref.at[:, :, half], self.send2.at[half], self.recv2.at[half], self.left if half else self.right)

    def load(self, n):
        if n == THIRD:
            return pltpu.make_async_copy(self.came_ref, self.buf.at[SECOND], self.local.at[n])
        if n > THIRD:
            return pltpu.make_async_copy(self.part(FIRST, n - 3), self.buf.at[THIRD, :, :, n - 3], self.local.at[n])
        return pltpu.make_async_copy(self.part(-1 if n else SECOND, n), self.buf.at[FIRST, :, :, n], self.local.at[n])

    def stores(self):
        return [pltpu.make_async_copy(self.buf.at[FIRST], self.held_ref, self.local.at[5]), pltpu.make_async_copy(self.buf.at[THIRD], self.own_ref, self.local.at[6])]

    def start(self):
        if self.raw:
            for n in FOUR:
                self.raws(n).start()

    def turn(self):
        if self.raw and self.mid:
            for n in BOTH:
                self.raws(n).wait_recv()
        if self.mid:
            for n in range(5):
                self.load(n).start()

    def add(self):
        if not self.mid:
            return
        for n in range(5):
            self.load(n).wait()
        for t in range(self.shape[FIRST]):
            for i in range(self.shape[SECOND]):
                self.buf[FIRST, t, i] = (self.buf[FIRST, t, i].astype(f32) + self.buf[SECOND, t, i].astype(f32)).astype(bf16)
        for copy in self.stores():
            copy.start()

    def pass_on(self):
        if self.mid:
            for copy in self.stores():
                copy.wait()
            for half in BOTH:
                self.mids(half).start()

    def finish(self):
        if self.raw:
            for n in FOUR:
                self.raws(n).wait_send()
                if n >= 2 or not self.mid:
                    self.raws(n).wait_recv()
        if self.mid:
            for half in BOTH:
                self.mids(half).wait()

    def events(self):
        return self.start, self.turn, self.add, self.pass_on, self.finish


class TileRing(Ring):
    def given(self):
        return []

    def scratch(self):
        return [dma((4, self.shape[FIRST]))] * 2

    def go(self, t):
        for n in FOUR:
            self.raws(n, pl.ds(t, 1), (t,)).start()

    def finish(self):
        for t in range(self.shape[FIRST]):
            for n in FOUR:
                self.raws(n, pl.ds(t, 1), (t,)).wait()

    def events(self):
        return (self.finish,)


def first_rings(kind, u, came=(NONE, NONE), made=Ring, tiles=NONE):
    w = u.shape[-1] // 2
    return [made(kind, "x", u, SECOND, FIRST, w, came[FIRST], tiles), made(kind, "y", u, THIRD, w, w, came[SECOND], tiles)]


def second_rings(v):
    return [Ring("ring", axis, part, SECOND, FIRST, part.shape[-1]) for axis, part in zip("yx", v, strict=True)]


def ended(raw, own, sums):
    got = (own.astype(f32) + raw.astype(f32) + sums.astype(f32)).astype(bf16)
    return got.reshape(*got.shape[:2], 1, -1, got.shape[-1])


NEAR = (0, 1, -1, 2)


class Gather:
    def __init__(self, source, layer, shape):
        self.source, self.layer, self.shape = source, layer, shape

    def given(self):
        return [self.source]

    def results(self):
        return [struct(self.shape)]

    def scratch(self):
        return [dma, dma((2, 36)), dma((2, 36))]

    def bind(self, given, results, scratch, side):
        self.side, self.me = side, place(side)
        (self.from_ref,), (self.full,), (self.local, self.send, self.recv) = given, results, scratch

    def own(self):
        return pltpu.make_async_copy(self.from_ref.at[self.layer], self.whole(number_of(*self.me, self.side)), self.local)

    def spot(self, h, di, dj):
        _, x, y = self.me
        return (x + di, y + dj) if h == FIRST else (x + dj, y + di)

    def move(self, h, k, which, to, quarter=NONE, other=False):
        core = self.me[FIRST]
        share = self.view(number_of(core, *self.spot(h, *which), self.side), h, quarter)
        return remote(share if any(which) else self.mine(h), share, self.send.at[h, k], self.recv.at[h, k], number_of(1 - core if other else core, *self.spot(h, *to), self.side))

    def near(self, h):
        return [self.move(h, k, HERE, (1 - 2 * k, 0)) for k in BOTH]

    def far(self, h):
        return [self.move(h, 2 + k, (2 * k - 1, 0), (1 - 2 * k, 0), k) for k in BOTH]

    def side_ways(self, h, a):
        return [self.move(h, 4 + 2 * a + k, (NEAR[a], 0), (0, 1 - 2 * k)) for k in BOTH]

    def over(self, h, a):
        return [self.move(h, 12 + 2 * a + k, (NEAR[a], 2 * k - 1), (0, 1 - 2 * k), k) for k in BOTH]

    def twin(self, h, a, b):
        return [self.move(h, 20 + 4 * a + b, (NEAR[a], NEAR[b]), HERE, NONE, True)]

    def go(self, what, *places):
        for h in BOTH:
            for a in places:
                for copy in what(h, *a):
                    copy.start()

    def come(self, what, *places):
        for h in BOTH:
            for a in places:
                for copy in what(h, *a):
                    copy.wait_recv()

    def begin(self):
        self.go(self.near, ())
        self.go(self.side_ways, (0,))
        self.go(self.twin, HERE)
        self.own().start()

    def row(self):
        self.come(self.near, ())
        self.go(self.far, ())
        self.go(self.side_ways, (1,), (2,))
        self.go(self.twin, (1, 0), (2, 0))

    def row_end(self):
        self.come(self.far, ())
        self.go(self.side_ways, (3,))
        self.go(self.twin, (3, 0))
        self.come(self.side_ways, (0,))
        self.go(self.over, (0,))

    def plane(self):
        for a in (1, 2):
            self.come(self.side_ways, (a,))
            self.go(self.over, (a,))
        self.go(self.twin, *((a, b) for a in (0, 1, 2) for b in (1, 2)))

    def plane_rest(self):
        self.come(self.side_ways, (3,))
        self.go(self.over, (3,))
        self.go(self.twin, (3, 1), (3, 2))

    def plane_end(self):
        for a in FOUR:
            self.come(self.over, (a,))
            self.go(self.twin, (a, 3))

    def finish(self):
        every = [(a, b) for a in FOUR for b in FOUR]
        self.come(self.twin, *every)
        self.own().wait()
        for what, places in ((self.near, [()]), (self.far, [()]), (self.side_ways, [(a,) for a in FOUR]), (self.over, [(a,) for a in FOUR]), (self.twin, every)):
            for h in BOTH:
                for a in places:
                    for copy in what(h, *a):
                        copy.wait_send()

    def events(self):
        return self.begin, self.row, self.row_end, self.plane, self.plane_rest, self.plane_end, self.finish


class GatherColumns(Gather):
    def __init__(self, source, layer, n):
        _, self.rows, self.width = source.shape
        super().__init__(source, layer, (self.rows * n, self.width))

    def lanes(self, h, quarter):
        part = self.width // 4
        return pl.ds((2 * h + (quarter or 0)) * part, part * (2 if quarter is NONE else 1))

    def view(self, device, h, quarter):
        return self.full.at[pl.ds(device * self.rows, self.rows), self.lanes(h, quarter)]

    def mine(self, h):
        return self.from_ref.at[self.layer, :, self.lanes(h, NONE)]

    def whole(self, device):
        return self.full.at[pl.ds(device * self.rows, self.rows)]


class GatherTiles(Gather):
    def __init__(self, source, layer, n):
        _, self.tiles, self.rows, width = source.shape
        super().__init__(source, layer, (self.tiles, self.rows * n, width))

    def range(self, h, quarter):
        half = self.tiles // 2
        cut = (half + 1) // 2
        first, count = ((0, half), (0, cut), (cut, half - cut))[0 if quarter is NONE else quarter + 1]
        return pl.ds(h * half + first, count)

    def view(self, device, h, quarter):
        return self.full.at[self.range(h, quarter), pl.ds(device * self.rows, self.rows)]

    def mine(self, h):
        return self.from_ref.at[self.layer, self.range(h, NONE)]

    def whole(self, device):
        return self.full.at[:, pl.ds(device * self.rows, self.rows)]


class GatherRows(Gather):
    def __init__(self, source, layer, n):
        _, self.rows, self.width = source.shape
        super().__init__(source, layer, (self.rows * n, self.width))

    def first_row(self, device):
        return ((device % 2) * self.side * self.side + device // 2) * self.rows

    def lanes(self, h):
        return pl.ds(h * (self.width // 2), self.width // 2)

    def view(self, device, h, quarter):
        part = self.rows // 2
        rows = pl.ds(self.first_row(device) + (quarter or 0) * part, self.rows if quarter is NONE else part)
        return self.full.at[rows, self.lanes(h)]

    def mine(self, h):
        return self.from_ref.at[self.layer, :, self.lanes(h)]

    def whole(self, device):
        return self.full.at[pl.ds(self.first_row(device), self.rows)]


def barrier(side, far, partner):
    core, x, y = place(side)
    near = [number_of(core, x + a, y + b, side) for a, b in ((1, 0), (-1, 0), (0, 1), (0, -1))] if far else []
    if partner:
        near.append(number_of(1 - core, x, y, side))
    sem = pltpu.get_barrier_semaphore()
    for to in near:
        pl.semaphore_signal(sem, inc=1, device_id={"dp": to}, device_id_type=pl.DeviceIdType.MESH)
    pl.semaphore_wait(sem, len(near))


class Program:
    def __init__(self, side):
        self.side, self.count = side, 0

    def kernel(self, body, name, steps, ins, outs, shapes, scratch=(), flops=0, args=(), jobs=(), partner=False, alias=NONE):
        self.count += 1
        kinds = [j for j, _ in jobs]
        given = [x for j in kinds for x in j.given()]
        results = [x for j in kinds for x in j.results()]
        ends = [j.scratch() for j in kinds]
        sizes = [len(ins), len(given), len(outs), len(results), len(scratch)]
        talks = bool(jobs) or partner
        side = self.side

        def run(*refs):
            groups, at = [], 0
            for n in sizes:
                groups.append(refs[at : at + n])
                at += n
            own_in, job_in, own_out, job_out, own_scratch = groups
            todo = {}
            for (j, when), scr in zip(jobs, ends, strict=True):
                n, m = len(j.given()), len(j.results())
                j.bind(job_in[:n], job_out[:m], refs[at : at + len(scr)], side)
                job_in, job_out, at = job_in[n:], job_out[m:], at + len(scr)
                for order, (event, step) in enumerate(zip(j.events(), (*when, steps), strict=True)):
                    todo.setdefault((min(step, steps - 1), step >= steps), []).append((order, event))
            i = now()

            @pl.when(i == FIRST)
            def _():
                if talks:
                    barrier(side, bool(jobs), partner or any(isinstance(j, Gather) for j in kinds))

            def perform(last):
                for (step, late), events in sorted(todo.items(), key=lambda e: e[FIRST]):
                    if late == last:

                        @pl.when(i == step)
                        def _(events=events):
                            for _, event in sorted(events, key=lambda e: e[FIRST]):
                                event()

            perform(False)
            body(*own_in, *own_out, *own_scratch)
            perform(True)

        size = sum(a.size * a.dtype.itemsize for a in args)
        extra = dict(collective_id=self.count, has_side_effects=True) if talks else {}
        got = pl.pallas_call(
            run,
            name=name,
            grid=(steps,),
            in_specs=[*ins, *[HBM] * len(given)],
            out_specs=[*outs, *[HBM] * len(results)],
            out_shape=[*shapes, *results],
            scratch_shapes=[*scratch, *[s for e in ends for s in e]],
            input_output_aliases=alias or {},
            compiler_params=pltpu.CompilerParams(dimension_semantics=("arbitrary",), vmem_limit_bytes=VMEM, **extra),
            cost_estimate=pl.CostEstimate(flops=flops, bytes_accessed=size, transcendentals=0),
        )(*args, *given)
        mine, rest = got[: len(outs)], got[len(outs) :]
        per_job = []
        for j in kinds:
            n = len(j.results())
            per_job.append(rest[:n])
            rest = rest[n:]
        return mine, per_job

    def carry(self, name, jobs):
        def body(out_ref):
            out_ref[...] = jnp.zeros_like(out_ref)

        spec = pl.BlockSpec((8, HEAD), lambda i: (0, 0))
        return self.kernel(body, name, 1, [], [spec], [struct((8, HEAD), f32)], jobs=[(j, [0] * (len(j.events()) - 1)) for j in jobs])[SECOND]


def front_body(h_ref, w_ref, wo_ref, cos_ref, sin_ref, qkv_ref, o_ref, lse_ref, mid_ref, a_s, qkv_s, acc_s, *, pairs):
    i = now()

    @pl.when(i == FIRST)
    def _():
        a_s[...] = normed(h_ref[...])
        acc_s[...] = jnp.zeros_like(acc_s)

    def project(turn):
        for n in range(pairs):
            lanes = slice(n * COLS, (n + 1) * COLS)
            got = dot(a_s[...], w_ref[:, lanes]).astype(bf16)
            if turn:
                got = jnp.concatenate([turned(got[:, :HEAD], cos_ref, sin_ref), turned(got[:, HEAD:], cos_ref, sin_ref)], axis=1)
            qkv_ref[:, lanes] = got
            qkv_s[i * pairs + n] = got

    pl.when(i < 2)(lambda: project(True))
    pl.when(i == 2)(lambda: project(False))

    @pl.when(i > 2)
    def _():
        n = i - 3
        attend(qkv_s.at[n], qkv_s.at[pairs + n], qkv_s.at[2 * pairs + n], o_ref, lse_ref)
        acc_s[...] += dot(o_ref[...], wo_ref[...])

    @pl.when(i == count() - 1)
    def _():
        mid_ref[...] = plus(h_ref[...], acc_s[...])


def turned(t, cos_ref, sin_ref):
    t = t.astype(f32)
    return (t * cos_ref[...] + pltpu.roll(t, HEAD // 2, 1) * sin_ref[...]).astype(bf16)


def hides():
    return lax.broadcasted_iota(jnp.int32, (BQ, BQ), SECOND) >= lax.broadcasted_iota(jnp.int32, (BQ, BQ), FIRST)


def attend(q_ref, k_ref, v_ref, o_ref, lse_ref):
    t, heads = q_ref.shape[FIRST], q_ref.shape[SECOND] // HEAD
    scale = HEAD**-0.5
    e = scale * LOG2E
    seen = hides()
    for n in range(heads):
        lanes = slice(n * HEAD, (n + 1) * HEAD)
        for at in range(0, t, BQ):
            end = at + BQ
            s = dot_t(k_ref[:end, lanes], q_ref[at:end, lanes])
            low = jnp.where(seen, s[at:], HIDDEN)
            s = jnp.concatenate([s[:at], low], axis=0) if at else low
            top = s.max(axis=0, keepdims=True)
            p = jnp.exp2((s - top) * e)
            total = p.sum(axis=0, keepdims=True)
            out = dot(v_ref[:end, lanes].T, p.astype(bf16))
            o_ref[at:end, lanes] = (out * (1 / total)).T.astype(bf16)
            lse_ref[0, n : n + 1, at:end] = top * scale + jnp.log(total)


def front(program, h, wa, tables, jobs):
    t, d = h.shape
    q = wa.shape[SECOND] // 4
    pairs = q // COLS
    late = lambda i: jnp.maximum(i - 3, 0)
    first = lambda i: (0, jnp.minimum(i, 2))
    return program.kernel(
        functools.partial(front_body, pairs=pairs), "front", 3 + pairs,
        [still((t, d)), block((d, q), first), block((COLS, d), lambda i: (late(i), 3)), still((t, HEAD)), still((t, HEAD))],
        [block((t, q), first), block((t, COLS), lambda i: (0, late(i))), block((1, 2, t), lambda i: (late(i), 0, 0)), still((t, d))],
        [struct((t, 3 * q)), struct((t, q)), struct((pairs, 2, t), f32), struct((t, d))],
        [pltpu.VMEM((t, d), bf16), pltpu.VMEM((3 * pairs, t, COLS), bf16), pltpu.VMEM((t, d), f32)],
        8 * t * d * q + 3 * t * t * q, (h, wa, wa, *tables), jobs)


def mlp_body(h_ref, wg_ref, wd_ref, gu_ref, out_ref, b_s, acc_s):
    i = now()

    @pl.when(i == FIRST)
    def _():
        b_s[...] = normed(h_ref[...])
        acc_s[...] = jnp.zeros_like(acc_s)

    p = []
    for n in range(wg_ref.shape[FIRST]):
        got = dot(b_s[...], wg_ref[n])
        gate, up = got[:, :COLS], got[:, COLS:]
        gu_ref[n] = got
        p.append((gate * jax.nn.sigmoid(gate) * up).astype(bf16))
    acc_s[...] += dot(jnp.concatenate(p, axis=1), wd_ref[...])

    @pl.when(i == count() - 1)
    def _():
        out_ref[...] = plus(h_ref[...], acc_s[...])


def mlp(program, h, wg, wd, jobs):
    (t, d), tiles = h.shape, wg.shape[FIRST]
    wide = lambda rows: block((2, rows, 2 * COLS), lambda i: (i, 0, 0))
    return program.kernel(
        mlp_body, "mlp", tiles // 2,
        [still((t, d)), wide(d), block((2 * COLS, d), lambda i: (i, 0))], [wide(t), still((t, d))],
        [struct((tiles, t, 2 * COLS), f32), struct((t, d))], [pltpu.VMEM((t, d), bf16), pltpu.VMEM((t, d), f32)],
        6 * t * d * tiles * COLS, (h, wg, wd), jobs)


def mlp_back_body(dh_ref, h_ref, wd_ref, wg_ref, gu_ref, out_ref, ug_ref, ud_ref, bt_s, acc_s, hold_g, hold_d, got_g, got_d, send_sem, recv_sem, *, side, rings):
    i = now()
    last = count() - 1
    half = count() // 2
    for ring in rings:
        ring.src_ref = ug_ref
    core, x, y = place(side)
    other = number_of(1 - core, x, y, side)

    def sends(n):
        return [remote(hold.at[n % 2], got.at[n], send_sem.at[n, k], recv_sem.at[n, k], other) for k, (hold, got) in enumerate(((hold_g, got_g), (hold_d, got_d)))]

    def stores(n):
        own = n - half
        return [pltpu.make_async_copy(hold_g.at[n % 2], ug_ref.at[own], send_sem.at[n, FIRST]),
                pltpu.make_async_copy(hold_d.at[n % 2], ud_ref.at[pl.ds(own * COLS, COLS)], send_sem.at[n, SECOND])]

    def left(n):
        @pl.when(n < half)
        def _():
            for copy in sends(n):
                copy.wait_send()

        @pl.when(n >= half)
        def _():
            for copy in stores(n):
                copy.wait()
            @pl.when(n < last)
            def _():
                for ring in rings:
                    ring.go(n - half)

    @pl.when(i == FIRST)
    def _():
        bt_s[...] = normed(h_ref[...]).T
        acc_s[...] = jnp.zeros_like(acc_s)
        got_g[half] = jnp.zeros(got_g.shape[1:], bf16)
        got_d[half] = jnp.zeros(got_d.shape[1:], bf16)

    pl.when((i >= 2) & (i < half + 2))(lambda: left(i - 2))
    pl.when(i > half)(lambda: left(i - 1))

    @pl.when(i >= half)
    def _():
        for copy in sends(i - half):
            copy.wait_recv()

    came = jnp.where(i < half, half, i - half)
    dp = dot_t(dh_ref[...], wd_ref[...]).astype(bf16).astype(f32)
    gate, up = gu_ref[0, :, :COLS], gu_ref[0, :, COLS:]
    s = jax.nn.sigmoid(gate)
    silu = gate * s
    p = (silu * up).astype(bf16)
    by = jnp.concatenate([(dp * up * (s * (1 + gate * (1 - s)))).astype(bf16), (dp * silu).astype(bf16)], axis=1)
    hold_d[i % 2] = (dot(p.T, dh_ref[...]) + got_d[came].astype(f32)).astype(bf16)
    there = got_g[came].reshape(bt_s.shape[FIRST], -1).astype(f32)
    hold_g[i % 2] = (dot(bt_s[...], by) + there).astype(bf16).reshape(hold_g.shape[1:])
    acc_s[...] += dot_t(by, wg_ref[0])

    @pl.when(i < half)
    def _():
        for copy in sends(i):
            copy.start()

    @pl.when(i >= half)
    def _():
        for copy in stores(i):
            copy.start()

    @pl.when(i == last)
    def _():
        left(i)
        out_ref[...] = norm_back(h_ref[...], acc_s[...], dh_ref[...])


def mlp_back(program, dh, h, wd, wg, gu, jobs):
    (t, d), tiles = h.shape, wg.shape[FIRST]
    half = tiles // 2

    def tile(i):
        core = lax.axis_index("dp") % 2
        return jnp.where(i < half, (1 - core) * half + i, core * half + i - half)

    wide = lambda rows: block((1, rows, 2 * COLS), lambda i: (tile(i), 0, 0))
    side = program.side
    by_chip = (side, side, d // side // side, 2 * COLS)
    vmem = lambda n: [pltpu.VMEM((n, *by_chip), bf16), pltpu.VMEM((n, COLS, d), bf16)]
    rings = first_rings("raw", struct((half, *by_chip)), made=TileRing, tiles=(FIRST, half - 1))
    (out, ug, ud), got = program.kernel(
        functools.partial(mlp_back_body, side=side, rings=rings), "mlp_back", tiles,
        [still((t, d)), still((t, d)), block((COLS, d), lambda i: (tile(i), 0)), wide(d), wide(t)], [still((t, d)), HBM, HBM],
        [struct((t, d)), struct((half, *by_chip)), struct((half * COLS, d))],
        [pltpu.VMEM((d, t), bf16), pltpu.VMEM((t, d), f32), *vmem(2), *vmem(half + 1), dma((tiles, 2)), dma((half, 2))],
        12 * t * d * tiles * COLS, (dh, h, wd, wg, gu), [*jobs, *((r, ()) for r in rings)], True)
    return out, ug, cut(ud[NONE], side), got[: len(jobs)], got[len(jobs) :]


def cut(u, side):
    return u.reshape(u.shape[FIRST], side, side, -1, u.shape[-1])


def attend_back_body(dh_ref, w_ref, o_ref, q_ref, k_ref, v_ref, lse_ref, cos_ref, sin_ref, out_ref, u_ref, do_s, dq_s, keep_s, got_s, send_sem, recv_sem, *, side):
    i = now()
    pairs = count() // 2
    rows = keep_s.shape[SECOND]
    core, x, y = place(side)
    other = number_of(1 - core, x, y, side)
    copy = lambda n: remote(keep_s.at[n], got_s.at[n], send_sem.at[n], recv_sem.at[n], other)
    store = lambda n: pltpu.make_async_copy(keep_s.at[n], u_ref.at[FIRST, pl.ds(n * rows, rows)], send_sem.at[n])

    @pl.when(i < pairs)
    def _():
        do_s[i] = dot_t(dh_ref[...], w_ref[...]).astype(bf16)
        keep_s[i] = dot(o_ref[...].T, dh_ref[...]).astype(bf16)
        pl.when(core == FIRST)(lambda: copy(i).start())

    @pl.when(i >= pairs)
    def _():
        n = i - pairs
        pl.when(core == FIRST)(lambda: copy(n).wait_send())

        @pl.when(core == SECOND)
        def _():
            copy(n).wait_recv()
            keep_s[n] = (keep_s[n].astype(f32) + got_s[n].astype(f32)).astype(bf16)
            store(n).start()

        heads_back(q_ref, k_ref, v_ref, do_s.at[n], o_ref, lse_ref, cos_ref, sin_ref, out_ref, dq_s)
        pl.when(core == SECOND)(lambda: store(n).wait())


def heads_back(q_ref, k_ref, v_ref, do_ref, o_ref, lse_ref, cos_ref, sin_ref, out_ref, dq_s):
    t, heads = q_ref.shape[FIRST], q_ref.shape[SECOND] // HEAD
    scale = HEAD**-0.5
    e = scale * LOG2E
    seen = hides()

    def turned_back(x, rows):
        x = (x * scale).astype(bf16).astype(f32)
        return (x * cos_ref[rows, :] - pltpu.roll(x, HEAD // 2, 1) * sin_ref[rows, :]).astype(bf16)

    for n in range(heads):
        lanes = slice(n * HEAD, (n + 1) * HEAD)
        lse = lse_ref[0, n : n + 1, :] * LOG2E
        delta = (do_ref[:, lanes].astype(f32) * o_ref[:, lanes].astype(f32)).T.sum(axis=0, keepdims=True)
        for at in range(0, t, BQ):
            end = at + BQ
            k, v, q, do = k_ref[at:end, lanes], v_ref[at:end, lanes], q_ref[at:, lanes], do_ref[at:, lanes]
            p = jnp.exp2(dot_t(k, q) * e - lse[:, at:])
            low = jnp.where(seen, p[:, :BQ], 0.0)
            p = low if end == t else jnp.concatenate([low, p[:, BQ:]], axis=1)
            ds = (p * (dot_t(v, do) - delta[:, at:])).astype(bf16)
            out_ref[THIRD, at:end, lanes] = dot(p.astype(bf16), do).astype(bf16)
            out_ref[SECOND, at:end, lanes] = turned_back(dot(ds, q), slice(at, end))
            part = dot(k.T, ds)
            if at:
                dq_s[n, :, at:] += part
            else:
                dq_s[n] = part
        out_ref[FIRST, :, lanes] = turned_back(dq_s[n].T, slice(0, t))


def attend_back(program, dh, wa, qkv, o, lse, tables, jobs):
    (t, d), q = dh.shape, o.shape[SECOND]
    pairs = q // COLS
    late = lambda j: jnp.maximum(j - pairs, 0)
    head = lambda first: block((t, COLS), lambda j: (0, first + late(j)))
    tiles = [pltpu.VMEM((pairs, COLS, d), bf16)] * 2
    return program.kernel(
        functools.partial(attend_back_body, side=program.side), "attend_back", 2 * pairs,
        [still((t, d)), block((COLS, d), lambda j: (jnp.minimum(j, pairs - 1), 3)), block((t, COLS), lambda j: (0, j % pairs)),
         head(0), head(pairs), head(2 * pairs), block((1, 2, t), lambda j: (late(j), 0, 0)), still((t, HEAD)), still((t, HEAD))],
        [block((3, t, COLS), lambda j: (0, 0, late(j))), HBM], [struct((3, t, q)), struct((2, d, q))],
        [pltpu.VMEM((pairs, t, COLS), bf16), pltpu.VMEM((2, HEAD, t), f32), *tiles, dma((pairs,)), dma((pairs,))],
        4 * t * d * q + 7 * t * t * q, (dh, wa, o, qkv, qkv, qkv, lse, *tables), jobs, True)


def qkv_back_body(dh_ref, h_ref, d_ref, w_ref, _, out_ref, u_ref, at_s, acc_s, hold_s, got_s, send_sem, recv_sem, *, side):
    s = now()
    last = count() - 1
    rows = w_ref.shape[FIRST]
    per = at_s.shape[FIRST] // rows
    r = s % per
    core, x, y = place(side)
    other = number_of(1 - core, x, y, side)
    sends = jnp.where(core == FIRST, per, 2 * per)
    zero = 2 * per

    def send(n):
        to = n + (1 - core) * per
        return remote(hold_s.at[n % 2], got_s.at[to], send_sem.at[n], recv_sem.at[to], other)

    def store(n):
        return pltpu.make_async_copy(hold_s.at[n % 2], u_ref.at[n // per - 1, pl.ds((n % per) * rows, rows)], send_sem.at[n])

    def left(n):
        pl.when(n < sends)(lambda: send(n).wait_send())
        pl.when(n >= sends)(lambda: store(n).wait())

    @pl.when(s == FIRST)
    def _():
        at_s[...] = normed(h_ref[...]).T
        acc_s[...] = jnp.zeros_like(acc_s)
        got_s[zero] = jnp.zeros(got_s.shape[1:], bf16)

    pl.when(s >= 2)(lambda: left(s - 2))

    @pl.when(s >= sends)
    def _():
        pltpu.make_async_copy(got_s.at[s - per], got_s.at[s - per], recv_sem.at[s - per]).wait()

    lanes = pl.ds(pl.multiple_of(r * rows, rows), rows)
    acc_s[:, lanes] += dot_t(d_ref[0], w_ref[...])
    came = jnp.where(s < sends, zero, s - per)
    hold_s[s % 2] = (dot(at_s[lanes, :], d_ref[0]) + got_s[came].astype(f32)).astype(bf16)
    pl.when(s < sends)(lambda: send(s).start())
    pl.when(s >= sends)(lambda: store(s).start())

    @pl.when(s == last)
    def _():
        out_ref[...] = norm_back(h_ref[...], acc_s[...], dh_ref[...])
        left(s - 1)
        left(s)


def qkv_back(program, dh, h, dqkv, wa, u, jobs):
    (t, d), q = h.shape, wa.shape[SECOND] // 4
    rows = COLS
    per = d // rows
    matrix = lambda s: (s // per + 2 * (1 - lax.axis_index("dp") % 2)) % 3
    (out, u), got = program.kernel(
        functools.partial(qkv_back_body, side=program.side), "qkv_back", 3 * per,
        [still((t, d)), still((t, d)), block((1, t, q), lambda s: (matrix(s), 0, 0)), block((rows, q), lambda s: (s % per, matrix(s))), HBM],
        [still((t, d)), HBM], [struct((t, d)), struct(u.shape)],
        [pltpu.VMEM((d, t), bf16), pltpu.VMEM((t, d), f32), pltpu.VMEM((2, rows, q), bf16), pltpu.VMEM((2 * per + 1, rows, q), bf16), dma((3 * per,)), dma((2 * per,))],
        12 * t * d * q, (dh, h, dqkv, wa, u), jobs, True, {4: 1})
    return out, cut(u, program.side), got


def tables_of(t):
    half = HEAD // 2
    angle = jnp.arange(t, dtype=f32)[:, None] * THETA ** (-jnp.arange(half, dtype=f32) / half)
    cos, sin = jnp.cos(angle), jnp.sin(angle)
    return jnp.concatenate([cos, cos], -1), jnp.concatenate([-sin, sin], -1)


def padded(rows):
    return -(-rows // 16) * 16


def spread_body(gate_ref, up_ref, out_ref, *, n, rows):
    for k, ref in enumerate((gate_ref, up_ref)):
        wide = ref[0].astype(f32)
        gap = [jnp.zeros((wide.shape[0], padded(rows) - rows), f32)] if padded(rows) > rows else []
        parts = []
        for core in BOTH:
            for chip in range(n // 2):
                first = (2 * chip + core) * rows
                parts += [wide[:, first : first + rows], *gap]
        both = jnp.concatenate(parts, axis=1).astype(bf16)
        for t in range(out_ref.shape[SECOND]):
            out_ref[0, t, :, k * COLS : (k + 1) * COLS] = both[:, t * COLS : (t + 1) * COLS]


def opening(program, w_gate, w_up, rows, n, gather):
    layers, r, width = w_gate.shape
    tiles = n * padded(rows) // COLS
    return program.kernel(
        functools.partial(spread_body, n=n, rows=rows), "first", layers, [block((1, r, width), lambda i: (i, 0, 0))] * 2,
        [block((1, tiles, r, 2 * COLS), lambda i: (i, 0, 0, 0))], [struct((layers, tiles, r, 2 * COLS))], args=(w_gate, w_up), jobs=[(gather, OPENING)])


def unpack(wg, n, rows):
    layers, r = wg.shape[FIRST], wg.shape[THIRD]

    def back(w):
        w = w.swapaxes(SECOND, THIRD).reshape(layers, r, 2, n // 2, -1)[..., :rows]
        return w.swapaxes(-2, -3).reshape(layers, r, n * rows)

    return back(wg[..., :COLS]), back(wg[..., COLS:])


def solution(mesh):
    n = mesh.shape["dp"]
    side = math.isqrt(n // 2)

    def step(x, dy, wq, wk, wv, wo, w_gate, w_up, w_down):
        program = Program(side)
        layers, rows = w_down.shape[:2]
        core = place(side)[FIRST]
        tables = tables_of(x.shape[SECOND])
        columns = jnp.concatenate([wq, wk, wv, wo], axis=-1)
        of_a = lambda number: GatherColumns(columns, number, n)
        (tiles,), ((wa,),) = opening(program, w_gate, w_up, rows, n, of_a(0))
        downs = jnp.pad(w_down, ((0, 0), (0, padded(rows) - rows), (0, 0)))
        of_g, of_d = (lambda number: GatherTiles(tiles, number, n)), (lambda number: GatherRows(downs, number, n))
        h, kept, wd = x[0], [], NONE
        for number in range(layers):
            jobs = [(of_g(number), FRONT)] if number else [(of_g(number), FRONT_BOTH), (of_d(number), FRONT_BOTH)]
            (qkv, o, lse, mid), got = front(program, h, wa, tables, jobs)
            wg, wd = got[FIRST][FIRST], wd if number else got[SECOND][FIRST]
            jobs = [] if number == layers - 1 else [(of_a(number + 1), MLP), (of_d(number + 1), MLP)]
            (gu, out), got = mlp(program, mid, wg, wd, jobs)
            kept.append((wa, wg, wd, h, qkv, o, lse, mid, gu))
            h = out
            if jobs:
                (wa,), (wd,) = got

        def close(got):
            return [ended(raw, own, sums) for _, raw, _, own, sums in got]

        def both(raw, mid):
            return close([(*r, *m) for r, m in zip(raw, mid, strict=True)])

        def whole(got):
            return jnp.concatenate([part[:, FIRST, FIRST] for part in close(got)], axis=-1)

        came = lambda raw: [r[FIRST] for r in raw]
        at = lambda steps, rings: [(r, steps) for r in rings]
        by_h, above = dy[0], NONE
        results = []
        for number in reversed(range(layers)):
            wa, wg, wd, hin, qkv, o, lse, mid, gu = kept[number]
            jobs = at(MLP_BACK, second_rings(above[FIRST]) + first_rings("ring", above[SECOND])) if above else []
            by_mid, ug, ud, got, raw_g = mlp_back(program, by_h, mid, wd, wg, gu, jobs)
            done_d, tail = (whole(got[:2]), second_rings(close(got[2:]))) if above else (NONE, [])
            most = ug.shape[FIRST] - 1
            jobs = at(LAST_TILE, first_rings("ring", ug, tiles=(most, 1))) + at(MIDS, first_rings("raw", ud) + first_rings("mid", ug, came(raw_g), tiles=(FIRST, most)))
            (dqkv, u), got = attend_back(program, by_mid, wa, qkv, o, lse, tables, jobs)
            raw_d, parts_g = got[2:4], zip(both(raw_g, got[4:]), close(got[:2]), strict=True)
            second_g = second_rings([jnp.concatenate(parts) for parts in parts_g])
            jobs = at(MIDS, first_rings("mid", ud, came(raw_d))) + at(QKV_BACK_RINGS, second_g + tail)
            by_h, ua, got = qkv_back(program, by_mid, hin, dqkv, wa, u, jobs)
            if above:
                results[-1] += [whole(got[4:]), done_d]
            results.append([whole(got[2:4])])
            above = both(raw_d, got[:2]), ua
        got = program.carry("tail", second_rings(above[FIRST]) + first_rings("ring", above[SECOND]))
        done_d, tail = whole(got[:2]), second_rings(close(got[2:]))
        results[-1] += [whole(program.carry("end", tail)), done_d]

        zg, za, zd = (jnp.stack(parts) for parts in zip(*reversed(results), strict=True))

        def swapped(z):
            z = z.reshape(*z.shape[:2], 2, -1, z.shape[-1])
            mine, other = (lax.dynamic_index_in_dim(z, c, 2, keepdims=False) for c in (core, 1 - core))
            got = lax.ppermute(other, "dp", [(b, b ^ 1) for b in range(n)])
            return jnp.where(core == FIRST, mine, got), jnp.where(core == FIRST, got, mine)

        qk, ov = swapped(za)
        by_gate, by_up = unpack(jnp.concatenate(swapped(zg), axis=SECOND), n, rows)
        by_down = zd.reshape(layers, -1, zd.shape[-1])[:, :rows]
        return by_h[None], qk[:, FIRST], qk[:, SECOND], ov[:, SECOND], ov[:, FIRST], by_gate, by_up, by_down

    states, cut_rows = P(("rep", "dp"), None, None), P(None, "dp", None)
    return jax.shard_map(
        step,
        mesh=mesh,
        in_specs=(states, states) + (cut_rows,) * 7,
        out_specs=(states,) + (P("rep", "dp", None),) * 7,
        check_vma=False,
    )


AFTER = (100,) * 3
FRONT = (0, 2, 3, 6, 7, 8)
FRONT_BOTH = MLP = (0, 2, 4, *AFTER)
OPENING = (0, 1, 2, *AFTER)
MIDS = (0, 0, 1, 2)
LAST_TILE = (0, 2, 3, 4)
MLP_BACK = (0, 5, 6, 7)
QKV_BACK_RINGS = (0, 7, 8, 9)
```
